128 devices in a mesh: dp: 1, tp: 16 (over z, y), pp: 8 (over x, core).
Axes of the slice: x: 4, y: 4, z: 4, core: 2. Of those that a mesh axis runs over, the one named last changes fastest.
Arguments:
- tokens: int32 [32, 64], P('dp')
- labels: int32 [32, 64], P('dp')
- emb_table: bfloat16 [50304, 1024], P('tp')
- w_in: bfloat16 [8, 1024, 4096], P('pp', None, 'tp')
- w_out: bfloat16 [8, 4096, 1024], P('pp', 'tp')
Outputs:
- output 1: float32 [1], P('dp')
- output 2: float32 [8, 1024, 4096], P(('dp', 'pp'), None, 'tp')
- output 3: float32 [8, 4096, 1024], P(('dp', 'pp'), 'tp')
- output 4: float32 [50304, 1024], P(('dp', 'tp'))
All inputs are finite; a program needn't handle non-finite values.
Results may differ from the reference program's by a relative error of at most 0.012808.
Values are sent between devices in bfloat16 or wider.
A program may use at most 1 GiB of HBM per device.

```python
import jax
import jax.numpy as jnp
from jax import lax

VOCAB_SIZE = 50304
MODEL_DIM = 1024
HIDDEN_DIM = 4096
NUM_STAGES = 8
MICRO_BATCHES = 32
SEQ_LEN = 64
NORM_EPS = 1e-6


def setup_inputs(seed: int = 0, part: int = 0) -> dict:
    part_key = jax.random.fold_in(jax.random.key(seed), part)
    key_outer, key_inner, key_rank, key_perm = jax.random.split(part_key, 4)
    id_shape = (MICRO_BATCHES, SEQ_LEN + 1)
    outer_cap = jax.random.randint(key_outer, id_shape, 1, VOCAB_SIZE + 1)
    inner_cap = jax.random.randint(key_inner, id_shape, 1, outer_cap + 1)
    rank_ids = jax.random.randint(key_rank, id_shape, 0, inner_cap)
    vocab_order = jax.random.permutation(key_perm, VOCAB_SIZE)
    id_seq = vocab_order[rank_ids].astype(jnp.int32)
    key_table, key_first, key_second = jax.random.split(jax.random.key(seed + 1), 3)
    emb_table = jax.random.normal(key_table, (VOCAB_SIZE, MODEL_DIM), jnp.float32) * MODEL_DIM ** -0.5
    w_in = jax.random.normal(key_first, (NUM_STAGES, MODEL_DIM, HIDDEN_DIM), jnp.float32) * MODEL_DIM ** -0.5
    w_out = jax.random.normal(key_second, (NUM_STAGES, HIDDEN_DIM, MODEL_DIM), jnp.float32) * (HIDDEN_DIM * NUM_STAGES / 2) ** -0.5
    return {'tokens': id_seq[:, :SEQ_LEN], 'labels': id_seq[:, 1:], 'emb_table': emb_table.astype(jnp.bfloat16), 'w_in': w_in.astype(jnp.bfloat16), 'w_out': w_out.astype(jnp.bfloat16)}


def reference(tokens, labels, emb_table, w_in, w_out):
    vocab_ids = jnp.arange(VOCAB_SIZE, dtype=jnp.int32)

    def layer_fwd(x_act, weights):
        w_one, w_two = weights
        hidden = jnp.dot(x_act, w_one, preferred_element_type=jnp.float32)
        gate_act = jax.nn.gelu(hidden).astype(jnp.bfloat16)
        branch_out = jnp.dot(gate_act, w_two, preferred_element_type=jnp.float32)
        return (x_act.astype(jnp.float32) + branch_out).astype(jnp.bfloat16), (x_act, hidden)

    def layer_bwd(grad_y, saved_act):
        x_act, hidden, w_one, w_two = saved_act
        gate_act, gelu_vjp = jax.vjp(jax.nn.gelu, hidden)
        grad_gate = jnp.dot(grad_y, w_two.T, preferred_element_type=jnp.float32)
        grad_hidden = gelu_vjp(grad_gate)[0].astype(jnp.bfloat16)
        grad_two = jnp.dot(gate_act.astype(jnp.bfloat16).T, grad_y, preferred_element_type=jnp.float32)
        grad_one = jnp.dot(x_act.T, grad_hidden, preferred_element_type=jnp.float32)
        grad_x = (grad_y.astype(jnp.float32) + jnp.dot(grad_hidden, w_one.T, preferred_element_type=jnp.float32)).astype(jnp.bfloat16)
        return grad_x, (grad_one, grad_two)

    def micro_step(carry_in, micro_in):
        loss_sum, acc_one, acc_two, acc_table = carry_in
        tok_row, lab_row = micro_in
        x_first = emb_table[tok_row]
        x_top, saved_fwd = lax.scan(layer_fwd, x_first, (w_in, w_out))
        x_wide = x_top.astype(jnp.float32)
        inv_rms = lax.rsqrt(jnp.mean(x_wide * x_wide, axis=-1, keepdims=True) + NORM_EPS)
        normed = x_wide * inv_rms
        normed_b = normed.astype(jnp.bfloat16)
        logits = jnp.dot(normed_b, emb_table.T, preferred_element_type=jnp.float32)
        log_norm = jax.nn.logsumexp(logits, axis=-1)
        target_hit = lab_row[:, None] == vocab_ids[None, :]
        target_logit = jnp.sum(jnp.where(target_hit, logits, 0.0), axis=-1)
        grad_logits = (jnp.exp(logits - log_norm[:, None]) - target_hit.astype(jnp.float32)).astype(jnp.bfloat16)
        head_grad = jnp.dot(grad_logits.T, normed_b, preferred_element_type=jnp.float32)
        grad_normed = jnp.dot(grad_logits, emb_table, preferred_element_type=jnp.float32)
        grad_top = (inv_rms * (grad_normed - normed * jnp.mean(normed * grad_normed, axis=-1, keepdims=True))).astype(jnp.bfloat16)
        grad_first, stage_grads = lax.scan(layer_bwd, grad_top, (saved_fwd[0], saved_fwd[1], w_in, w_out), reverse=True)
        new_table = (acc_table + head_grad).at[tok_row].add(grad_first.astype(jnp.float32))
        return (loss_sum + jnp.sum(log_norm - target_logit), acc_one + stage_grads[0], acc_two + stage_grads[1], new_table), None

    zero_state = (jnp.zeros((), jnp.float32), jnp.zeros((NUM_STAGES, MODEL_DIM, HIDDEN_DIM), jnp.float32), jnp.zeros((NUM_STAGES, HIDDEN_DIM, MODEL_DIM), jnp.float32), jnp.zeros((VOCAB_SIZE, MODEL_DIM), jnp.float32))
    totals = lax.scan(micro_step, zero_state, (tokens, labels))[0]
    mean_loss = (totals[0] / (MICRO_BATCHES * SEQ_LEN)).reshape(1)
    return mean_loss, totals[1], totals[2], totals[3]
```

```python
import jax
import jax.numpy as jnp
from jax import lax
from jax.sharding import PartitionSpec as P

NORM_EPS = 1e-6


def contract(lhs, rhs, lhs_dim, rhs_dim):
    return lax.dot_general(lhs, rhs, (((lhs_dim,), (rhs_dim,)), ((), ())), preferred_element_type=jnp.float32)


def gelu_slope(hidden):
    gate, pull = jax.vjp(jax.nn.gelu, hidden)
    return gate, pull(jnp.ones_like(gate))[0]


def solution(mesh):
    pp_size = mesh.shape['pp']
    tp_size = mesh.shape['tp']
    fwd_perm = [(src, src + 1) for src in range(pp_size - 1)]
    bwd_perm = [(src + 1, src) for src in range(pp_size - 1)]

    def device_fn(tokens, labels, emb_table, w_in, w_out):
        num_tokens = tokens.shape[0] * tokens.shape[1]
        vocab_rows, model_dim = emb_table.shape
        w_one, w_two = w_in[0], w_out[0]
        stage = lax.axis_index('pp')
        is_first = stage == 0
        is_last = stage == pp_size - 1
        base = lax.axis_index('tp') * vocab_rows
        unit = num_tokens // (pp_size * tp_size)

        def reorder(ids):
            return ids.reshape(pp_size, tp_size, unit).transpose(1, 0, 2).reshape(num_tokens)

        tok_local = reorder(tokens) - base
        lab_local = reorder(labels) - base
        row_ids = jnp.arange(vocab_rows, dtype=jnp.int32)

        owned = (tok_local >= 0) & (tok_local < vocab_rows)
        looked = jnp.take(emb_table, jnp.clip(tok_local, 0, vocab_rows - 1), axis=0)
        looked = jnp.where(owned[:, None], looked, jnp.zeros_like(looked))
        x_act = lax.psum_scatter(looked, 'tp', scatter_dimension=0, tiled=True)

        w_one_full = lax.all_gather(w_one, 'tp', axis=1, tiled=True)
        w_two_full = lax.all_gather(w_two, 'tp', axis=0, tiled=True)

        x_mine = jnp.zeros_like(x_act)
        for tick in range(pp_size):
            x_mine = jnp.where(stage == tick, x_act, x_mine)
            gate = jax.nn.gelu(jnp.dot(x_act, w_one_full, preferred_element_type=jnp.float32)).astype(jnp.bfloat16)
            branch = jnp.dot(gate, w_two_full, preferred_element_type=jnp.float32)
            y_act = (x_act.astype(jnp.float32) + branch).astype(jnp.bfloat16)
            if tick < pp_size - 1:
                x_act = lax.ppermute(y_act, 'pp', fwd_perm)

        slope = gelu_slope(jnp.dot(x_mine, w_one_full, preferred_element_type=jnp.float32))[1]

        top = lax.psum(jnp.where(is_last, y_act, jnp.zeros_like(y_act)), 'pp')
        top = lax.all_gather(top, 'tp', axis=0, tiled=True)
        x_wide = top.astype(jnp.float32)
        inv_rms = lax.rsqrt(jnp.mean(x_wide * x_wide, axis=-1, keepdims=True) + NORM_EPS)
        normed = x_wide * inv_rms
        normed_b = normed.astype(jnp.bfloat16)
        hit = lab_local[:, None] == row_ids[None, :]
        logits = contract(normed_b, emb_table, 1, 1)
        local_lse = jax.nn.logsumexp(logits, axis=-1)
        local_target = jnp.sum(jnp.where(hit, logits, 0.0), axis=-1)
        stats = lax.all_gather(jnp.stack([local_lse, local_target]), 'tp')
        log_norm = jax.nn.logsumexp(stats[:, 0], axis=0)
        target_logit = jnp.sum(stats[:, 1], axis=0)
        mean_loss = jnp.sum(log_norm - target_logit) / num_tokens
        grad_logits = (jnp.exp(logits - log_norm[:, None]) - hit.astype(jnp.float32)).astype(jnp.bfloat16)

        def my_part(arr):
            return lax.dynamic_index_in_dim(arr.reshape(tp_size, pp_size, unit, arr.shape[-1]), stage, 1, keepdims=False).reshape(tp_size * unit, arr.shape[-1])

        dn_part = contract(my_part(grad_logits), emb_table, 1, 0)
        dn = lax.psum_scatter(dn_part, 'tp', scatter_dimension=0, tiled=True)
        tp_idx = lax.axis_index('tp')
        m_own = lax.dynamic_slice_in_dim(my_part(normed), tp_idx * unit, unit, 0)
        r_own = lax.dynamic_slice_in_dim(my_part(inv_rms), tp_idx * unit, unit, 0)
        g_own = (r_own * (dn - m_own * jnp.mean(m_own * dn, axis=-1, keepdims=True))).astype(jnp.bfloat16)
        g_act = lax.all_gather(g_own, 'pp', axis=0, tiled=True)

        dy_mine = jnp.zeros_like(g_act)
        for tick in range(pp_size - 1, -1, -1):
            dy_mine = jnp.where(stage == tick, g_act, dy_mine)
            grad_hidden = (slope * contract(g_act, w_two_full, 1, 1)).astype(jnp.bfloat16)
            grad_x = (g_act.astype(jnp.float32) + contract(grad_hidden, w_one_full, 1, 1)).astype(jnp.bfloat16)
            if tick > 0:
                g_act = lax.ppermute(grad_x, 'pp', bwd_perm)

        x_all = lax.all_gather(x_mine, 'tp', axis=0, tiled=True)
        dy_all = lax.all_gather(dy_mine, 'tp', axis=0, tiled=True)
        gate_all, slope_all = gelu_slope(jnp.dot(x_all, w_one, preferred_element_type=jnp.float32))
        dh_all = (slope_all * contract(dy_all, w_two, 1, 1)).astype(jnp.bfloat16)
        grad_two = contract(gate_all.astype(jnp.bfloat16), dy_all, 0, 0)
        grad_one = contract(x_all, dh_all, 0, 0)

        dx_first = lax.psum(jnp.where(is_first, grad_x, jnp.zeros_like(grad_x)), 'pp')
        dx_first = lax.all_gather(dx_first, 'tp', axis=0, tiled=True)
        one_hot = (tok_local[:, None] == row_ids[None, :]).astype(jnp.bfloat16)
        grad_table = contract(grad_logits, normed_b, 0, 0) + contract(one_hot, dx_first, 0, 0)
        return mean_loss.reshape(1), grad_one[None], grad_two[None], grad_table

    return jax.shard_map(device_fn, mesh=mesh, in_specs=(P('dp', None), P('dp', None), P('tp', None), P('pp', None, 'tp'), P('pp', 'tp', None)), out_specs=(P('dp'), P(('dp', 'pp'), None, 'tp'), P(('dp', 'pp'), 'tp', None), P(('dp', 'tp'), None)), check_vma=False)
```

```python
import functools

import jax
import jax.numpy as jnp
from jax import lax
from jax.experimental import pallas as pl
from jax.experimental.pallas import tpu as pltpu
from jax.sharding import PartitionSpec as P

NORM_EPS = 1e-6
SIDE = 4
MESH = pl.DeviceIdType.MESH
F32 = jnp.float32
BF16 = jnp.bfloat16
VMEM_LIMIT = 63 * 1024 * 1024
CUBE = 0.044715
ROOT = 0.7978845608028654


def contract(lhs, rhs, lhs_dim, rhs_dim):
    return lax.dot_general(lhs, rhs, (((lhs_dim,), (rhs_dim,)), ((), ())), preferred_element_type=F32)


def gelu(h):
    return h * (0.5 * (1.0 + jnp.tanh(ROOT * (h + CUBE * (h * h * h)))))


def gelu_slope(h):
    sq = h * h
    t = jnp.tanh(ROOT * (h + CUBE * (sq * h)))
    return 0.5 * (1.0 + t) + (0.5 * h) * (1.0 - t * t) * (ROOT * (1.0 + (3.0 * CUBE) * sq))


def remote(src, dst, send, recv, where):
    return pltpu.make_async_remote_copy(src_ref=src, dst_ref=dst, send_sem=send, recv_sem=recv, device_id=where, device_id_type=MESH)


def signal(peer):
    pl.semaphore_signal(pltpu.get_barrier_semaphore(), inc=1, device_id=peer, device_id_type=MESH)


class Plane:
    def __init__(self):
        self.tp = lax.axis_index('tp')
        self.y = lax.rem(self.tp, SIDE)
        self.z = self.tp // SIDE

    def at(self, dy, dz):
        return lax.rem(self.z + dz + SIDE, SIDE) * SIDE + lax.rem(self.y + dy + SIDE, SIDE)

    def blk(self, half, df, ds):
        return self.at(df, ds) if half == 0 else self.at(ds, df)

    def near(self):
        return [{'tp': self.at(1, 0)}, {'tp': self.at(-1, 0)}, {'tp': self.at(0, 1)}, {'tp': self.at(0, -1)}]

    def rings(self):
        return [{'tp': self.at(d, 0)} for d in (1, 2, 3)] + [{'tp': self.at(0, d)} for d in (1, 2, 3)]


HOPS = (0, -1, 1, 2)
SLOTS = 20


def plane_gather(plane, bufs, send_sem, recv_sem, lo, on_block):
    def msg(a, half, slot, df, ds, part, to):
        buf, base, count = bufs[a]
        size = count // 2
        start = base + half * size
        if part is not None:
            size = size // 2
            start = start + part * size
        ref = buf.at[plane.blk(half, df, ds), pl.ds(start, size)]
        k = (a * 2 + half) * SLOTS + slot
        return remote(ref, ref, send_sem.at[k], recv_sem.at[k], {'tp': plane.blk(half, *to)})

    def f(a, half, slot, sending):
        if slot == 0:
            return msg(a, half, 0, 0 if sending else -1, 0, None, (1, 0))
        if slot == 1:
            return msg(a, half, 1, 0 if sending else 1, 0, None, (-1, 0))
        if slot == 2:
            return msg(a, half, 2, -1 if sending else 2, 0, 0, (1, 0))
        return msg(a, half, 3, 1 if sending else 2, 0, 1, (-1, 0))

    def s(a, half, j, k, sending):
        df = HOPS[j]
        slot = 4 + 4 * j + k
        if k == 0:
            return msg(a, half, slot, df, 0 if sending else -1, None, (0, 1))
        if k == 1:
            return msg(a, half, slot, df, 0 if sending else 1, None, (0, -1))
        if k == 2:
            return msg(a, half, slot, df, -1 if sending else 2, 0, (0, 1))
        return msg(a, half, slot, df, 1 if sending else 2, 1, (0, -1))

    pairs = [(a, half) for a in range(len(bufs)) for half in (0, 1)]
    for a, half in pairs:
        for slot in (0, 1):
            f(a, half, slot, True).start()
        for k in (0, 1):
            s(a, half, 0, k, True).start()
        on_block(a, half, 0, 0)
    for a, half in pairs:
        for slot, j in ((0, 1), (1, 2)):
            f(a, half, slot, False).wait_recv()
            f(a, half, slot + 2, True).start()
            for k in (0, 1):
                s(a, half, j, k, True).start()
            on_block(a, half, j, 0)
    for a, half in pairs:
        for k in (0, 1):
            s(a, half, 0, k, False).wait_recv()
            s(a, half, 0, k + 2, True).start()
            on_block(a, half, 0, k + 1)
    for a, half in pairs:
        f(a, half, 2, False).wait_recv()
        f(a, half, 3, False).wait_recv()
        for k in (0, 1):
            s(a, half, 3, k, True).start()
        on_block(a, half, 3, 0)
    for j in (1, 2, 3):
        for a, half in pairs:
            for k in (0, 1):
                s(a, half, j, k, False).wait_recv()
                s(a, half, j, k + 2, True).start()
                on_block(a, half, j, k + 1)
    for j in range(4):
        for a, half in pairs:
            s(a, half, j, 2, False).wait_recv()
            s(a, half, j, 3, False).wait_recv()
            on_block(a, half, j, 3)

    def finish():
        for a, half in pairs:
            for slot in range(4):
                f(a, half, slot, True).wait_send()
            for j in range(4):
                for k in range(4):
                    s(a, half, j, k, True).wait_send()

    return finish


def local(src, dst, sem):
    return pltpu.make_async_copy(src, dst, sem)


def forward_kernel(last, x_first, w_one, w_two, x_out, y_out, slope_ref, one_out, two_out, ones, twos, x_buf, y_buf, a_buf, send_sem, recv_sem, hop_sem, loc_sem):
    plane = Plane()
    stage = lax.axis_index('pp')
    tp = plane.tp
    own_one = local(w_one, ones.at[tp], loc_sem.at[0])
    own_two = local(w_two, twos.at[tp], loc_sem.at[1])
    own_one.start()
    own_two.start()
    after = {'pp': lax.rem(stage + 1, last + 1)}
    before = {'pp': lax.rem(stage + last, last + 1)}
    peers = plane.near() + [after, before]
    for peer in peers:
        signal(peer)
    own_one.wait()
    own_two.wait()
    pl.semaphore_wait(pltpu.get_barrier_semaphore(), len(peers))
    finish = plane_gather(plane, [(ones, 0, ones.shape[1]), (twos, 0, twos.shape[1])], send_sem, recv_sem, 0, lambda *_: None)
    save_one = local(ones, one_out, loc_sem.at[0])
    save_two = local(twos, two_out, loc_sem.at[1])
    save_one.start()
    save_two.start()
    hop = remote(y_buf, x_buf, hop_sem.at[0], hop_sem.at[1], after)

    @pl.when(stage == 0)
    def _():
        x_buf[...] = x_first[...]

    @pl.when(stage > 0)
    def _():
        hop.wait_recv()

    x_act = x_buf[...]
    blocks, _, cols = ones.shape
    for k in range(blocks):
        hidden = jnp.dot(x_act, ones[k], preferred_element_type=F32)
        slope_ref[k] = hidden
        a_buf[:, k * cols:(k + 1) * cols] = gelu(hidden).astype(BF16)
    gate = a_buf[...]
    wide = x_act.shape[1]
    for n in range(0, wide, 256):
        branch = jnp.dot(gate, twos[:, :, n:n + 256].reshape(blocks * cols, 256), preferred_element_type=F32)
        y_buf[:, n:n + 256] = (x_buf[:, n:n + 256].astype(F32) + branch).astype(BF16)

    @pl.when(stage < last)
    def _():
        hop.start()

    y_out[...] = y_buf[...]
    x_out[...] = x_buf[...]
    for k in range(blocks):
        slope_ref[k] = gelu_slope(slope_ref[k])
    finish()
    save_one.wait()
    save_two.wait()

    @pl.when(stage < last)
    def _():
        hop.wait_send()


def backward_kernel(last, g_top, slope_ref, one_all, two_all, dy_out, dx_out, ones, twos, dy_buf, dx_buf, d_buf, hop_sem, one_sem, two_sem):
    stage = lax.axis_index('pp')
    blocks, _, cols = one_all.shape
    loads_two = [local(two_all.at[k], twos.at[k], two_sem.at[k]) for k in range(blocks)]
    loads_one = [local(one_all.at[k], ones.at[:, pl.ds(k * cols, cols)], one_sem.at[k]) for k in range(blocks)]
    for load in loads_two + loads_one:
        load.start()
    after = {'pp': lax.rem(stage + 1, last + 1)}
    before = {'pp': lax.rem(stage + last, last + 1)}
    signal(after)
    signal(before)
    pl.semaphore_wait(pltpu.get_barrier_semaphore(), 2)
    hop = remote(dx_buf, dy_buf, hop_sem.at[0], hop_sem.at[1], before)
    for load in loads_two:
        load.wait()

    @pl.when(stage == last)
    def _():
        dy_buf[...] = g_top[...]

    @pl.when(stage < last)
    def _():
        hop.wait_recv()

    grad_y = dy_buf[...]
    for k in range(blocks):
        grad_gate = contract(grad_y, twos[k], 1, 1)
        d_buf[:, k * cols:(k + 1) * cols] = (slope_ref[k] * grad_gate).astype(BF16)
    for load in loads_one:
        load.wait()
    grad_hidden = d_buf[...]
    for n in range(0, grad_y.shape[1], 256):
        back = contract(grad_hidden, ones[n:n + 256, :], 1, 1)
        dx_buf[:, n:n + 256] = (dy_buf[:, n:n + 256].astype(F32) + back).astype(BF16)

    @pl.when(stage > 0)
    def _():
        hop.start()

    dy_out[...] = dy_buf[...]
    dx_out[...] = dx_buf[...]

    @pl.when(stage > 0)
    def _():
        hop.wait_send()


def spread_kernel(source, stages, y_ref, out, line_send, line_recv, send_sem, recv_sem, die_send, die_recv):
    plane = Plane()
    stage = lax.axis_index('pp')
    core = lax.rem(stage, 2)
    mate = {'pp': stage + 1 - 2 * core}
    tp = plane.tp
    rows = y_ref.shape[0] // 2
    lo = pl.multiple_of(core * rows, rows)
    others = [p for p in range(stages) if p != source]
    near = plane.near()
    for peer in near:
        signal(peer)
    twin = source ^ 1

    @pl.when(stage == source)
    def _():
        for p in others:
            signal({'pp': p})

    @pl.when(stage != source)
    def _():
        signal({'pp': source})

    @pl.when((stage != source) & (stage != twin))
    def _():
        signal(mate)

    extra = jnp.where(stage == source, len(others), jnp.where(stage == twin, 1, 2))
    pl.semaphore_wait(pltpu.get_barrier_semaphore(), len(near) + extra)

    def line(p):
        part = pl.ds((p % 2) * rows, rows)
        return remote(y_ref.at[part], out.at[tp, part], line_send.at[p], line_recv, {'pp': p})

    @pl.when(stage == source)
    def _():
        for p in others:
            line(p).start()
        out[tp, pl.ds(lo, rows)] = y_ref[pl.ds(lo, rows)]

    @pl.when(stage != source)
    def _():
        mine = out.at[tp, pl.ds(lo, rows)]
        remote(mine, mine, line_recv, line_recv, mate).wait_recv()

    half_rows = rows // 2

    def die(half, j, k, other):
        df = HOPS[j]
        ds = (0, -1, 1, 2)[k]
        start = (pl.multiple_of((1 - core) * rows, rows) if other else lo) + half * half_rows
        ref = out.at[plane.blk(half, df, ds), pl.ds(start, half_rows)]
        n = half * 16 + j * 4 + k
        return remote(ref, ref, die_send.at[n], die_recv.at[n], mate)

    finish = plane_gather(plane, [(out, lo, rows)], send_sem, recv_sem, lo, lambda a, half, j, k: die(half, j, k, False).start())
    for half in (0, 1):
        for j in range(4):
            for k in range(4):
                die(half, j, k, True).wait_recv()
    for half in (0, 1):
        for j in range(4):
            for k in range(4):
                die(half, j, k, False).wait_send()
    finish()

    @pl.when(stage == source)
    def _():
        for p in others:
            line(p).wait_send()


def share_kernel(stats, out, send_sem, recv_sem):
    tp = lax.axis_index('tp')
    size = out.shape[0]
    for d in range(1, size):
        signal({'tp': lax.rem(tp + d, size)})
    out[tp] = stats[...]
    pl.semaphore_wait(pltpu.get_barrier_semaphore(), size - 1)

    def msg(d, block):
        return remote(stats, out.at[block], send_sem.at[d], recv_sem.at[d], {'tp': lax.rem(tp + d, size)})

    for d in range(1, size):
        msg(d, tp).start()
    for d in range(1, size):
        msg(d, lax.rem(tp + size - d, size)).wait_recv()
    for d in range(1, size):
        msg(d, tp).wait_send()


def reduce_kernel(target, stages, head, parts, own_x, out, got_one, sum_one, got_two, piece, one_send, one_recv, two_send, two_recv, line_send, line_recv):
    plane = Plane()
    stage = lax.axis_index('pp')
    ring = plane.rings()
    others = [p for p in range(stages) if p != target]
    for peer in ring:
        signal(peer)

    @pl.when(stage == target)
    def _():
        for p in others:
            signal({'pp': p})
        pl.semaphore_wait(pltpu.get_barrier_semaphore(), len(ring) + len(others))

    @pl.when(stage != target)
    def _():
        signal({'pp': target})
        pl.semaphore_wait(pltpu.get_barrier_semaphore(), len(ring) + 1)

    width = parts.shape[3]
    half_cols = width // 2
    y, z = plane.y, plane.z

    def cols(half):
        return pl.ds(half * half_cols, half_cols)

    def row(half, index):
        return parts.at[:, index, :, cols(half)] if half == 0 else parts.at[index, :, :, cols(half)]

    def first(half, d):
        dest = lax.rem((y if half == 0 else z) + d, SIDE)
        n = half * 3 + d - 1
        return remote(row(half, dest), got_one.at[n], one_send.at[n], one_recv.at[n], {'tp': plane.blk(half, d, 0)})

    def second(half, d):
        dest = lax.rem((z if half == 0 else y) + d, SIDE)
        n = half * 3 + d - 1
        return remote(sum_one.at[half, dest], got_two.at[n], two_send.at[n], two_recv.at[n], {'tp': plane.blk(half, 0, d)})

    for d in (2, 1, 3):
        for half in (0, 1):
            first(half, d).start()
    for half in (0, 1):
        total = row(half, y if half == 0 else z)[...].astype(F32)
        for d in (1, 3, 2):
            first(half, d).wait_recv()
            total = total + got_one[half * 3 + d - 1].astype(F32)
        sum_one[half] = total.astype(sum_one.dtype)
        for d in (2, 1, 3):
            second(half, d).start()
    sums = []
    for half in (0, 1):
        total = sum_one[half, z if half == 0 else y].astype(F32)
        for d in (1, 3, 2):
            second(half, d).wait_recv()
            total = total + got_two[half * 3 + d - 1].astype(F32)
        sums.append(total)
    if head:
        x_wide = own_x[...].astype(F32)
        inv_rms = lax.rsqrt(jnp.mean(x_wide * x_wide, axis=-1, keepdims=True) + NORM_EPS)
        normed = x_wide * inv_rms
        mean = (jnp.sum(normed[:, :half_cols] * sums[0], axis=-1, keepdims=True) + jnp.sum(normed[:, half_cols:] * sums[1], axis=-1, keepdims=True)) / width
        sums = [inv_rms * (sums[h] - normed[:, h * half_cols:(h + 1) * half_cols] * mean) for h in (0, 1)]
    for half in (0, 1):
        piece[:, half * half_cols:(half + 1) * half_cols] = sums[half].astype(BF16)

    def line(p):
        return remote(piece, out.at[p], line_send, line_recv.at[p], {'pp': target})

    @pl.when(stage != target)
    def _():
        line(stage).start()

    @pl.when(stage == target)
    def _():
        out[target] = piece[...]
        for p in others:
            line(p).wait_recv()

    for half in (0, 1):
        for d in (1, 2, 3):
            first(half, d).wait_send()
            second(half, d).wait_send()

    @pl.when(stage != target)
    def _():
        line(stage).wait_send()


def collect_kernel(x_ref, dy_ref, x_all, dy_all, send_sem, recv_sem):
    plane = Plane()
    near = plane.near()
    for peer in near:
        signal(peer)
    x_all[plane.tp] = x_ref[...]
    dy_all[plane.tp] = dy_ref[...]
    pl.semaphore_wait(pltpu.get_barrier_semaphore(), len(near))
    plane_gather(plane, [(x_all, 0, x_all.shape[1]), (dy_all, 0, dy_all.shape[1])], send_sem, recv_sem, 0, lambda *_: None)()


def vmem():
    return pl.BlockSpec(memory_space=pltpu.VMEM)


def anywhere():
    return pl.BlockSpec(memory_space=pl.ANY)


def params(cid):
    return pltpu.CompilerParams(collective_id=cid, has_side_effects=True, vmem_limit_bytes=VMEM_LIMIT)


DMA = pltpu.SemaphoreType.DMA


def solution(mesh):
    pp_size = mesh.shape['pp']
    tp_size = mesh.shape['tp']
    last = pp_size - 1

    def device_fn(tokens, labels, emb_table, w_in, w_out):
        num_tokens = tokens.shape[0] * tokens.shape[1]
        vocab_rows, width = emb_table.shape
        w_one, w_two = w_in[0], w_out[0]
        cols = w_one.shape[1]
        stage = lax.axis_index('pp')
        tp_idx = lax.axis_index('tp')
        base = tp_idx * vocab_rows
        unit = num_tokens // (pp_size * tp_size)
        block = pp_size * unit
        shape = jax.ShapeDtypeStruct

        def reorder(ids):
            return ids.reshape(pp_size, tp_size, unit).transpose(1, 0, 2).reshape(num_tokens)

        def my_part(arr):
            return lax.dynamic_index_in_dim(arr.reshape(tp_size, pp_size, unit, arr.shape[-1]), stage, 1, keepdims=False)

        tok_local = reorder(tokens) - base
        lab_local = reorder(labels) - base
        row_ids = jnp.arange(vocab_rows, dtype=jnp.int32)

        def reduce_call(parts, own_x, target, head, cid):
            dtype = parts.dtype
            half = width // 2
            return pl.pallas_call(
                functools.partial(reduce_kernel, target, pp_size, head),
                out_shape=shape((pp_size, unit, width), BF16),
                in_specs=[vmem(), vmem()], out_specs=vmem(),
                scratch_shapes=[pltpu.VMEM((6, SIDE, unit, half), dtype), pltpu.VMEM((2, SIDE, unit, half), dtype), pltpu.VMEM((6, unit, half), dtype),
                                pltpu.VMEM((unit, width), BF16), DMA((6,)), DMA((6,)), DMA((6,)), DMA((6,)), DMA, DMA((pp_size,))],
                compiler_params=params(cid), name='reduce_head' if head else 'reduce_lookup',
            )(parts.reshape(SIDE, SIDE, unit, width), own_x).reshape(block, width)

        def spread_call(arr, source, cid):
            return pl.pallas_call(
                functools.partial(spread_kernel, source, pp_size),
                out_shape=shape((tp_size, block, width), BF16),
                in_specs=[vmem()], out_specs=vmem(),
                scratch_shapes=[DMA((pp_size,)), DMA, DMA((2 * SLOTS,)), DMA((2 * SLOTS,)), DMA((32,)), DMA((32,))],
                compiler_params=params(cid), name=f'spread_{source}',
            )(arr).reshape(num_tokens, width)

        tok_part = my_part(tok_local[:, None]).reshape(tp_size * unit)
        owned = (tok_part >= 0) & (tok_part < vocab_rows)
        looked = jnp.take(emb_table, jnp.clip(tok_part, 0, vocab_rows - 1), axis=0)
        looked = jnp.where(owned[:, None], looked, jnp.zeros_like(looked))
        x_first = reduce_call(looked, looked[:unit], 0, False, 1)

        x_mine, y_act, slope, ones, twos = pl.pallas_call(
            functools.partial(forward_kernel, last),
            out_shape=(shape((block, width), BF16), shape((block, width), BF16), shape((tp_size, block, cols), F32),
                       shape((tp_size, width, cols), BF16), shape((tp_size, cols, width), BF16)),
            in_specs=[vmem(), anywhere(), anywhere()],
            out_specs=(vmem(), vmem(), vmem(), anywhere(), anywhere()),
            scratch_shapes=[pltpu.VMEM((tp_size, width, cols), BF16), pltpu.VMEM((tp_size, cols, width), BF16), pltpu.VMEM((block, width), BF16),
                            pltpu.VMEM((block, width), BF16), pltpu.VMEM((block, tp_size * cols), BF16),
                            DMA((4 * SLOTS,)), DMA((4 * SLOTS,)), DMA((2,)), DMA((2,))],
            compiler_params=params(2), name='forward_chain',
        )(x_first, w_one, w_two)

        top = spread_call(y_act, last, 3)
        x_wide = top.astype(F32)
        inv_rms = lax.rsqrt(jnp.mean(x_wide * x_wide, axis=-1, keepdims=True) + NORM_EPS)
        normed_b = (x_wide * inv_rms).astype(BF16)
        hit = lab_local[:, None] == row_ids[None, :]
        logits = contract(normed_b, emb_table, 1, 1)
        local_lse = jax.nn.logsumexp(logits, axis=-1)
        local_target = jnp.sum(jnp.where(hit, logits, 0.0), axis=-1)
        stats = jnp.concatenate([local_lse.reshape(-1, 128), local_target.reshape(-1, 128)], axis=0)
        shared = pl.pallas_call(
            share_kernel, out_shape=shape((tp_size,) + stats.shape, F32), in_specs=[vmem()], out_specs=vmem(),
            scratch_shapes=[DMA((tp_size,)), DMA((tp_size,))], compiler_params=params(4), name='share_stats',
        )(stats).reshape(tp_size, 2, num_tokens)
        log_norm = jax.nn.logsumexp(shared[:, 0], axis=0)
        target_logit = jnp.sum(shared[:, 1], axis=0)
        mean_loss = jnp.sum(log_norm - target_logit) / num_tokens
        grad_logits = (jnp.exp(logits - log_norm[:, None]) - hit.astype(F32)).astype(BF16)
        dn_part = contract(my_part(grad_logits).reshape(tp_size * unit, vocab_rows), emb_table, 1, 0)
        own_x = lax.dynamic_slice_in_dim(top, tp_idx * block + stage * unit, unit, 0)
        g_act = reduce_call(dn_part, own_x, last, True, 5)

        dy_mine, grad_x = pl.pallas_call(
            functools.partial(backward_kernel, last),
            out_shape=(shape((block, width), BF16), shape((block, width), BF16)),
            in_specs=[vmem(), vmem(), anywhere(), anywhere()], out_specs=(vmem(), vmem()),
            scratch_shapes=[pltpu.VMEM((width, tp_size * cols), BF16), pltpu.VMEM((tp_size, cols, width), BF16), pltpu.VMEM((block, width), BF16),
                            pltpu.VMEM((block, width), BF16), pltpu.VMEM((block, tp_size * cols), BF16), DMA((2,)), DMA((tp_size,)), DMA((tp_size,))],
            compiler_params=params(6), name='backward_chain',
        )(g_act, slope, ones, twos)

        x_all, dy_all = pl.pallas_call(
            collect_kernel, out_shape=(shape((tp_size, block, width), BF16),) * 2, in_specs=[vmem(), vmem()], out_specs=(vmem(), vmem()),
            scratch_shapes=[DMA((4 * SLOTS,)), DMA((4 * SLOTS,))], compiler_params=params(7), name='collect',
        )(x_mine, dy_mine)
        x_all, dy_all = x_all.reshape(num_tokens, width), dy_all.reshape(num_tokens, width)
        hidden_all = jnp.dot(x_all, w_one, preferred_element_type=F32)
        dh_all = (gelu_slope(hidden_all) * contract(dy_all, w_two, 1, 1)).astype(BF16)
        grad_two = contract(gelu(hidden_all).astype(BF16), dy_all, 0, 0)
        grad_one = contract(x_all, dh_all, 0, 0)

        dx_first = spread_call(grad_x, 0, 8)
        one_hot = (tok_local[:, None] == row_ids[None, :]).astype(BF16)
        grad_table = contract(grad_logits, normed_b, 0, 0) + contract(one_hot, dx_first, 0, 0)
        return mean_loss.reshape(1), grad_one[None], grad_two[None], grad_table

    return jax.shard_map(device_fn, mesh=mesh, in_specs=(P('dp', None), P('dp', None), P('tp', None), P('pp', None, 'tp'), P('pp', 'tp', None)), out_specs=(P('dp'), P(('dp', 'pp'), None, 'tp'), P(('dp', 'pp'), 'tp', None), P(('dp', 'tp'), None)), check_vma=False)
```

```python
import functools

import jax
import jax.numpy as jnp
from jax import lax
from jax.experimental import pallas as pl
from jax.experimental.pallas import tpu as pltpu
from jax.sharding import PartitionSpec as P

NORM_EPS = 1e-6
SIDE = 4
MESH = pl.DeviceIdType.MESH
F32 = jnp.float32
BF16 = jnp.bfloat16
VMEM_LIMIT = 63 * 1024 * 1024
CUBE = 0.044715
ROOT = 0.7978845608028654


def contract(lhs, rhs, lhs_dim, rhs_dim):
    return lax.dot_general(lhs, rhs, (((lhs_dim,), (rhs_dim,)), ((), ())), preferred_element_type=F32)


def gelu(h):
    return h * (0.5 * (1.0 + jnp.tanh(ROOT * (h + CUBE * (h * h * h)))))


def gelu_slope(h):
    sq = h * h
    t = jnp.tanh(ROOT * (h + CUBE * (sq * h)))
    return 0.5 * (1.0 + t) + (0.5 * h) * (1.0 - t * t) * (ROOT * (1.0 + (3.0 * CUBE) * sq))


def remote(src, dst, send, recv, where):
    return pltpu.make_async_remote_copy(src_ref=src, dst_ref=dst, send_sem=send, recv_sem=recv, device_id=where, device_id_type=MESH)


def signal(peer):
    pl.semaphore_signal(pltpu.get_barrier_semaphore(), inc=1, device_id=peer, device_id_type=MESH)


class Plane:
    def __init__(self):
        self.tp = lax.axis_index('tp')
        self.y = lax.rem(self.tp, SIDE)
        self.z = self.tp // SIDE

    def at(self, dy, dz):
        return lax.rem(self.z + dz + SIDE, SIDE) * SIDE + lax.rem(self.y + dy + SIDE, SIDE)

    def blk(self, half, df, ds):
        return self.at(df, ds) if half == 0 else self.at(ds, df)

    def near(self):
        return [{'tp': self.at(1, 0)}, {'tp': self.at(-1, 0)}, {'tp': self.at(0, 1)}, {'tp': self.at(0, -1)}]

    def rings(self):
        return [{'tp': self.at(d, 0)} for d in (1, 2, 3)] + [{'tp': self.at(0, d)} for d in (1, 2, 3)]


HOPS = (0, -1, 1, 2)
WALK = ((0, -1, None, 1), (0, 1, None, -1), (-1, 2, 0, 1), (1, 2, 1, -1))
BOTH = (0, 1)
SLOTS = 20


def plane_gather(plane, bufs, send_sem, recv_sem, on_block=lambda *_: None):
    def msg(a, half, slot, block, part, to):
        buf, start, size = bufs[a]
        size = size // 2
        start = start + half * size
        if part is not None:
            size = size // 2
            start = start + part * size
        ref = buf.at[plane.blk(half, *block), pl.ds(start, size)]
        k = (a * 2 + half) * SLOTS + slot
        return remote(ref, ref, send_sem.at[k], recv_sem.at[k], {'tp': plane.blk(half, *to)})

    def f(a, half, k, end):
        step = WALK[k]
        return msg(a, half, k, (step[end], 0), step[2], (step[3], 0))

    def s(a, half, j, k, end):
        step = WALK[k]
        return msg(a, half, SIDE * (j + 1) + k, (HOPS[j], step[end]), step[2], (0, step[3]))

    send, recv = BOTH
    pairs = [(a, half) for a in range(len(bufs)) for half in BOTH]

    def across(a, half, j):
        for k in BOTH:
            s(a, half, j, k, send).start()
        on_block(a, half, j, 0)

    def onward(a, half, j):
        for k in BOTH:
            s(a, half, j, k, recv).wait_recv()
            s(a, half, j, k + 2, send).start()
            on_block(a, half, j, k + 1)

    for pair in pairs:
        for k in BOTH:
            f(*pair, k, send).start()
        across(*pair, 0)
    yield
    for pair in pairs:
        for k in BOTH:
            f(*pair, k, recv).wait_recv()
            f(*pair, k + 2, send).start()
            across(*pair, k + 1)
    yield
    for pair in pairs:
        onward(*pair, 0)
    yield
    for pair in pairs:
        for k in BOTH:
            f(*pair, k + 2, recv).wait_recv()
        across(*pair, SIDE - 1)
    yield
    for j in range(1, SIDE):
        for pair in pairs:
            onward(*pair, j)
        yield
    for j in range(SIDE):
        for pair in pairs:
            for k in BOTH:
                s(*pair, j, k + 2, recv).wait_recv()
            on_block(*pair, j, SIDE - 1)
    for pair in pairs:
        for k in range(SIDE):
            f(*pair, k, send).wait_send()
            for j in range(SIDE):
                s(*pair, j, k, send).wait_send()


def drain(steps):
    for _ in steps:
        pass


def local(src, dst, sem):
    return pltpu.make_async_copy(src, dst, sem)


class Reduce:
    def __init__(self, plane, parts, got_one, sum_one, got_two, one_send, one_recv, two_send, two_recv):
        self.plane, self.parts, self.got_one, self.sum_one, self.got_two = plane, parts, got_one, sum_one, got_two
        self.one_send, self.one_recv, self.two_send, self.two_recv = one_send, one_recv, two_send, two_recv

    def row(self, half, index):
        size = self.parts.shape[3] // 2
        cols = pl.ds(half * size, size)
        return self.parts.at[:, index, :, cols] if half == 0 else self.parts.at[index, :, :, cols]

    def here(self, half):
        return (self.plane.y, self.plane.z) if half == 0 else (self.plane.z, self.plane.y)

    def first(self, half, d):
        n = half * 3 + d - 1
        dest = lax.rem(self.here(half)[0] + d, SIDE)
        return remote(self.row(half, dest), self.got_one.at[n], self.one_send.at[n], self.one_recv.at[n], {'tp': self.plane.blk(half, d, 0)})

    def second(self, half, d):
        n = half * 3 + d - 1
        dest = lax.rem(self.here(half)[1] + d, SIDE)
        return remote(self.sum_one.at[half, dest], self.got_two.at[n], self.two_send.at[n], self.two_recv.at[n], {'tp': self.plane.blk(half, 0, d)})

    def begin(self):
        for d in (2, 1, 3):
            for half in BOTH:
                self.first(half, d).start()

    def middle(self):
        for half in BOTH:
            total = self.row(half, self.here(half)[0])[:].astype(F32)
            for d in (1, 3, 2):
                self.first(half, d).wait_recv()
                total = total + self.got_one[half * 3 + d - 1].astype(F32)
            self.sum_one[half] = total.astype(self.sum_one.dtype)
            for d in (2, 1, 3):
                self.second(half, d).start()

    def end(self):
        sums = []
        for half in BOTH:
            total = self.sum_one[half, self.here(half)[1]].astype(F32)
            for d in (1, 3, 2):
                self.second(half, d).wait_recv()
                total = total + self.got_two[half * 3 + d - 1].astype(F32)
            sums.append(total)
        return sums

    def close(self):
        for half in BOTH:
            for d in (1, 2, 3):
                self.first(half, d).wait_send()
                self.second(half, d).wait_send()


def greet(peers):
    for peer in peers:
        signal(peer)
    pl.semaphore_wait(pltpu.get_barrier_semaphore(), len(peers))


def forward_kernel(last, swap, ids, emb, w_one, w_two, x_out, y_out, slope_ref, one_out, two_out, ones, twos, one_t, two_t, table, hot, parts,
                   got_one, sum_one, got_two, piece, x_buf, y_buf, a_buf, send_sem, recv_sem, one_send, one_recv, two_send, two_recv, line_send, line_recv, hop_sem, loc_sem):
    plane = Plane()
    stage = lax.axis_index('pp')
    tp = plane.tp
    stages = last + 1
    own_one = local(w_one, ones.at[tp], loc_sem.at[0])
    own_two = local(w_two, twos.at[tp], loc_sem.at[1])
    load = local(emb, table, loc_sem.at[2])
    own_one.start()
    own_two.start()
    load.start()
    for peer in plane.rings() + [{'pp': lax.rem(stage + d, stages)} for d in range(1, stages)]:
        signal(peer)
    own_one.wait()
    own_two.wait()
    pl.semaphore_wait(pltpu.get_barrier_semaphore(), 6 + last)
    gather = plane_gather(plane, [(ones, 0, ones.shape[1]), (twos, 0, twos.shape[1])], send_sem, recv_sem)
    next(gather)

    rows, width = table.shape
    group, full = hot.shape
    load.wait()
    row_ids = ids[:]
    lanes = lax.broadcasted_iota(jnp.int32, (group, full), 1)
    hot[:] = jnp.where(row_ids == lanes, 1.0, 0.0).astype(BF16)
    tail = jnp.where(row_ids == full + lax.broadcasted_iota(jnp.int32, (group, rows - full), 1), 1.0, 0.0).astype(BF16)
    for n in range(0, width, 256):
        picked = jnp.dot(hot[:], table[:full, n:n + 256], preferred_element_type=F32) + jnp.dot(tail, table[full:, n:n + 256], preferred_element_type=F32)
        parts[:, :, :, n:n + 256] = picked.astype(BF16).reshape(parts.shape[:3] + (256,))
    red = Reduce(plane, parts, got_one, sum_one, got_two, one_send, one_recv, two_send, two_recv)
    red.begin()
    next(gather)
    red.middle()
    next(gather)
    unit = piece.shape[0]
    for half, total in enumerate(red.end()):
        piece[:, half * (width // 2):(half + 1) * (width // 2)] = total.astype(BF16)

    def line(p):
        return remote(piece, x_buf.at[pl.ds(pl.multiple_of(p * unit, unit), unit)], line_send, line_recv.at[p], {'pp': 0})

    @pl.when(stage != 0)
    def _():
        line(stage).start()

    @pl.when(stage == 0)
    def _():
        x_buf[:unit] = piece[:]

    drain(gather)

    blocks, _, cols = ones.shape
    save_one = local(one_t, one_out, loc_sem.at[3])
    save_two = local(two_t, two_out, loc_sem.at[4])

    def turn():
        @pl.loop(0, blocks)
        def _(k):
            one_t[k] = ones[k].T
            two_t[k] = twos[k].T

        save_one.start()
        save_two.start()

    pl.when(stage >= swap)(turn)
    hop = remote(y_buf, x_buf, hop_sem.at[0], hop_sem.at[1], {'pp': lax.rem(stage + 1, stages)})

    @pl.when(stage == 0)
    def _():
        for p in range(1, stages):
            line(p).wait_recv()

    @pl.when(stage > 0)
    def _():
        hop.wait_recv()

    x_act = x_buf[:]
    for k in range(blocks):
        hidden = jnp.dot(x_act, ones[k], preferred_element_type=F32)
        slope_ref[k] = hidden
        a_buf[:, k * cols:(k + 1) * cols] = gelu(hidden).astype(BF16)
    gate = a_buf[:]
    for n in range(0, width, 256):
        branch = jnp.dot(gate, twos[:, :, n:n + 256].reshape(blocks * cols, 256), preferred_element_type=F32)
        y_buf[:, n:n + 256] = (x_buf[:, n:n + 256].astype(F32) + branch).astype(BF16)

    @pl.when(stage < last)
    def _():
        hop.start()

    y_out[:] = y_buf[:]
    x_out[:] = x_buf[:]
    for k in range(blocks):
        slope_ref[k] = gelu_slope(slope_ref[k])
    pl.when(stage < swap)(turn)
    red.close()
    save_one.wait()
    save_two.wait()

    @pl.when(stage != 0)
    def _():
        line(stage).wait_send()

    @pl.when(stage < last)
    def _():
        hop.wait_send()


def norm_of(x):
    wide = x.astype(F32)
    inv_rms = lax.rsqrt(jnp.mean(wide * wide, axis=-1, keepdims=True) + NORM_EPS)
    return inv_rms, wide * inv_rms


def spread_kernel(source, stages, head, y_ref, out, *refs):
    if head:
        own_out, n_buf, own_send, own_recv, line_send, line_recv, send_sem, recv_sem, die_send, die_recv = refs
    else:
        line_send, line_recv, send_sem, recv_sem, die_send, die_recv = refs
    plane = Plane()
    stage = lax.axis_index('pp')
    core = lax.rem(stage, 2)
    mate = {'pp': stage + 1 - 2 * core}
    tp = plane.tp
    rows = y_ref.shape[0] // 2
    lo = pl.multiple_of(core * rows, rows)
    others = [p for p in range(stages) if p != source]
    near = plane.near()
    for peer in near:
        signal(peer)
    twin = source ^ 1

    @pl.when(stage == source)
    def _():
        for p in others:
            signal({'pp': p})

    @pl.when(stage != source)
    def _():
        signal({'pp': source})

    @pl.when((stage != source) & (stage != twin))
    def _():
        signal(mate)

    if head:
        n_buf[:] = norm_of(y_ref[:])[1].astype(BF16)
        src = n_buf
        unit = own_out.shape[0]
    else:
        src = y_ref
    extra = jnp.where(stage == source, len(others), jnp.where(stage == twin, 1, 2))
    pl.semaphore_wait(pltpu.get_barrier_semaphore(), len(near) + extra)

    def line(p):
        part = pl.ds((p % 2) * rows, rows)
        return remote(src.at[part], out.at[tp, part], line_send.at[p], line_recv, {'pp': p})

    def own(p):
        return remote(y_ref.at[pl.ds(p * unit, unit)], own_out, own_send.at[p], own_recv, {'pp': p})

    @pl.when(stage == source)
    def _():
        for p in others:
            line(p).start()
        out[tp, pl.ds(lo, rows)] = src[pl.ds(lo, rows)]
        if head:
            for p in others:
                own(p).start()
            own_out[:] = y_ref[source * unit:(source + 1) * unit]

    @pl.when(stage != source)
    def _():
        mine = out.at[tp, pl.ds(lo, rows)]
        remote(mine, mine, line_recv, line_recv, mate).wait_recv()

    half_rows = rows // 2

    def die(half, j, k, other):
        df = HOPS[j]
        ds = HOPS[k]
        start = (pl.multiple_of((1 - core) * rows, rows) if other else lo) + half * half_rows
        ref = out.at[plane.blk(half, df, ds), pl.ds(start, half_rows)]
        n = half * 16 + j * 4 + k
        return remote(ref, ref, die_send.at[n], die_recv.at[n], mate)

    drain(plane_gather(plane, [(out, lo, rows)], send_sem, recv_sem, lambda a, half, j, k: die(half, j, k, False).start()))
    for half in BOTH:
        for j in range(4):
            for k in range(4):
                die(half, j, k, True).wait_recv()
    for half in BOTH:
        for j in range(4):
            for k in range(4):
                die(half, j, k, False).wait_send()

    @pl.when(stage == source)
    def _():
        for p in others:
            line(p).wait_send()
            if head:
                own(p).wait_send()

    if head:
        @pl.when(stage != source)
        def _():
            remote(own_out, own_out, own_recv, own_recv, mate).wait_recv()


def fold(op, value):
    rows, cols = value.shape
    return op(value.reshape(rows // 8, 8, cols), axis=0)


def head_kernel(target, stages, chunk, emb, top, lab, lab_two, own_x, x_mine, loss_out, g_out, n_out, g_top, x_all,
                table, n_buf, e_buf, g_buf, peak, stat, shared, scale_ref, parts, got_one, sum_one, got_two, piece,
                send_sem, recv_sem, share_send, share_recv, one_send, one_recv, two_send, two_recv, line_send, line_recv, loc_sem):
    plane = Plane()
    stage = lax.axis_index('pp')
    tp = plane.tp
    size = shared.shape[0]
    others = [p for p in range(stages) if p != target]
    load = local(emb, table, loc_sem.at[0])
    load.start()
    for d in range(1, size):
        signal({'tp': lax.rem(tp + d, size)})

    @pl.when(stage == target)
    def _():
        for p in others:
            signal({'pp': p})

    @pl.when(stage != target)
    def _():
        signal({'pp': target})

    x_all[tp] = x_mine[:]
    group = peak.shape[1]
    unit = group // size
    for p in range(stages):
        n_buf[p * group:(p + 1) * group] = top[:, p * unit:(p + 1) * unit, :].reshape(group, top.shape[2])
    pl.semaphore_wait(pltpu.get_barrier_semaphore(), size - 1 + jnp.where(stage == target, len(others), 1))
    gather = plane_gather(plane, [(x_all, 0, x_all.shape[1])], send_sem, recv_sem)
    next(gather)
    save_n = local(n_buf, n_out, loc_sem.at[1])
    save_n.start()
    load.wait()

    rows, width = table.shape
    full = rows // chunk
    pieces = e_buf.shape[0]
    pair = e_buf.shape[2]

    def logit_chunk(b, start, count):
        logits = contract(table[pl.ds(start, count), :], n_buf[b * pair:(b + 1) * pair, :], 1, 1)
        e_buf[b, pl.ds(start, count), :] = logits
        return fold(jnp.max, logits)

    def exp_chunk(b, start, count, top_b, total, hits):
        logits = e_buf[b, pl.ds(start, count), :]
        hit = lab_two[b:b + 1, :] == start + lax.broadcasted_iota(jnp.int32, logits.shape, 0)
        e = jnp.exp(logits - top_b)
        e_buf[b, pl.ds(start, count), :] = e
        return total + fold(jnp.sum, e), hits + fold(jnp.sum, jnp.where(hit, logits, 0.0))

    top_b = None
    zero = jnp.zeros((8, pair), F32)
    for b in range(pieces + 1):
        def both(start, count, carry, b=b, top_b=top_b):
            best, total, hits = carry
            if b < pieces:
                best = jnp.maximum(best, logit_chunk(b, start, count))
            if b > 0:
                total, hits = exp_chunk(b - 1, start, count, top_b, total, hits)
            return best, total, hits

        carry = (jnp.full((8, pair), -jnp.inf, F32), zero, zero)
        carry = lax.fori_loop(0, full, lambda c, carry: both(pl.multiple_of(c * chunk, chunk), chunk, carry), carry)
        best, total, hits = both(full * chunk, rows - full * chunk, carry)
        if b > 0:
            lse = top_b + jnp.log(jnp.sum(total, axis=0, keepdims=True))
            hits = jnp.sum(hits, axis=0, keepdims=True)
            for i in range(pair // group):
                p = (b - 1) * (pair // group) + i
                stat[0, p:p + 1, :] = lse[:, i * group:(i + 1) * group]
                stat[1, p:p + 1, :] = hits[:, i * group:(i + 1) * group]
                peak[p:p + 1, :] = top_b[:, i * group:(i + 1) * group]
        if b < pieces:
            top_b = jnp.max(best, axis=0, keepdims=True)
            for _ in range((1, 2, 1, 2)[b]):
                next(gather)

    def msg(d, block):
        return remote(stat, shared.at[block], share_send.at[d], share_recv.at[d], {'tp': lax.rem(tp + d, size)})

    for d in range(1, size):
        msg(d, tp).start()
    shared[tp] = stat[:]
    drain(gather)
    for d in range(1, size):
        msg(d, lax.rem(tp + size - d, size)).wait_recv()
    every = shared[:, 0]
    most = jnp.max(every, axis=0)
    log_norm = most + jnp.log(jnp.sum(jnp.exp(every - most[None]), axis=0))
    loss_out[:] = jnp.sum(log_norm - jnp.sum(shared[:, 1], axis=0), keepdims=True)
    scale_ref[:] = jnp.exp(peak[:] - log_norm)

    def grad_block(p, slot):
        b = p // (pair // group)
        col = pl.multiple_of(lax.rem(p, pair // group) * group, group)
        factor = scale_ref[pl.ds(p, 1), :]
        label = lab[pl.ds(p, 1), :]

        def part(start, count):
            e = e_buf[b, pl.ds(start, count), pl.ds(col, group)]
            hit = label == start + lax.broadcasted_iota(jnp.int32, e.shape, 0)
            g_buf[slot, pl.ds(start, count), :] = (e * factor - jnp.where(hit, 1.0, 0.0)).astype(BF16)

        @pl.loop(0, full)
        def _(c):
            part(pl.multiple_of(c * chunk, chunk), chunk)

        part(full * chunk, rows - full * chunk)

    def save(p, slot):
        return local(g_buf.at[slot], g_out.at[:, pl.ds(pl.multiple_of(p * group, group), group)], loc_sem.at[2 + slot])

    grad_block(stage, 0)
    cut = full * chunk
    for n in range(0, width, 256):
        back = contract(g_buf[0, :cut, :], table[:cut, n:n + 256], 0, 0) + contract(g_buf[0, cut:, :], table[cut:, n:n + 256], 0, 0)
        parts[:, :, :, n:n + 256] = back.reshape(parts.shape[:3] + (256,))
    red = Reduce(plane, parts, got_one, sum_one, got_two, one_send, one_recv, two_send, two_recv)
    red.begin()
    save(stage, 0).start()
    for k in range(1, stages):
        p = lax.rem(stage + k, stages)
        slot = k % 2
        if k >= 2:
            save(p, slot).wait()
        grad_block(p, slot)
        save(p, slot).start()
    red.middle()
    sums = red.end()
    inv_rms, normed = norm_of(own_x[:])
    half = width // 2
    mean = (jnp.sum(normed[:, :half] * sums[0], axis=-1, keepdims=True) + jnp.sum(normed[:, half:] * sums[1], axis=-1, keepdims=True)) / width
    for h in BOTH:
        piece[:, h * half:(h + 1) * half] = (inv_rms * (sums[h] - normed[:, h * half:(h + 1) * half] * mean)).astype(BF16)

    def line(p):
        return remote(piece, g_top.at[p], line_send, line_recv.at[p], {'pp': target})

    @pl.when(stage != target)
    def _():
        line(stage).start()

    @pl.when(stage == target)
    def _():
        g_top[target] = piece[:]
        for p in others:
            line(p).wait_recv()

    red.close()
    for d in range(1, size):
        msg(d, tp).wait_send()
    save_n.wait()
    save(stage, 0).wait()
    save(stage, 1).wait()

    @pl.when(stage != target)
    def _():
        line(stage).wait_send()


def backward_kernel(last, early, chunk, g_top, slope_ref, one_all, two_all, g_all, n_all, dx_out, dy_all, de_out,
                    ones, twos, g_buf, n_buf, de_buf, dy_buf, dx_buf, d_buf, send_sem, recv_sem, hop_sem, loc_sem):
    plane = Plane()
    stage = lax.axis_index('pp')
    blocks, cols, width = one_all.shape
    loads = [local(two_all, twos, loc_sem.at[0]), local(one_all, ones, loc_sem.at[1]), local(g_all, g_buf, loc_sem.at[2]), local(n_all, n_buf, loc_sem.at[3])]
    for load in loads:
        load.start()
    after = {'pp': lax.rem(stage + 1, last + 1)}
    before = {'pp': lax.rem(stage + last, last + 1)}
    greet(plane.near() + [after, before])
    hop = remote(dx_buf, dy_buf, hop_sem.at[0], hop_sem.at[1], before)
    save = local(de_buf, de_out, loc_sem.at[4])
    rows = de_buf.shape[0]
    full = rows // chunk

    def table_part(start, count):
        de_buf[pl.ds(start, count), :] = jnp.dot(g_buf[pl.ds(start, count), :], n_buf[:], preferred_element_type=F32)

    def table_parts(lo, hi):
        @pl.loop(lo, hi)
        def _(c):
            table_part(pl.multiple_of(c * chunk, chunk), chunk)

    @pl.when(stage <= early)
    def _():
        loads[2].wait()
        loads[3].wait()
        table_parts(0, full)
        table_part(full * chunk, rows - full * chunk)
        save.start()

    loads[0].wait()

    @pl.when(stage == last)
    def _():
        dy_buf[:] = g_top[:]

    @pl.when(stage < last)
    def _():
        hop.wait_recv()

    grad_y = dy_buf[:]
    for k in range(blocks):
        grad_gate = jnp.dot(grad_y, twos[k], preferred_element_type=F32)
        d_buf[:, k * cols:(k + 1) * cols] = (slope_ref[k] * grad_gate).astype(BF16)
    loads[1].wait()
    grad_hidden = d_buf[:]
    for n in range(0, width, 256):
        back = jnp.dot(grad_hidden, ones[:, :, n:n + 256].reshape(blocks * cols, 256), preferred_element_type=F32)
        dx_buf[:, n:n + 256] = (dy_buf[:, n:n + 256].astype(F32) + back).astype(BF16)

    @pl.when(stage > 0)
    def _():
        hop.start()

    dx_out[:] = dx_buf[:]
    dy_all[plane.tp] = dy_buf[:]

    def gather():
        return plane_gather(plane, [(dy_all, 0, dy_all.shape[1])], send_sem, recv_sem)

    @pl.when(stage <= early)
    def _():
        drain(gather())

    @pl.when(stage > early)
    def _():
        steps = gather()
        next(steps)
        loads[2].wait()
        loads[3].wait()
        for c in range(full):
            table_parts(c, c + 1)
            next(steps)
        table_part(full * chunk, rows - full * chunk)
        save.start()
        drain(steps)

    save.wait()

    @pl.when(stage > 0)
    def _():
        hop.wait_send()


def weight_kernel(x_ref, dy_ref, one_ref, two_ref, out_one, out_two):
    @pl.when(pl.program_id(0) == 0)
    def _():
        out_one[:] = jnp.zeros_like(out_one)
        out_two[:] = jnp.zeros_like(out_two)

    x_act, grad_y = x_ref[:], dy_ref[:]
    hidden = jnp.dot(x_act, one_ref[:], preferred_element_type=F32)
    grad_gate = contract(grad_y, two_ref[:], 1, 1)
    grad_hidden = (gelu_slope(hidden) * grad_gate).astype(BF16)
    out_one[:] += contract(x_act, grad_hidden, 0, 0)
    out_two[:] += contract(gelu(hidden).astype(BF16), grad_y, 0, 0)


def vmem():
    return pl.BlockSpec(memory_space=pltpu.VMEM)


def anywhere():
    return pl.BlockSpec(memory_space=pl.ANY)


def params(cid):
    return pltpu.CompilerParams(collective_id=cid, has_side_effects=True, vmem_limit_bytes=VMEM_LIMIT)


DMA = pltpu.SemaphoreType.DMA


def solution(mesh):
    pp_size = mesh.shape['pp']
    tp_size = mesh.shape['tp']
    last = pp_size - 1

    def device_fn(tokens, labels, emb_table, w_in, w_out):
        num_tokens = tokens.shape[0] * tokens.shape[1]
        vocab_rows, width = emb_table.shape
        w_one, w_two = w_in[0], w_out[0]
        cols = w_one.shape[1]
        stage = lax.axis_index('pp')
        base = lax.axis_index('tp') * vocab_rows
        unit = num_tokens // (pp_size * tp_size)
        block = pp_size * unit
        group = tp_size * unit
        half = width // 2
        chunk = 512
        pair = 2 * group
        shape = jax.ShapeDtypeStruct
        VM = pltpu.VMEM

        tok_local = tokens.reshape(num_tokens) - base
        lab_local = labels.reshape(num_tokens) - base
        ids = lax.dynamic_slice_in_dim(tok_local, stage * group, group)[:, None]

        def reduce_scratch(dtype):
            return [VM((SIDE, SIDE, unit, width), dtype), VM((6, SIDE, unit, half), dtype), VM((2, SIDE, unit, half), dtype), VM((6, unit, half), dtype), VM((unit, width), BF16)]

        reduce_sems = [DMA((6,)), DMA((6,)), DMA((6,)), DMA((6,)), DMA, DMA((pp_size,))]

        x_mine, y_act, slope, one_t, two_t = pl.pallas_call(
            functools.partial(forward_kernel, last, pp_size // 2),
            out_shape=(shape((block, width), BF16), shape((block, width), BF16), shape((tp_size, block, cols), F32),
                       shape((tp_size, cols, width), BF16), shape((tp_size, width, cols), BF16)),
            in_specs=[vmem(), anywhere(), anywhere(), anywhere()],
            out_specs=(vmem(), vmem(), vmem(), anywhere(), anywhere()),
            scratch_shapes=[VM((tp_size, width, cols), BF16), VM((tp_size, cols, width), BF16), VM((tp_size, cols, width), BF16), VM((tp_size, width, cols), BF16),
                            VM((vocab_rows, width), BF16), VM((group, vocab_rows // chunk * chunk), BF16), *reduce_scratch(BF16),
                            VM((block, width), BF16), VM((block, width), BF16), VM((block, tp_size * cols), BF16),
                            DMA((4 * SLOTS,)), DMA((4 * SLOTS,)), *reduce_sems, DMA((2,)), DMA((5,))],
            compiler_params=params(1), name='forward_chain',
        )(ids, emb_table, w_one, w_two)

        def spread_call(arr, source, head, cid):
            out = shape((tp_size, block, width), BF16)
            sems = [DMA((pp_size,)), DMA, DMA((2 * SLOTS,)), DMA((2 * SLOTS,)), DMA((32,)), DMA((32,))]
            return pl.pallas_call(
                functools.partial(spread_kernel, source, pp_size, head),
                out_shape=(out, shape((unit, width), BF16)) if head else out,
                in_specs=[vmem()], out_specs=(vmem(), vmem()) if head else vmem(),
                scratch_shapes=[VM((block, width), BF16), DMA((pp_size,)), DMA, *sems] if head else sems,
                compiler_params=params(cid), name=f'spread_{source}',
            )(arr)

        top, own_x = spread_call(y_act, last, True, 2)
        loss, g_all, n_all, g_top, x_all = pl.pallas_call(
            functools.partial(head_kernel, last, pp_size, chunk),
            out_shape=(shape((1, 1), F32), shape((vocab_rows, num_tokens), BF16), shape((num_tokens, width), BF16), shape((pp_size, unit, width), BF16), shape((tp_size, block, width), BF16)),
            in_specs=[anywhere(), vmem(), vmem(), vmem(), vmem(), vmem()],
            out_specs=(vmem(), anywhere(), anywhere(), vmem(), vmem()),
            scratch_shapes=[VM((vocab_rows, width), BF16), VM((num_tokens, width), BF16), VM((num_tokens // pair, vocab_rows, pair), F32), VM((2, vocab_rows, group), BF16),
                            VM((pp_size, group), F32), VM((2, pp_size, group), F32), VM((tp_size, 2, pp_size, group), F32), VM((pp_size, group), F32), *reduce_scratch(F32),
                            DMA((2 * SLOTS,)), DMA((2 * SLOTS,)), DMA((tp_size,)), DMA((tp_size,)), *reduce_sems, DMA((4,))],
            compiler_params=params(3), name='head',
        )(emb_table, top, lab_local.reshape(pp_size, group), lab_local.reshape(num_tokens // pair, pair), own_x, x_mine)

        grad_x, dy_all, de_head = pl.pallas_call(
            functools.partial(backward_kernel, last, 4, chunk),
            out_shape=(shape((block, width), BF16), shape((tp_size, block, width), BF16), shape((vocab_rows, width), F32)),
            in_specs=[vmem(), vmem()] + [anywhere()] * 4, out_specs=(vmem(), vmem(), anywhere()),
            scratch_shapes=[VM((tp_size, cols, width), BF16), VM((tp_size, width, cols), BF16), VM((vocab_rows, num_tokens), BF16), VM((num_tokens, width), BF16), VM((vocab_rows, width), F32),
                            VM((block, width), BF16), VM((block, width), BF16), VM((block, tp_size * cols), BF16), DMA((2 * SLOTS,)), DMA((2 * SLOTS,)), DMA((2,)), DMA((5,))],
            compiler_params=params(4), name='backward_chain',
        )(g_top.reshape(block, width), slope, one_t, two_t, g_all, n_all)

        dx_first = spread_call(grad_x, 0, False, 5).reshape(num_tokens, width)

        step = 512
        grad_one, grad_two = pl.pallas_call(
            weight_kernel, grid=(num_tokens // step,),
            out_shape=(shape((width, cols), F32), shape((cols, width), F32)),
            in_specs=[pl.BlockSpec((step, width), lambda i: (i, 0)), pl.BlockSpec((step, width), lambda i: (i, 0)),
                      pl.BlockSpec((width, cols), lambda i: (0, 0)), pl.BlockSpec((cols, width), lambda i: (0, 0))],
            out_specs=(pl.BlockSpec((width, cols), lambda i: (0, 0)), pl.BlockSpec((cols, width), lambda i: (0, 0))),
            compiler_params=pltpu.CompilerParams(vmem_limit_bytes=VMEM_LIMIT), name='weight_grads',
        )(x_all.reshape(num_tokens, width), dy_all.reshape(num_tokens, width), w_one, w_two)

        chain_tok = tok_local.reshape(pp_size, tp_size, unit).transpose(1, 0, 2).reshape(num_tokens)
        one_hot = (chain_tok[:, None] == jnp.arange(vocab_rows, dtype=jnp.int32)[None, :]).astype(BF16)
        grad_table = de_head + contract(one_hot, dx_first, 0, 0)
        return loss.reshape(1) / num_tokens, grad_one[None], grad_two[None], grad_table

    return jax.shard_map(device_fn, mesh=mesh, in_specs=(P('dp', None), P('dp', None), P('tp', None), P('pp', None, 'tp'), P('pp', 'tp', None)), out_specs=(P('dp'), P(('dp', 'pp'), None, 'tp'), P(('dp', 'pp'), 'tp', None), P(('dp', 'tp'), None)), check_vma=False)
```

```python
import functools

import jax
import jax.numpy as jnp
from jax import lax
from jax.experimental import pallas as pl
from jax.experimental.pallas import tpu as pltpu
from jax.sharding import PartitionSpec as P

NORM_EPS = 1e-6
SIDE = 4
MESH = pl.DeviceIdType.MESH
F32 = jnp.float32
BF16 = jnp.bfloat16
CUBE = 0.044715
ROOT = 0.7978845608028654


def contract(lhs, rhs, lhs_dim, rhs_dim):
    return lax.dot_general(lhs, rhs, (((lhs_dim,), (rhs_dim,)), ((), ())), preferred_element_type=F32)


def gelu(h):
    return h * (0.5 * (1.0 + jnp.tanh(ROOT * (h + CUBE * (h * h * h)))))


def gelu_slope(h):
    sq = h * h
    t = jnp.tanh(ROOT * (h + CUBE * (sq * h)))
    return 0.5 * (1.0 + t) + (0.5 * h) * (1.0 - t * t) * (ROOT * (1.0 + (3.0 * CUBE) * sq))


def remote(src, dst, send, recv, where):
    return pltpu.make_async_remote_copy(src_ref=src, dst_ref=dst, send_sem=send, recv_sem=recv, device_id=where, device_id_type=MESH)


def signal(peer):
    pl.semaphore_signal(pltpu.get_barrier_semaphore(), inc=1, device_id=peer, device_id_type=MESH)


class Plane:
    def __init__(self):
        self.tp = lax.axis_index('tp')
        self.y = lax.rem(self.tp, SIDE)
        self.z = self.tp // SIDE

    def at(self, dy, dz):
        return lax.rem(self.z + dz + SIDE, SIDE) * SIDE + lax.rem(self.y + dy + SIDE, SIDE)

    def blk(self, half, df, ds):
        return self.at(df, ds) if half == 0 else self.at(ds, df)

    def near(self):
        return [{'tp': self.at(1, 0)}, {'tp': self.at(-1, 0)}, {'tp': self.at(0, 1)}, {'tp': self.at(0, -1)}]

    def rings(self):
        return [{'tp': self.at(d, 0)} for d in (1, 2, 3)] + [{'tp': self.at(0, d)} for d in (1, 2, 3)]


HOPS = (0, -1, 1, 2)
WALK = ((0, -1, None, 1), (0, 1, None, -1), (-1, 2, 0, 1), (1, 2, 1, -1))
BOTH = (0, 1)
SLOTS = 15


def plane_gather(plane, bufs, send_sem, recv_sem, on_block=lambda *_: None, base=0):
    def msg(a, half, slot, block, part, to):
        buf, start, size = bufs[a]
        size = size // 2
        start = start + half * size
        if part is not None:
            size = size // 2
            start = start + part * size
        ref = buf.at[plane.blk(half, *block), pl.ds(start, size)]
        return remote(ref, ref, send_sem.at[base + a], recv_sem.at[((base + a) * 2 + half) * SLOTS + slot], {'tp': plane.blk(half, *to)})

    def f(a, half, k, end):
        step = WALK[k]
        return msg(a, half, min(k, 2), (step[end], 0), None if end and k > 1 else step[2], (step[3], 0))

    def s(a, half, j, k, end):
        step = WALK[k]
        return msg(a, half, 3 * (j + 1) + min(k, 2), (HOPS[j], step[end]), None if end and k > 1 else step[2], (0, step[3]))

    send, recv = BOTH
    pairs = [(a, half) for a in range(len(bufs)) for half in BOTH]

    def across(a, half, j):
        for k in BOTH:
            s(a, half, j, k, send).start()
        on_block(a, half, j, 0)

    def onward(a, half, j):
        for k in BOTH:
            s(a, half, j, k, recv).wait_recv()
            s(a, half, j, k + 2, send).start()
            on_block(a, half, j, k + 1)

    for pair in pairs:
        for k in BOTH:
            f(*pair, k, send).start()
        across(*pair, 0)
    yield
    for pair in pairs:
        for k in BOTH:
            f(*pair, k, recv).wait_recv()
            f(*pair, k + 2, send).start()
            across(*pair, k + 1)
    yield
    for pair in pairs:
        onward(*pair, 0)
    yield
    for pair in pairs:
        f(*pair, 2, recv).wait_recv()
        across(*pair, SIDE - 1)
    yield
    for j in range(1, SIDE):
        for pair in pairs:
            onward(*pair, j)
        yield
    for j in range(SIDE):
        for pair in pairs:
            s(*pair, j, 2, recv).wait_recv()
            on_block(*pair, j, SIDE - 1)
    for a, (buf, start, size) in enumerate(bufs):
        sent = buf.at[pl.ds(0, SIDE * SIDE - 1), pl.ds(start, size)]
        remote(sent, sent, send_sem.at[base + a], recv_sem.at[0], {'tp': plane.at(1, 0)}).wait_send()


def drain(steps):
    for _ in steps:
        pass


def local(src, dst, sem):
    return pltpu.make_async_copy(src, dst, sem)


class Reduce:
    def __init__(self, plane, parts, got_one, sum_one, got_two, one_send, one_recv, two_send, two_recv):
        self.plane, self.parts, self.got_one, self.sum_one, self.got_two = plane, parts, got_one, sum_one, got_two
        self.one_send, self.one_recv, self.two_send, self.two_recv = one_send, one_recv, two_send, two_recv

    def row(self, half, index):
        size = self.parts.shape[3] // 2
        cols = pl.ds(half * size, size)
        return self.parts.at[:, index, :, cols] if half == 0 else self.parts.at[index, :, :, cols]

    def here(self, half):
        return (self.plane.y, self.plane.z) if half == 0 else (self.plane.z, self.plane.y)

    def first(self, half, d):
        n = half * 3 + d - 1
        dest = lax.rem(self.here(half)[0] + d, SIDE)
        return remote(self.row(half, dest), self.got_one.at[n], self.one_send, self.one_recv.at[half], {'tp': self.plane.blk(half, d, 0)})

    def second(self, half, d):
        n = half * 3 + d - 1
        dest = lax.rem(self.here(half)[1] + d, SIDE)
        return remote(self.sum_one.at[half, dest], self.got_two.at[n], self.two_send, self.two_recv.at[half], {'tp': self.plane.blk(half, 0, d)})

    def whole(self, got, send, recv, half=None):
        ref = got if half is None else got.at[pl.ds(half * 3, 3)]
        return remote(ref, ref, send, recv.at[half or 0], {'tp': self.plane.at(1, 0)})

    def begin(self):
        for d in (2, 1, 3):
            for half in BOTH:
                self.first(half, d).start()

    def middle(self):
        for half in BOTH:
            total = self.row(half, self.here(half)[0])[:].astype(F32)
            self.whole(self.got_one, self.one_send, self.one_recv, half).wait_recv()
            for d in (1, 3, 2):
                total = total + self.got_one[half * 3 + d - 1].astype(F32)
            self.sum_one[half] = total.astype(self.sum_one.dtype)
            for d in (2, 1, 3):
                self.second(half, d).start()

    def end(self):
        sums = []
        for half in BOTH:
            total = self.sum_one[half, self.here(half)[1]].astype(F32)
            self.whole(self.got_two, self.two_send, self.two_recv, half).wait_recv()
            for d in (1, 3, 2):
                total = total + self.got_two[half * 3 + d - 1].astype(F32)
            sums.append(total)
        return sums

    def close(self):
        self.whole(self.got_one, self.one_send, self.one_recv).wait_send()
        self.whole(self.got_two, self.two_send, self.two_recv).wait_send()


def fold(op, value):
    rows, cols = value.shape
    return op(value.reshape(rows // 8, 8, cols), axis=0)


def flatten(ids, flat):
    size, cols = ids.shape[1], flat.shape[1]
    for r in range(ids.shape[0]):
        at = r * size
        flat[at // cols:at // cols + 1, at % cols:at % cols + size] = ids[r:r + 1, :]


def rank_rows(tokens, base, rows, group, unit, rank, out):
    count = tokens.shape[1]
    blocks = count // group
    row = tokens[:] - base
    row = jnp.where((row >= 0) & (row < rows), row, 2 * rows)
    lanes = lax.broadcasted_iota(jnp.int32, (group, count), 1)
    down = lax.broadcasted_iota(jnp.int32, (group, 1), 0)

    def keys(start):
        return jnp.sum(jnp.where(lanes == start + down, row, 0), axis=1, keepdims=True)

    @pl.loop(0, blocks)
    def _(c):
        start = pl.multiple_of(c * group, group)
        mine = keys(start)
        before = (row < mine) | ((row == mine) & (lanes < start + down))
        rank[pl.ds(start, group), :] = jnp.sum(before.astype(jnp.int32), axis=1, keepdims=True)

    place = down // unit * (blocks * unit) + lax.rem(down, unit)

    def body(c, carry):
        start = pl.multiple_of(c * group, group)
        here = rank[pl.ds(start, group), :] == lanes
        return tuple(total + fold(jnp.sum, jnp.where(here, value, 0)) for total, value in zip(carry, (place + c * unit, keys(start))))

    zero = jnp.zeros((8, count), jnp.int32)
    for i, total in enumerate(lax.fori_loop(0, blocks, body, (zero, zero))):
        out[i:i + 1, :] = jnp.sum(total, axis=0, keepdims=True)


def forward_kernel(last, tokens, emb, w_one, w_two, y_out, hid_out, one_out, two_out, x_out, ones, twos, one_t, two_t, table, hot, parts,
                   got_one, sum_one, got_two, piece, x_buf, y_buf, a_buf, hid_ref, x_all, ids,
                   send_sem, recv_sem, one_send, one_recv, two_send, two_recv, line_send, line_recv, hop_sem, loc_sem):
    plane = Plane()
    stage = lax.axis_index('pp')
    tp = plane.tp
    stages = last + 1
    load = local(emb, table, loc_sem.at[2])
    own_one = local(w_one, ones.at[tp], loc_sem.at[0])
    own_two = local(w_two, twos.at[tp], loc_sem.at[1])
    load.start()
    own_one.start()
    own_two.start()
    for peer in plane.rings() + [{'pp': lax.rem(stage + d, stages)} for d in range(1, stages)]:
        signal(peer)

    rows, width = table.shape
    group = ids.shape[1]
    unit = piece.shape[0]
    count = group // tokens.shape[1]
    flatten(tokens.at[pl.ds(pl.multiple_of(stage * count, count), count)], ids)
    hot[:] = jnp.where(ids[:] - tp * rows == lax.broadcasted_iota(jnp.int32, hot.shape, 0), 1.0, 0.0).astype(BF16)
    load.wait()
    cut = rows // group * group
    for n in range(0, width, 256):
        picked = contract(hot[:cut], table[:cut, n:n + 256], 0, 0) + contract(hot[cut:], table[cut:, n:n + 256], 0, 0)
        parts[:, :, :, n:n + 256] = picked.astype(BF16).reshape(parts.shape[:3] + (256,))
    red = Reduce(plane, parts, got_one, sum_one, got_two, one_send, one_recv, two_send, two_recv)
    own_one.wait()
    own_two.wait()
    pl.semaphore_wait(pltpu.get_barrier_semaphore(), 6 + last)

    red.begin()
    gather = plane_gather(plane, [(ones, 0, ones.shape[1]), (twos, 0, twos.shape[1])], send_sem, recv_sem)
    next(gather)
    next(gather)
    red.middle()
    next(gather)
    next(gather)
    for half, total in enumerate(red.end()):
        piece[:, half * (width // 2):(half + 1) * (width // 2)] = total.astype(BF16)

    def line(p):
        return remote(piece, x_buf.at[pl.ds(pl.multiple_of(p * unit, unit), unit)], line_send, line_recv, {'pp': 0})

    @pl.when(stage != 0)
    def _():
        line(stage).start()

    @pl.when(stage == 0)
    def _():
        x_buf[:unit] = piece[:]

    drain(gather)

    blocks, _, cols = ones.shape
    save_one = local(one_t, one_out, loc_sem.at[3])
    save_two = local(two_t, two_out, loc_sem.at[4])

    def spare_time():
        @pl.loop(0, blocks)
        def _(k):
            one_t[k] = ones[k].T
            two_t[k] = twos[k].T

        save_one.start()
        save_two.start()

    pl.when(stage > 1)(spare_time)
    hop = remote(y_buf, x_buf, hop_sem.at[0], hop_sem.at[1], {'pp': lax.rem(stage + 1, stages)})

    @pl.when(stage == 0)
    def _():
        got = x_buf.at[pl.ds(0, last * unit)]
        remote(got, got, line_send, line_recv, {'pp': last}).wait_recv()

    @pl.when(stage > 0)
    def _():
        hop.wait_recv()

    x_act = x_buf[:]
    for k in range(blocks):
        hidden = jnp.dot(x_act, ones[k], preferred_element_type=F32)
        hid_ref[k] = hidden
        a_buf[:, k * cols:(k + 1) * cols] = gelu(hidden).astype(BF16)
    save_hid = local(hid_ref, hid_out, loc_sem.at[5])
    save_hid.start()
    gate = a_buf[:]
    for n in range(0, width, 256):
        branch = jnp.dot(gate, twos[:, :, n:n + 256].reshape(blocks * cols, 256), preferred_element_type=F32)
        y_buf[:, n:n + 256] = (x_buf[:, n:n + 256].astype(F32) + branch).astype(BF16)

    @pl.when(stage < last)
    def _():
        hop.start()

    y_out[:] = y_buf[:]
    x_all[tp] = x_buf[:]

    @pl.when(stage < SIDE)
    def _():
        steps = plane_gather(plane, [(x_all, 0, x_all.shape[1])], send_sem, recv_sem, base=2)
        next(steps)
        next(steps)
        pl.when(stage <= 1)(spare_time)
        drain(steps)

    save_x = local(x_all, x_out, loc_sem.at[6])
    save_x.start()
    red.close()

    @pl.when(stage != 0)
    def _():
        line(stage).wait_send()

    @pl.when(stage < last)
    def _():
        hop.wait_send()

    for save in (save_one, save_two, save_hid, save_x):
        save.wait()


def norm_of(x):
    wide = x.astype(F32)
    inv_rms = lax.rsqrt(jnp.mean(wide * wide, axis=-1, keepdims=True) + NORM_EPS)
    return inv_rms, wide * inv_rms


class Spread:
    def __init__(self, plane, source, stages, src, out, line_send, line_recv, die_send, die_recv):
        self.plane, self.source, self.stages, self.src, self.out = plane, source, stages, src, out
        self.line_send, self.line_recv, self.die_send, self.die_recv = line_send, line_recv, die_send, die_recv
        self.stage = lax.axis_index('pp')
        self.core = lax.rem(self.stage, 2)
        self.mate = {'pp': self.stage + 1 - 2 * self.core}
        self.rows = out.shape[1] // 2
        self.lo = pl.multiple_of(self.core * self.rows, self.rows)
        self.others = [p for p in range(stages) if p != source]

    def greet(self):
        twin = self.source ^ 1

        @pl.when(self.stage == self.source)
        def _():
            for p in self.others:
                signal({'pp': p})

        @pl.when(self.stage != self.source)
        def _():
            signal({'pp': self.source})

        @pl.when((self.stage != self.source) & (self.stage != twin))
        def _():
            signal(self.mate)

        return jnp.where(self.stage == self.source, len(self.others), jnp.where(self.stage == twin, 1, 2))

    def line(self, p):
        part = pl.ds((p % 2) * self.rows, self.rows)
        return remote(self.src.at[part], self.out.at[self.plane.tp, part], self.line_send, self.line_recv, {'pp': p})

    def send(self):
        for p in self.others:
            self.line(p).start()
        part = pl.ds(self.lo, self.rows)
        self.out[self.plane.tp, part] = self.src[part]

    def arrive(self):
        mine = self.out.at[self.plane.tp, pl.ds(self.lo, self.rows)]
        remote(mine, mine, self.line_recv, self.line_recv, self.mate).wait_recv()

    def on_block(self, a, half, j, k):
        if a == 0:
            size = self.rows // 2
            ref = self.out.at[self.plane.blk(half, HOPS[j], HOPS[k]), pl.ds(self.lo + half * size, size)]
            remote(ref, ref, self.die_send, self.die_recv, self.mate).start()

    def half(self, lo):
        ref = self.out.at[:, pl.ds(lo, self.rows)]
        return remote(ref, ref, self.die_send, self.die_recv, self.mate)

    def finish(self):
        self.half(pl.multiple_of((1 - self.core) * self.rows, self.rows)).wait_recv()

    def close(self):
        self.half(self.lo).wait_send()

        @pl.when(self.stage == self.source)
        def _():
            sent = self.out.at[pl.ds(0, len(self.others)), pl.ds(self.lo, self.rows)]
            remote(sent, sent, self.line_send, self.line_recv, self.mate).wait_send()


def head_kernel(target, stages, chunk, emb, y_ref, labels, loss_out, g_top, g_out, n_out,
                table, top, own_x, n_src, n_buf, lab, g_buf, peak, stat, shared, scale_ref, parts, got_one, sum_one, got_two, piece,
                send_sem, recv_sem, share_send, share_recv, own_send, own_recv, spread_send, spread_recv, die_send, die_recv,
                one_send, one_recv, two_send, two_recv, line_send, line_recv, loc_sem, *e_bufs):
    plane = Plane()
    stage = lax.axis_index('pp')
    tp = plane.tp
    size = shared.shape[0]
    others = [p for p in range(stages) if p != target]
    load = local(emb, table, loc_sem.at[0])
    load.start()
    spread = Spread(plane, target, stages, n_src, top, spread_send, spread_recv, die_send, die_recv)
    for d in range(1, size):
        signal({'tp': lax.rem(tp + d, size)})
    extra = spread.greet()
    n_src[:] = norm_of(y_ref[:])[1].astype(BF16)
    group = peak.shape[1]
    unit = group // size
    pl.semaphore_wait(pltpu.get_barrier_semaphore(), size - 1 + extra)

    def own(p):
        return remote(y_ref.at[pl.ds(p * unit, unit)], own_x, own_send, own_recv, {'pp': p})

    @pl.when(stage == target)
    def _():
        spread.send()
        for p in others:
            own(p).start()
        own_x[:] = y_ref[target * unit:(target + 1) * unit]

    pl.when(stage != target)(spread.arrive)
    drain(plane_gather(plane, [(top, spread.lo, spread.rows)], send_sem, recv_sem, spread.on_block))
    spread.finish()
    for p in range(stages):
        n_buf[p * group:(p + 1) * group] = top[:, p * unit:(p + 1) * unit, :].reshape(group, top.shape[2])
    save_n = local(n_buf, n_out, loc_sem.at[1])
    save_n.start()
    load.wait()

    rows, width = table.shape
    flatten(labels, lab)
    lab[:] = lab[:] - tp * rows
    pieces = len(e_bufs)
    pair = e_bufs[0].shape[1]

    def logit_chunk(b, start, count):
        logits = contract(table[pl.ds(start, count), :], n_buf[b * pair:(b + 1) * pair, :], 1, 1)
        e_bufs[b][pl.ds(start, count), :] = logits
        return fold(jnp.max, logits)

    def exp_chunk(b, start, count, top_b, total, hits):
        logits = e_bufs[b][pl.ds(start, count), :]
        label = jnp.concatenate([lab[p:p + 1, :] for p in range(b * pair // group, (b + 1) * pair // group)], axis=1)
        hit = label == start + lax.broadcasted_iota(jnp.int32, logits.shape, 0)
        e = jnp.exp(logits - top_b)
        e_bufs[b][pl.ds(start, count), :] = e
        return total + fold(jnp.sum, e), hits + fold(jnp.sum, jnp.where(hit, logits, 0.0))

    top_b = None
    zero = jnp.zeros((8, pair), F32)
    for b in range(pieces + 1):
        def both(start, count, carry, b=b, top_b=top_b):
            best, total, hits = carry
            if b < pieces:
                best = jnp.maximum(best, logit_chunk(b, start, count))
            if b > 0:
                total, hits = exp_chunk(b - 1, start, count, top_b, total, hits)
            return best, total, hits

        carry = (jnp.full((8, pair), -jnp.inf, F32), zero, zero)
        best, total, hits = lax.fori_loop(0, rows // chunk, lambda c, carry: both(pl.multiple_of(c * chunk, 8), chunk, carry), carry)
        if b > 0:
            lse = top_b + jnp.log(jnp.sum(total, axis=0, keepdims=True))
            hits = jnp.sum(hits, axis=0, keepdims=True)
            for i in range(pair // group):
                p = (b - 1) * (pair // group) + i
                stat[0, p:p + 1, :] = lse[:, i * group:(i + 1) * group]
                stat[1, p:p + 1, :] = hits[:, i * group:(i + 1) * group]
                peak[p:p + 1, :] = top_b[:, i * group:(i + 1) * group]
        if b < pieces:
            top_b = jnp.max(best, axis=0, keepdims=True)

    def msg(d, block):
        return remote(stat, shared.at[block], share_send, share_recv, {'tp': lax.rem(tp + d, size)})

    for d in range(1, size):
        msg(d, tp).start()
    shared[tp] = stat[:]
    all_stats = shared.at[pl.ds(0, size - 1)]
    shares = remote(all_stats, all_stats, share_send, share_recv, {'tp': plane.at(1, 0)})
    shares.wait_recv()
    every = shared[:, 0]
    most = jnp.max(every, axis=0)
    log_norm = most + jnp.log(jnp.sum(jnp.exp(every - most[None]), axis=0))
    loss_out[:] = jnp.sum(log_norm - jnp.sum(shared[:, 1], axis=0), keepdims=True) / (stages * group)
    scale_ref[:] = jnp.exp(peak[:] - log_norm)

    def grad_block(p, slot):
        e_ref = e_bufs[p // (pair // group)]
        col = p % (pair // group) * group

        def part(start, count):
            e = e_ref[pl.ds(start, count), col:col + group]
            hit = lab[p:p + 1, :] == start + lax.broadcasted_iota(jnp.int32, e.shape, 0)
            g_buf[slot, pl.ds(start, count), :] = (e * scale_ref[p:p + 1, :] - jnp.where(hit, 1.0, 0.0)).astype(BF16)

        @pl.loop(0, rows // chunk)
        def _(c):
            part(pl.multiple_of(c * chunk, 8), chunk)

    def save(p):
        slot = 1 + p % 2
        return local(g_buf.at[slot], g_out.at[:, p * group:(p + 1) * group], loc_sem.at[2 + slot])

    for p in range(stages):
        pl.when(stage == p)(functools.partial(grad_block, p, 0))
    cut = rows // group * group
    for n in range(0, width, 256):
        back = contract(g_buf[0, :cut, :], table[:cut, n:n + 256], 0, 0) + contract(g_buf[0, cut:, :], table[cut:, n:n + 256], 0, 0)
        parts[:, :, :, n:n + 256] = back.reshape(parts.shape[:3] + (256,))
    red = Reduce(plane, parts, got_one, sum_one, got_two, one_send, one_recv, two_send, two_recv)
    red.begin()
    for p in range(stages):
        if p >= 2:
            save(p - 2).wait()
        grad_block(p, 1 + p % 2)
        save(p).start()
    red.middle()
    sums = red.end()

    @pl.when(stage != target)
    def _():
        remote(own_x, own_x, own_recv, own_recv, spread.mate).wait_recv()

    inv_rms, normed = norm_of(own_x[:])
    half = width // 2
    mean = (jnp.sum(normed[:, :half] * sums[0], axis=-1, keepdims=True) + jnp.sum(normed[:, half:] * sums[1], axis=-1, keepdims=True)) / width
    for h in BOTH:
        piece[:, h * half:(h + 1) * half] = (inv_rms * (sums[h] - normed[:, h * half:(h + 1) * half] * mean)).astype(BF16)

    def line(p):
        return remote(piece, g_top.at[p], line_send, line_recv, {'pp': target})

    @pl.when(stage != target)
    def _():
        line(stage).start()

    @pl.when(stage == target)
    def _():
        g_top[target] = piece[:]
        got = g_top.at[pl.ds(0, len(others))]
        remote(got, got, line_send, line_recv, spread.mate).wait_recv()

    red.close()
    shares.wait_send()
    save_n.wait()
    save(stages - 2).wait()
    save(stages - 1).wait()
    spread.close()

    @pl.when(stage == target)
    def _():
        sent = y_ref.at[pl.ds(0, len(others) * unit)]
        remote(sent, sent, own_send, own_recv, spread.mate).wait_send()

    @pl.when(stage != target)
    def _():
        line(stage).wait_send()


def backward_kernel(last, early, chunk, tokens, g_top, hid_in, one_all, two_all, g_all, n_all, x_in, w_one, w_two, de_buf, dx_all, grad_one, grad_two, order_out,
                    ones, twos, slope_ref, g_buf, n_buf, x_all, w_one_buf, w_two_buf, dy_all, dy_buf, dx_buf, d_buf, flat, rank,
                    send_sem, recv_sem, spread_send, spread_recv, die_send, die_recv, hop_sem, go_sem, g_sem, loc_sem):
    plane = Plane()
    stage = lax.axis_index('pp')
    stages = last + 1
    blocks, cols, width = one_all.shape
    pairs = ((hid_in, slope_ref), (two_all, twos), (one_all, ones), (n_all, n_buf), (w_one, w_one_buf), (w_two, w_two_buf))
    loads = [local(src, dst, loc_sem.at[i]) for i, (src, dst) in enumerate(pairs)]
    for load in loads:
        load.start()
    late = stage >= SIDE
    own_x = local(x_in.at[plane.tp], x_all.at[plane.tp], loc_sem.at[6])
    all_x = local(x_in, x_all, loc_sem.at[6])
    pl.when(late)(own_x.start)
    pl.when(jnp.logical_not(late))(all_x.start)
    spread = Spread(plane, 0, stages, dx_buf, dx_all, spread_send, spread_recv, die_send, die_recv)
    near = plane.near()
    for peer in near:
        signal(peer)
    extra = spread.greet()
    after = {'pp': lax.rem(stage + 1, stages)}
    before = {'pp': lax.rem(stage + last, stages)}
    signal(after)
    signal(before)
    pl.semaphore_wait(pltpu.get_barrier_semaphore(), len(near) + 2 + extra)
    hop = remote(dx_buf, dy_buf, hop_sem.at[0], hop_sem.at[1], before)
    rows = de_buf.shape[0]
    full = rows // chunk
    rest = rows - full * chunk

    def fetch(c, count):
        slot = lax.rem(c, 2)
        return local(g_all.at[pl.ds(pl.multiple_of(c * chunk, chunk), count)], g_buf.at[slot, pl.ds(0, count)], g_sem.at[slot])

    def table_part(c, count):
        fetch(c, count).wait()
        de_buf[pl.ds(pl.multiple_of(c * chunk, chunk), count), :] = jnp.dot(g_buf[lax.rem(c, 2), pl.ds(0, count), :], n_buf[:], preferred_element_type=F32)

    def table():
        fetch(0, chunk).start()
        loads[3].wait()

        @pl.loop(0, full - 1)
        def _(c):
            fetch(c + 1, chunk).start()
            table_part(c, chunk)

        fetch(full, rest).start()
        table_part(full - 1, chunk)
        table_part(full, rest)

    loads[0].wait()
    for k in range(blocks):
        slope_ref[k] = gelu_slope(slope_ref[k])
    def ranking():
        flatten(tokens, flat)
        rank_rows(flat, plane.tp * rows, rows, blocks * dy_all.shape[1] // stages, dy_all.shape[1] // stages, rank, order_out)

    @pl.when(stage <= early)
    def _():
        table()
        pl.when(stage <= 1)(ranking)

    loads[1].wait()

    @pl.when(stage == last)
    def _():
        dy_buf[:] = g_top[:]

    @pl.when(stage < last)
    def _():
        hop.wait_recv()

    dy_all[plane.tp] = dy_buf[:]
    whole = (dy_all, 0, dy_all.shape[1])
    part = (dx_all, spread.lo, spread.rows)
    first = plane_gather(plane, [whole], send_sem, recv_sem, base=1)

    @pl.when(stage <= 1)
    def _():
        next(first)

    grad_y = dy_buf[:]
    for k in range(blocks):
        grad_gate = jnp.dot(grad_y, twos[k], preferred_element_type=F32)
        d_buf[:, k * cols:(k + 1) * cols] = (slope_ref[k] * grad_gate).astype(BF16)
    loads[2].wait()
    grad_hidden = d_buf[:]
    for n in range(0, width, 256):
        back = jnp.dot(grad_hidden, ones[:, :, n:n + 256].reshape(blocks * cols, 256), preferred_element_type=F32)
        dx_buf[:, n:n + 256] = (dy_buf[:, n:n + 256].astype(F32) + back).astype(BF16)

    @pl.when(stage > 0)
    def _():
        hop.start()

    pl.when(stage == 0)(spread.send)
    for load in loads[4:]:
        load.wait()
    pl.when(late)(own_x.wait)
    pl.when(jnp.logical_not(late))(all_x.wait)

    def weights():
        grad_one[:] = jnp.zeros_like(grad_one)
        grad_two[:] = jnp.zeros_like(grad_two)
        step = SIDE

        @pl.loop(0, x_all.shape[0] // step)
        def _(c):
            part = pl.ds(c * step, step)
            x_act = x_all[part].reshape(step * x_all.shape[1], width)
            grad_y = dy_all[part].reshape(step * x_all.shape[1], width)
            hidden = jnp.dot(x_act, w_one_buf[:], preferred_element_type=F32)
            grad_gate = contract(grad_y, w_two_buf[:], 1, 1)
            grad_hidden = (gelu_slope(hidden) * grad_gate).astype(BF16)
            grad_one[:] += contract(x_act, grad_hidden, 0, 0)
            grad_two[:] += contract(gelu(hidden).astype(BF16), grad_y, 0, 0)

    @pl.when(stage > 1)
    def _():
        hop.wait_send()

        @pl.when(spread.core == 0)
        def _():
            pl.semaphore_signal(go_sem, inc=1, device_id=spread.mate, device_id_type=MESH)

        @pl.when(spread.core == 1)
        def _():
            pl.semaphore_wait(go_sem, 1)

        @pl.when(late)
        def _():
            steps = plane_gather(plane, [whole, (x_all, 0, x_all.shape[1])], send_sem, recv_sem, base=1)
            next(steps)
            next(steps)
            table()
            drain(steps)

        @pl.when(jnp.logical_not(late))
        def _():
            drain(plane_gather(plane, [whole], send_sem, recv_sem, base=1))

        weights()
        ranking()
        spread.arrive()
        drain(plane_gather(plane, [part], send_sem, recv_sem, spread.on_block))
        spread.finish()

    @pl.when(stage <= 1)
    def _():
        pl.when(stage == 1)(spread.arrive)
        second = plane_gather(plane, [part], send_sem, recv_sem, spread.on_block)
        next(second)
        for _ in zip(first, second):
            pass
        drain(first)
        drain(second)
        weights()
        spread.finish()

    spread.close()

    @pl.when(stage == 1)
    def _():
        hop.wait_send()


def add_kernel(chunk, order, dx_ref, de_ref, one_ref, two_ref, de_out, table_out, one_out, two_out, wide, sem):
    saves = [local(one_ref, one_out, sem.at[0]), local(two_ref, two_out, sem.at[1])]
    for save in saves:
        save.start()
    wide[:] = dx_ref[:].astype(F32)
    count = order.shape[1]
    rows = de_ref.shape[0]
    j = 0
    for c in range(rows // chunk):
        def more(j, end=(c + 1) * chunk):
            return (j < count) & (order[1, jnp.minimum(j, count - 1)] < end)

        def add(j):
            row = pl.ds(order[1, j], 1)
            de_out[row, :] = de_out[row, :] + wide[pl.ds(order[0, j], 1), :]
            return j + 1

        j = lax.while_loop(more, add, j)
        part = pl.ds(c * chunk, chunk)
        saves.append(local(de_out.at[part], table_out.at[part], sem.at[2 + c]))
        saves[-1].start()
    for save in saves:
        save.wait()


def vmem():
    return pl.BlockSpec(memory_space=pltpu.VMEM)


def anywhere():
    return pl.BlockSpec(memory_space=pl.ANY)


def params(cid, mib):
    return pltpu.CompilerParams(collective_id=cid, has_side_effects=True, vmem_limit_bytes=mib << 20)


DMA = pltpu.SemaphoreType.DMA


def solution(mesh):
    pp_size = mesh.shape['pp']
    tp_size = mesh.shape['tp']
    last = pp_size - 1

    def device_fn(tokens, labels, emb_table, w_in, w_out):
        num_tokens = tokens.shape[0] * tokens.shape[1]
        vocab_rows, width = emb_table.shape
        w_one, w_two = w_in[0], w_out[0]
        cols = w_one.shape[1]
        unit = num_tokens // (pp_size * tp_size)
        block = pp_size * unit
        group = tp_size * unit
        half = width // 2
        chunk = vocab_rows // 3
        step = 512
        pair = 2 * group
        shape = jax.ShapeDtypeStruct
        VM = pltpu.VMEM

        def reduce_scratch(dtype):
            return [VM((SIDE, SIDE, unit, width), dtype), VM((6, SIDE, unit, half), dtype), VM((2, SIDE, unit, half), dtype), VM((6, unit, half), dtype), VM((unit, width), BF16)]

        reduce_sems = [DMA, DMA((2,)), DMA, DMA((2,)), DMA, DMA]
        many = shape((tp_size, block, width), BF16)
        many_buf = VM((tp_size, block, width), BF16)
        two_sums = 2 * SLOTS

        y_act, hidden, one_t, two_t, x_all = pl.pallas_call(
            functools.partial(forward_kernel, last),
            out_shape=(shape((block, width), BF16), shape((tp_size, block, cols), F32), shape((tp_size, cols, width), BF16), shape((tp_size, width, cols), BF16), many),
            in_specs=[vmem()] + [anywhere()] * 3,
            out_specs=[vmem()] + [anywhere()] * 4,
            scratch_shapes=[VM((tp_size, width, cols), BF16), VM((tp_size, cols, width), BF16), VM((tp_size, cols, width), BF16), VM((tp_size, width, cols), BF16),
                            VM((vocab_rows, width), BF16), VM((vocab_rows, group), BF16), *reduce_scratch(BF16),
                            VM((block, width), BF16), VM((block, width), BF16), VM((block, tp_size * cols), BF16), VM((tp_size, block, cols), F32), many_buf, VM((1, group), jnp.int32),
                            DMA((3,)), DMA((3 * two_sums,)), *reduce_sems, DMA((2,)), DMA((7,))],
            compiler_params=params(1, 58), name='forward_chain',
        )(tokens, emb_table, w_one, w_two)

        spread_sems = [DMA, DMA, DMA, DMA]
        loss, g_top, g_all, n_all = pl.pallas_call(
            functools.partial(head_kernel, last, pp_size, chunk),
            out_shape=(shape((1, 1), F32), shape((pp_size, unit, width), BF16), shape((vocab_rows, num_tokens), BF16), shape((num_tokens, width), BF16)),
            in_specs=[anywhere(), vmem(), vmem()],
            out_specs=[vmem()] * 2 + [anywhere()] * 2,
            scratch_shapes=[VM((vocab_rows, width), BF16), many_buf, VM((unit, width), BF16), VM((block, width), BF16), VM((num_tokens, width), BF16),
                            VM((pp_size, group), jnp.int32), VM((3, vocab_rows, group), BF16),
                            VM((pp_size, group), F32), VM((2, pp_size, group), F32), VM((tp_size, 2, pp_size, group), F32), VM((pp_size, group), F32), *reduce_scratch(F32),
                            DMA((1,)), DMA((two_sums,)), DMA, DMA, DMA, DMA, *spread_sems, *reduce_sems, DMA((5,)),
                            *[VM((vocab_rows, pair), F32) for _ in range(num_tokens // pair)]],
            compiler_params=params(2, 60), name='head',
        )(emb_table, y_act, labels)

        de_head, dx_first, grad_one, grad_two, order = pl.pallas_call(
            functools.partial(backward_kernel, last, 3, step),
            out_shape=(VM((vocab_rows, width), F32), many_buf, VM((width, cols), F32), VM((cols, width), F32), shape((2, num_tokens), jnp.int32)),
            in_specs=[vmem()] * 2 + [anywhere()] * 8, out_specs=[vmem()] * 5,
            scratch_shapes=[VM((tp_size, cols, width), BF16), VM((tp_size, width, cols), BF16), VM((tp_size, block, cols), F32), VM((2, step, num_tokens), BF16), VM((num_tokens, width), BF16),
                            many_buf, VM((width, cols), BF16), VM((cols, width), BF16), many_buf,
                            VM((block, width), BF16), VM((block, width), BF16), VM((block, tp_size * cols), BF16), VM((1, num_tokens), jnp.int32), VM((num_tokens, 1), jnp.int32),
                            DMA((3,)), DMA((3 * two_sums,)), *spread_sems, DMA((2,)), pltpu.SemaphoreType.REGULAR, DMA((2,)), DMA((7,))],
            compiler_params=params(3, 44), name='backward_chain',
        )(tokens, g_top.reshape(block, width), hidden, one_t, two_t, g_all, n_all, x_all, w_one, w_two)

        smem = pl.BlockSpec(memory_space=pltpu.SMEM)
        _, grad_table, grad_one, grad_two = pl.pallas_call(
            functools.partial(add_kernel, chunk),
            out_shape=(VM((vocab_rows, width), F32), shape((vocab_rows, width), F32), shape((width, cols), F32), shape((cols, width), F32)),
            in_specs=[smem] + [vmem()] * 4, out_specs=[vmem()] + [anywhere()] * 3,
            scratch_shapes=[VM((num_tokens, width), F32), DMA((5,))], input_output_aliases={2: 0},
            compiler_params=pltpu.CompilerParams(vmem_limit_bytes=24 << 20), name='add_rows',
        )(order, dx_first.reshape(num_tokens, width), de_head, grad_one, grad_two)
        return loss.reshape(1), grad_one[None], grad_two[None], grad_table

    return jax.shard_map(device_fn, mesh=mesh, in_specs=(P('dp', None), P('dp', None), P('tp', None), P('pp', None, 'tp'), P('pp', 'tp', None)), out_specs=(P('dp'), P(('dp', 'pp'), None, 'tp'), P(('dp', 'pp'), 'tp', None), P(('dp', 'tp'), None)), check_vma=False)
```

```python
import functools

import jax
import jax.numpy as jnp
from jax import lax
from jax.experimental import pallas as pl
from jax.experimental.pallas import tpu as pltpu
from jax.sharding import PartitionSpec as P

NORM_EPS = 1e-6
SIDE = 4
MESH = pl.DeviceIdType.MESH
F32 = jnp.float32
BF16 = jnp.bfloat16
CUBE = 0.044715
ROOT = 0.7978845608028654


def contract(lhs, rhs, lhs_dim, rhs_dim):
    return lax.dot_general(lhs, rhs, (((lhs_dim,), (rhs_dim,)), ((), ())), preferred_element_type=F32)


def gelu(h):
    return h * (0.5 * (1.0 + jnp.tanh(ROOT * (h + CUBE * (h * h * h)))))


def gelu_slope(h):
    sq = h * h
    t = jnp.tanh(ROOT * (h + CUBE * (sq * h)))
    return 0.5 * (1.0 + t) + (0.5 * h) * (1.0 - t * t) * (ROOT * (1.0 + (3.0 * CUBE) * sq))


def remote(src, dst, send, recv, where):
    return pltpu.make_async_remote_copy(src_ref=src, dst_ref=dst, send_sem=send, recv_sem=recv, device_id=where, device_id_type=MESH)


def signal(peer):
    pl.semaphore_signal(pltpu.get_barrier_semaphore(), inc=1, device_id=peer, device_id_type=MESH)


class Plane:
    def __init__(self):
        self.tp = lax.axis_index('tp')
        self.y = lax.rem(self.tp, SIDE)
        self.z = self.tp // SIDE

    def at(self, dy, dz):
        return lax.rem(self.z + dz + SIDE, SIDE) * SIDE + lax.rem(self.y + dy + SIDE, SIDE)

    def blk(self, half, df, ds):
        return self.at(df, ds) if half == 0 else self.at(ds, df)

    def near(self):
        return [{'tp': self.at(1, 0)}, {'tp': self.at(-1, 0)}, {'tp': self.at(0, 1)}, {'tp': self.at(0, -1)}]

    def rings(self):
        return [{'tp': self.at(d, 0)} for d in (1, 2, 3)] + [{'tp': self.at(0, d)} for d in (1, 2, 3)]


HOPS = (0, -1, 1, 2)
WALK = ((0, -1, None, 1), (0, 1, None, -1), (-1, 2, 0, 1), (1, 2, 1, -1))
BOTH = (0, 1)
TILE = 256
SLOTS = 15


def plane_gather(plane, bufs, send_sem, recv_sem, on_block=lambda *_: None, base=0, begun=False):
    def msg(a, half, slot, block, part, to):
        buf, start, size = bufs[a]
        size = size // 2
        start = start + half * size
        if part is not None:
            size = size // 2
            start = start + part * size
        ref = buf.at[plane.blk(half, *block), pl.ds(start, size)]
        return remote(ref, ref, send_sem.at[base + a], recv_sem.at[((base + a) * 2 + half) * SLOTS + slot], {'tp': plane.blk(half, *to)})

    def f(a, half, k, end):
        step = WALK[k]
        return msg(a, half, min(k, 2), (step[end], 0), None if end and k > 1 else step[2], (step[3], 0))

    def s(a, half, j, k, end):
        step = WALK[k]
        return msg(a, half, 3 * (j + 1) + min(k, 2), (HOPS[j], step[end]), None if end and k > 1 else step[2], (0, step[3]))

    send, recv = BOTH
    pairs = [(a, half) for a in range(len(bufs)) for half in BOTH]

    def across(a, half, j):
        for k in BOTH:
            s(a, half, j, k, send).start()
        on_block(a, half, j, 0)

    def onward(a, half, j):
        for k in BOTH:
            s(a, half, j, k, recv).wait_recv()
            s(a, half, j, k + 2, send).start()
            on_block(a, half, j, k + 1)

    if not begun:
        for pair in pairs:
            for k in BOTH:
                f(*pair, k, send).start()
            across(*pair, 0)
        yield
    for pair in pairs:
        for k in BOTH:
            f(*pair, k, recv).wait_recv()
            f(*pair, k + 2, send).start()
            across(*pair, k + 1)
    yield
    for pair in pairs:
        onward(*pair, 0)
    yield
    for pair in pairs:
        f(*pair, 2, recv).wait_recv()
        across(*pair, SIDE - 1)
    yield
    for j in range(1, SIDE):
        for pair in pairs:
            onward(*pair, j)
        yield
    for j in range(SIDE):
        for pair in pairs:
            s(*pair, j, 2, recv).wait_recv()
            on_block(*pair, j, SIDE - 1)
    for a, (buf, start, size) in enumerate(bufs):
        sent = buf.at[pl.ds(0, SIDE * SIDE - 1), pl.ds(start, size)]
        remote(sent, sent, send_sem.at[base + a], recv_sem.at[0], {'tp': plane.at(1, 0)}).wait_send()


def tiles(width):
    return [slice(n, n + TILE) for n in range(0, width, TILE)]


def drain(steps):
    for _ in steps:
        pass


def local(src, dst, sem):
    return pltpu.make_async_copy(src, dst, sem)


class Reduce:
    def __init__(self, plane, parts, got_one, sum_one, got_two, one_send, one_recv, two_send, two_recv):
        self.plane, self.parts, self.got_one, self.sum_one, self.got_two = plane, parts, got_one, sum_one, got_two
        self.one_send, self.one_recv, self.two_send, self.two_recv = one_send, one_recv, two_send, two_recv

    def row(self, half, index):
        size = self.parts.shape[3] // 2
        cols = pl.ds(half * size, size)
        return self.parts.at[:, index, :, cols] if half == 0 else self.parts.at[index, :, :, cols]

    def here(self, half):
        return (self.plane.y, self.plane.z) if half == 0 else (self.plane.z, self.plane.y)

    def first(self, half, d):
        n = half * 3 + d - 1
        dest = lax.rem(self.here(half)[0] + d, SIDE)
        return remote(self.row(half, dest), self.got_one.at[n], self.one_send, self.one_recv.at[half], {'tp': self.plane.blk(half, d, 0)})

    def second(self, half, d):
        n = half * 3 + d - 1
        dest = lax.rem(self.here(half)[1] + d, SIDE)
        return remote(self.sum_one.at[half, dest], self.got_two.at[n], self.two_send, self.two_recv.at[half], {'tp': self.plane.blk(half, 0, d)})

    def whole(self, got, send, recv, half=None):
        ref = got if half is None else got.at[pl.ds(half * 3, 3)]
        return remote(ref, ref, send, recv.at[half or 0], {'tp': self.plane.at(1, 0)})

    def begin(self, half):
        for d in (2, 1, 3):
            self.first(half, d).start()

    def middle(self):
        for half in BOTH:
            total = self.row(half, self.here(half)[0])[:].astype(F32)
            self.whole(self.got_one, self.one_send, self.one_recv, half).wait_recv()
            for d in (1, 3, 2):
                total = total + self.got_one[half * 3 + d - 1].astype(F32)
            self.sum_one[half] = total.astype(self.sum_one.dtype)
            for d in (2, 1, 3):
                self.second(half, d).start()

    def end(self):
        sums = []
        for half in BOTH:
            total = self.sum_one[half, self.here(half)[1]].astype(F32)
            self.whole(self.got_two, self.two_send, self.two_recv, half).wait_recv()
            for d in (1, 3, 2):
                total = total + self.got_two[half * 3 + d - 1].astype(F32)
            sums.append(total)
        return sums

    def close(self):
        self.whole(self.got_one, self.one_send, self.one_recv).wait_send()
        self.whole(self.got_two, self.two_send, self.two_recv).wait_send()


def fold(op, value):
    rows, cols = value.shape
    return op(value.reshape(rows // 8, 8, cols), axis=0)


def flatten(ids, flat):
    size, cols = ids.shape[1], flat.shape[1]
    for r in range(ids.shape[0]):
        at = r * size
        flat[at // cols:at // cols + 1, at % cols:at % cols + size] = ids[r:r + 1, :]


def list_rows(tokens, base, rows, group, unit, flat, slot, out):
    lines, lanes = flat.shape
    count = lines * lanes
    flatten(tokens, flat)
    row = flat[:] - base
    mine = (row >= 0) & (row < rows)
    upper = lax.broadcasted_iota(jnp.int32, (lanes, lanes), 0) <= lax.broadcasted_iota(jnp.int32, (lanes, lanes), 1)
    ones = [jnp.where(mask, 1.0, 0.0).astype(BF16) for mask in (mine, upper)]
    seen = jnp.dot(*ones, preferred_element_type=F32)
    total = jnp.zeros((1, 1), F32)
    for r in range(lines):
        line = slice(r, r + 1)
        here = slice(r * lanes, (r + 1) * lanes)
        slot[:1, here] = jnp.where(mine[line], seen[line] + (total - 1.0), -1.0).astype(jnp.int32)
        slot[1:, here] = row[line]
        total = total + seen[line, lanes - 1:]
    number = lax.broadcasted_iota(jnp.int32, (1, count), 1)
    inner = lax.rem(number, group)
    place = inner // unit * (count // group * unit) + number // group * unit + lax.rem(number, unit)
    digits = [part for value in (place, slot[1:, :]) for part in (value // 256, lax.rem(value, 256))]
    which = lax.broadcasted_iota(jnp.int32, (16, count), 0)
    values = sum(jnp.where(which == i, digit, 0) for i, digit in enumerate(digits)).astype(F32).astype(BF16)

    @pl.loop(0, count // group)
    def _(c):
        start = pl.multiple_of(c * group, group)
        pick = jnp.where(slot[:1, :] == start + lax.broadcasted_iota(jnp.int32, (group, count), 0), 1.0, 0.0).astype(BF16)
        found = contract(values, pick, 1, 1)
        for i in BOTH:
            out[i:i + 1, pl.ds(start, group)] = (found[2 * i:2 * i + 1] * 256.0 + found[2 * i + 1:2 * i + 2]).astype(jnp.int32)

    out[2:, :] = jnp.broadcast_to(total, (1, count)).astype(jnp.int32)


def forward_kernel(last, tokens, emb, w_one, w_two, y_out, order_out, hid_out, one_out, two_out, x_out, ones, twos, one_t, two_t, table, hot, parts,
                   got_one, sum_one, got_two, piece, x_buf, y_buf, a_buf, hid_ref, x_all, ids, flat, slot,
                   send_sem, recv_sem, one_send, one_recv, two_send, two_recv, line_send, line_recv, hop_send, hop_recv, loc_sem):
    plane = Plane()
    stage = lax.axis_index('pp')
    tp = plane.tp
    stages = last + 1
    moves = ((emb, table), (w_one, ones.at[tp]), (w_two, twos.at[tp]), (one_t, one_out), (two_t, two_out), (hid_ref, hid_out), (x_all, x_out))
    load, own_one, own_two, *saves = [local(src, dst, loc_sem.at[i]) for i, (src, dst) in enumerate(moves)]
    save_one, save_two, save_hid, save_x = saves
    load.start()
    own_one.start()
    own_two.start()
    for peer in plane.rings() + [{'pp': lax.rem(stage + d, stages)} for d in range(1, stages)]:
        signal(peer)

    own_one.wait()
    own_two.wait()
    pl.semaphore_wait(pltpu.get_barrier_semaphore(), 6 + last)
    gather = plane_gather(plane, [(ones, 0, ones.shape[1]), (twos, 0, twos.shape[1])], send_sem, recv_sem)
    next(gather)

    rows, width = table.shape
    group = ids.shape[1]
    unit = piece.shape[0]
    count = group // tokens.shape[1]
    flatten(tokens.at[pl.ds(pl.multiple_of(stage * count, count), count)], ids)
    hot[:] = jnp.where(ids[:] - tp * rows == lax.broadcasted_iota(jnp.int32, hot.shape, 0), 1.0, 0.0).astype(BF16)
    load.wait()
    cut = rows // group * group
    for cols in tiles(width):
        picked = contract(hot[:cut], table[:cut, cols], 0, 0) + contract(hot[cut:], table[cut:, cols], 0, 0)
        parts[:, :, :, cols] = picked.astype(BF16).reshape(*parts.shape[:-1], TILE)
    red = Reduce(plane, parts, got_one, sum_one, got_two, one_send, one_recv, two_send, two_recv)
    for half in BOTH:
        red.begin(half)
    next(gather)
    next(gather)
    red.middle()
    next(gather)
    next(gather)
    for half, total in enumerate(red.end()):
        piece[:, half * (width // 2):(half + 1) * (width // 2)] = total.astype(BF16)

    def line(p):
        return remote(piece, x_buf.at[pl.ds(pl.multiple_of(p * unit, unit), unit)], line_send, line_recv, {'pp': 0})

    @pl.when(stage != 0)
    def _():
        line(stage).start()

    @pl.when(stage == 0)
    def _():
        x_buf[:unit] = piece[:]

    drain(gather)

    blocks, _, cols = ones.shape

    def spare_time():
        @pl.loop(0, blocks)
        def _(k):
            one_t[k] = ones[k].T
            two_t[k] = twos[k].T

        save_one.start()
        save_two.start()
        list_rows(tokens, tp * rows, rows, group, unit, flat, slot, order_out)

    pl.when(stage > 1)(spare_time)
    hop = remote(y_buf, x_buf, hop_send, hop_recv, {'pp': lax.rem(stage + 1, stages)})

    @pl.when(stage == 0)
    def _():
        got = x_buf.at[pl.ds(0, last * unit)]
        remote(got, got, line_send, line_recv, {'pp': last}).wait_recv()

    pl.when(stage > 0)(hop.wait_recv)
    x_act = x_buf[:]
    for k in range(blocks):
        hidden = jnp.dot(x_act, ones[k], preferred_element_type=F32)
        hid_ref[k] = hidden
        a_buf[:, k * cols:(k + 1) * cols] = gelu(hidden).astype(BF16)
    save_hid.start()
    gate = a_buf[:]
    for tile in tiles(width):
        branch = jnp.dot(gate, twos[:, :, tile].reshape(blocks * cols, TILE), preferred_element_type=F32)
        y_buf[:, tile] = (x_buf[:, tile].astype(F32) + branch).astype(BF16)

    pl.when(stage < last)(hop.start)
    y_out[:] = y_buf[:]
    x_all[tp] = x_buf[:]

    @pl.when(stage < SIDE)
    def _():
        steps = plane_gather(plane, [(x_all, 0, x_all.shape[1])], send_sem, recv_sem, base=2)
        next(steps)
        next(steps)
        pl.when(stage <= 1)(spare_time)
        drain(steps)

    save_x.start()
    red.close()

    @pl.when(stage != 0)
    def _():
        line(stage).wait_send()

    pl.when(stage < last)(hop.wait_send)
    for save in saves:
        save.wait()


def norm_of(x):
    wide = x.astype(F32)
    inv_rms = lax.rsqrt(jnp.mean(wide * wide, axis=-1, keepdims=True) + NORM_EPS)
    return inv_rms, wide * inv_rms


class Spread:
    def __init__(self, plane, source, stages, src, out, line_send, line_recv, die_send, die_recv):
        self.plane, self.source, self.stages, self.src, self.out = plane, source, stages, src, out
        self.line_send, self.line_recv, self.die_send, self.die_recv = line_send, line_recv, die_send, die_recv
        self.stage = lax.axis_index('pp')
        self.core = lax.rem(self.stage, 2)
        self.mate = {'pp': self.stage + 1 - 2 * self.core}
        self.rows = out.shape[1] // 2
        self.lo = pl.multiple_of(self.core * self.rows, self.rows)
        self.others = [p for p in range(stages) if p != source]

    def greet(self):
        twin = self.source ^ 1

        @pl.when(self.stage == self.source)
        def _():
            for p in self.others:
                signal({'pp': p})

        @pl.when(self.stage != self.source)
        def _():
            signal({'pp': self.source})

        @pl.when((self.stage != self.source) & (self.stage != twin))
        def _():
            signal(self.mate)

        return jnp.where(self.stage == self.source, len(self.others), jnp.where(self.stage == twin, 1, 2))

    def line(self, p):
        part = pl.ds((p % 2) * self.rows, self.rows)
        return remote(self.src.at[part], self.out.at[self.plane.tp, part], self.line_send, self.line_recv, {'pp': p})

    def send(self):
        for p in self.others:
            self.line(p).start()
        part = pl.ds(self.lo, self.rows)
        self.out[self.plane.tp, part] = self.src[part]

    def arrive(self):
        mine = self.out.at[self.plane.tp, pl.ds(self.lo, self.rows)]
        remote(mine, mine, self.line_recv, self.line_recv, self.mate).wait_recv()

    def on_block(self, a, half, j, k):
        if a == 0:
            size = self.rows // 2
            ref = self.out.at[self.plane.blk(half, HOPS[j], HOPS[k]), pl.ds(self.lo + half * size, size)]
            remote(ref, ref, self.die_send, self.die_recv, self.mate).start()

    def half(self, lo):
        ref = self.out.at[:, pl.ds(lo, self.rows)]
        return remote(ref, ref, self.die_send, self.die_recv, self.mate)

    def finish(self):
        self.half(pl.multiple_of((1 - self.core) * self.rows, self.rows)).wait_recv()

    def close(self):
        self.half(self.lo).wait_send()

        @pl.when(self.stage == self.source)
        def _():
            sent = self.out.at[pl.ds(0, len(self.others)), pl.ds(self.lo, self.rows)]
            remote(sent, sent, self.line_send, self.line_recv, self.mate).wait_send()


def head_kernel(target, stages, middle, chunk, emb, y_ref, labels, x_in, loss_out, g_top, g_out, n_out, x_out,
                table, top, own_x, n_src, n_buf, x_all, lab, g_buf, peak, stat, shared, scale_ref, parts, got_one, sum_one, got_two, piece,
                send_sem, recv_sem, share_send, share_recv, own_send, own_recv, spread_send, spread_recv, die_send, die_recv,
                one_send, one_recv, two_send, two_recv, line_send, line_recv, loc_sem, *e_bufs):
    plane = Plane()
    stage = lax.axis_index('pp')
    tp = plane.tp
    size = shared.shape[1]
    others = [p for p in range(stages) if p != target]
    load = local(emb, table, loc_sem.at[0])
    load.start()
    upper = stage >= middle
    mine = local(x_in.at[tp], x_all.at[tp], loc_sem.at[2])
    pl.when(upper)(mine.start)
    spread = Spread(plane, target, stages, n_src, top, spread_send, spread_recv, die_send, die_recv)
    for d in range(1, size):
        signal({'tp': lax.rem(tp + d, size)})
    extra = spread.greet()
    n_src[:] = norm_of(y_ref[:])[1].astype(BF16)
    group = peak.shape[1]
    unit = group // size
    pl.semaphore_wait(pltpu.get_barrier_semaphore(), size - 1 + extra)

    def own(p):
        return remote(y_ref.at[pl.ds(p * unit, unit)], own_x, own_send, own_recv, {'pp': p})

    @pl.when(stage == target)
    def _():
        spread.send()
        for p in others:
            own(p).start()
        own_x[:] = y_ref[target * unit:(target + 1) * unit]

    pl.when(stage != target)(spread.arrive)
    drain(plane_gather(plane, [(top, spread.lo, spread.rows)], send_sem, recv_sem, spread.on_block))
    spread.finish()
    for p in range(stages):
        n_buf[p * group:(p + 1) * group] = top[:, p * unit:(p + 1) * unit, :].reshape(group, top.shape[2])
    save_n = local(n_buf, n_out, loc_sem.at[1])
    save_n.start()
    load.wait()

    top_plane = stage >= middle + 2
    ways = [(here, plane_gather(plane, [(x_all, 0, x_all.shape[1])], send_sem, recv_sem, base=1)) for here in (top_plane, upper & (stage < middle + 2))]
    pl.when(upper)(mine.wait)
    for here, steps in ways:
        pl.when(here)(functools.partial(next, steps))

    rows, width = table.shape
    flatten(labels, lab)
    lab[:] = lab[:] - tp * rows
    pieces = len(e_bufs)
    pair = e_bufs[0].shape[1]

    def logit_chunk(b, start, count):
        logits = contract(table[pl.ds(start, count), :], n_buf[b * pair:(b + 1) * pair, :], 1, 1)
        e_bufs[b][pl.ds(start, count), :] = logits
        return fold(jnp.max, logits)

    def exp_chunk(b, start, count, top_b, total, hits):
        logits = e_bufs[b][pl.ds(start, count), :]
        label = jnp.concatenate([lab[p:p + 1, :] for p in range(b * pair // group, (b + 1) * pair // group)], axis=1)
        hit = label == start + lax.broadcasted_iota(jnp.int32, logits.shape, 0)
        e = jnp.exp(logits - top_b)
        e_bufs[b][pl.ds(start, count), :] = e
        return total + fold(jnp.sum, e), hits + fold(jnp.sum, jnp.where(hit, logits, 0.0))

    top_b = None
    zero = jnp.zeros((8, pair), F32)
    for b in range(pieces + 1):
        def both(start, count, carry, b=b, top_b=top_b):
            best, total, hits = carry
            if b < pieces:
                best = jnp.maximum(best, logit_chunk(b, start, count))
            if b > 0:
                total, hits = exp_chunk(b - 1, start, count, top_b, total, hits)
            return best, total, hits

        carry = (jnp.full((8, pair), -jnp.inf, F32), zero, zero)
        best, total, hits = lax.fori_loop(0, rows // chunk, lambda c, carry: both(pl.multiple_of(c * chunk, 8), chunk, carry), carry)
        if b > 0:
            lse = top_b + jnp.log(jnp.sum(total, axis=0, keepdims=True))
            hits = jnp.sum(hits, axis=0, keepdims=True)
            for i in range(pair // group):
                p = (b - 1) * (pair // group) + i
                stat[0, p:p + 1, :] = lse[:, i * group:(i + 1) * group]
                stat[1, p:p + 1, :] = hits[:, i * group:(i + 1) * group]
                peak[p:p + 1, :] = top_b[:, i * group:(i + 1) * group]
        if b < pieces:
            top_b = jnp.max(best, axis=0, keepdims=True)
        if b in (2, 3):
            pl.when(top_plane)(functools.partial(next, ways[0][1]))
        if b == pieces - 1:
            pl.when(ways[1][0])(functools.partial(next, ways[1][1]))

    def msg(d, kind):
        return remote(stat.at[kind], shared.at[kind, tp], share_send.at[kind], share_recv.at[kind], {'tp': lax.rem(tp + d, size)})

    for kind in BOTH:
        for d in range(1, size):
            msg(d, kind).start()
        shared[kind, tp] = stat[kind]

    def shares(kind):
        ref = shared.at[kind, pl.ds(0, size - 1)]
        return remote(ref, ref, share_send.at[kind], share_recv.at[kind], {'tp': plane.at(1, 0)})

    shares(0).wait_recv()
    every = shared[0]
    most = jnp.max(every, axis=0)
    log_norm = most + jnp.log(jnp.sum(jnp.exp(every - most[None]), axis=0))
    scale_ref[:] = jnp.exp(peak[:] - log_norm)

    def grad_block(p, slot):
        e_ref = e_bufs[p // (pair // group)]
        col = p % (pair // group) * group

        def part(start, count):
            e = e_ref[pl.ds(start, count), col:col + group]
            hit = lab[p:p + 1, :] == start + lax.broadcasted_iota(jnp.int32, e.shape, 0)
            g_buf[slot, pl.ds(start, count), :] = (e * scale_ref[p:p + 1, :] - jnp.where(hit, 1.0, 0.0)).astype(BF16)

        @pl.loop(0, rows // chunk)
        def _(c):
            part(pl.multiple_of(c * chunk, 8), chunk)

    def save(p):
        slot = 1 + p % 2
        return local(g_buf.at[slot], g_out.at[:, p * group:(p + 1) * group], loc_sem.at[2 + slot])

    for p in range(stages):
        pl.when(stage == p)(functools.partial(grad_block, p, 0))
    cut = rows // group * group
    red = Reduce(plane, parts, got_one, sum_one, got_two, one_send, one_recv, two_send, two_recv)
    mine_g = g_buf.at[0]
    half = width // 2
    for cols in tiles(width):
        back = contract(mine_g[:cut, :], table[:cut, cols], 0, 0) + contract(mine_g[cut:, :], table[cut:, cols], 0, 0)
        parts[:, :, :, cols] = back.reshape(*parts.shape[:-1], TILE)
        if cols.stop % half == 0:
            red.begin(cols.start // half)
    for p in range(stages):
        if p >= 2:
            save(p - 2).wait()
        grad_block(p, 1 + p % 2)
        save(p).start()
    red.middle()
    sums = red.end()

    @pl.when(stage != target)
    def _():
        remote(own_x, own_x, own_recv, own_recv, spread.mate).wait_recv()

    inv_rms, normed = norm_of(own_x[:])
    mean = (jnp.sum(normed[:, :half] * sums[0], axis=-1, keepdims=True) + jnp.sum(normed[:, half:] * sums[1], axis=-1, keepdims=True)) / width
    for h in BOTH:
        piece[:, h * half:(h + 1) * half] = (inv_rms * (sums[h] - normed[:, h * half:(h + 1) * half] * mean)).astype(BF16)

    def line(p):
        return remote(piece, g_top.at[p], line_send, line_recv, {'pp': target})

    @pl.when(stage != target)
    def _():
        line(stage).start()

    for here, steps in ways:
        pl.when(here)(functools.partial(drain, steps))

    save_x = local(x_all, x_out, loc_sem.at[2])
    pl.when(upper)(save_x.start)

    @pl.when(stage == target)
    def _():
        g_top[target] = piece[:]
        got = g_top.at[pl.ds(0, len(others))]
        remote(got, got, line_send, line_recv, spread.mate).wait_recv()

    red.close()
    pl.when(upper)(save_x.wait)
    shares(1).wait_recv()
    loss_out[:] = jnp.sum(log_norm - jnp.sum(shared[1], axis=0), keepdims=True) / (stages * group)
    for kind in BOTH:
        shares(kind).wait_send()
    save_n.wait()
    save(stages - 2).wait()
    save(stages - 1).wait()
    spread.close()

    @pl.when(stage == target)
    def _():
        sent = y_ref.at[pl.ds(0, len(others) * unit)]
        remote(sent, sent, own_send, own_recv, spread.mate).wait_send()

    @pl.when(stage != target)
    def _():
        line(stage).wait_send()


def backward_kernel(last, middle, chunk, g_top, hid_in, one_all, two_all, g_all, n_all, x_in, x_mid, w_one, w_two, de_buf, dx_all, grad_one, grad_two,
                    ones, twos, slope_ref, g_buf, n_buf, x_all, w_one_buf, w_two_buf, dy_all, dy_buf, dx_buf, d_buf,
                    send_sem, recv_sem, spread_send, spread_recv, die_send, die_recv, hop_send, hop_recv, go_sem, ready_sem, g_sem, loc_sem):
    plane = Plane()
    stage = lax.axis_index('pp')
    stages = last + 1
    blocks, cols, width = one_all.shape
    pairs = ((hid_in, slope_ref), (two_all, twos), (one_all, ones), (n_all, n_buf), (w_one, w_one_buf), (w_two, w_two_buf))
    loads = [local(src, dst, loc_sem.at[i]) for i, (src, dst) in enumerate(pairs)]
    lower = stage < middle
    load_x = [local(src, x_all, loc_sem.at[6]) for src in (x_in, x_mid)]

    def load_rest(at):
        for load in loads[3:] + [load_x[at]]:
            load.start()

    for load in loads[:3]:
        load.start()
    pl.when(lower)(functools.partial(load_rest, 0))
    spread = Spread(plane, 0, stages, dx_buf, dx_all, spread_send, spread_recv, die_send, die_recv)
    near = plane.near()
    for peer in near:
        signal(peer)
    extra = spread.greet()
    before = {'pp': lax.rem(stage + last, stages)}
    pl.when(stage > 0)(functools.partial(signal, before))
    hop = remote(dx_buf, dy_buf, hop_send, hop_recv, before)
    rows = de_buf.shape[0]
    pieces = -(-rows // chunk)

    def piece_at(c):
        return pl.ds(pl.multiple_of(jnp.minimum(c * chunk, rows - chunk), 8), chunk)

    def fetch(c):
        slot = lax.rem(c, 2)
        return local(g_all.at[piece_at(c)], g_buf.at[slot], g_sem.at[slot])

    def table(lo, hi):
        if lo == 0:
            fetch(0).start()
            loads[3].wait()

        @pl.loop(lo, hi)
        def _(c):
            @pl.when(c < pieces - 1)
            def _():
                fetch(c + 1).start()

            fetch(c).wait()
            de_buf[piece_at(c), :] = jnp.dot(g_buf[lax.rem(c, 2)], n_buf[:], preferred_element_type=F32)

    pl.when(lower)(functools.partial(table, 0, pieces))
    pl.semaphore_wait(pltpu.get_barrier_semaphore(), len(near) + extra + jnp.where(stage < last, 1, 0))

    @pl.when(stage < last)
    def _():
        pl.semaphore_signal(ready_sem, inc=1, device_id={'pp': lax.rem(stage + 1, stages)}, device_id_type=MESH)

    loads[0].wait()
    for k in range(blocks):
        slope_ref[k] = gelu_slope(slope_ref[k])
    loads[1].wait()

    @pl.when(stage == last)
    def _():
        dy_buf[:] = g_top[:]

    pl.when(stage < last)(hop.wait_recv)
    dy_all[plane.tp] = dy_buf[:]
    whole = (dy_all, 0, dy_all.shape[1])
    part = (dx_all, spread.lo, spread.rows)

    def dy_steps(begun):
        return plane_gather(plane, [whole], send_sem, recv_sem, base=1, begun=begun)

    @pl.when(stage <= 1)
    def _():
        next(dy_steps(False))

    grad_y = dy_buf[:]
    for k in range(blocks):
        grad_gate = jnp.dot(grad_y, twos[k], preferred_element_type=F32)
        d_buf[:, k * cols:(k + 1) * cols] = (slope_ref[k] * grad_gate).astype(BF16)
    loads[2].wait()
    grad_hidden = d_buf[:]
    for tile in tiles(width):
        back = jnp.dot(grad_hidden, ones[:, :, tile].reshape(blocks * cols, TILE), preferred_element_type=F32)
        dx_buf[:, tile] = (dy_buf[:, tile].astype(F32) + back).astype(BF16)

    @pl.when(stage > 0)
    def _():
        pl.semaphore_wait(ready_sem, 1)
        hop.start()

    pl.when(stage == 0)(spread.send)
    pl.when(jnp.logical_not(lower))(functools.partial(load_rest, 1))
    for load in loads[4:]:
        load.wait()
    load_x[0].wait()

    grad_one[:] = jnp.zeros_like(grad_one)
    grad_two[:] = jnp.zeros_like(grad_two)

    def weights(lo, hi):
        step = SIDE

        @pl.loop(lo, hi)
        def _(c):
            part = pl.ds(c * step, step)
            x_act = x_all[part].reshape(step * x_all.shape[1], width)
            grad_y = dy_all[part].reshape(step * x_all.shape[1], width)
            hidden = jnp.dot(x_act, w_one_buf[:], preferred_element_type=F32)
            grad_gate = contract(grad_y, w_two_buf[:], 1, 1)
            grad_hidden = (gelu_slope(hidden) * grad_gate).astype(BF16)
            grad_one[:] += contract(x_act, grad_hidden, 0, 0)
            grad_two[:] += contract(gelu(hidden).astype(BF16), grad_y, 0, 0)

    def dx_steps():
        return plane_gather(plane, [part], send_sem, recv_sem, spread.on_block)

    @pl.when(stage > 1)
    def _():
        hop.wait_send()

        @pl.when(spread.core == 0)
        def _():
            pl.semaphore_signal(go_sem, inc=1, device_id=spread.mate, device_id_type=MESH)

        @pl.when(spread.core == 1)
        def _():
            pl.semaphore_wait(go_sem, 1)

        next(dy_steps(False))

    @pl.when(jnp.logical_not(lower))
    def _():
        steps = dy_steps(True)
        for lo in range(0, pieces, 3):
            next(steps)
            table(lo, min(lo + 3, pieces))
            next(steps)
        drain(steps)

    planes = [(stage <= 1, 'dxddxdxdxdx', 'xx'), ((stage > 1) & lower, 'dddxdxdxdx', 'xxx')]
    runs = []
    for here, order, rest in planes:
        steps = {'d': dy_steps(True), 'x': dx_steps()}

        def arrived(order=order, steps=steps):
            for i, kind in enumerate(order):
                if kind == 'x' and 'x' not in order[:i]:
                    pl.when(stage > 0)(spread.arrive)
                next(steps[kind])
            drain(steps['d'])

        def onward(rest=rest, steps=steps):
            for kind in rest:
                next(steps[kind])

        pl.when(here)(arrived)
        runs.append((here, onward, functools.partial(drain, steps['x'])))

    weights(0, 2)
    for here, onward, _ in runs:
        pl.when(here)(onward)
    weights(2, SIDE)
    for here, _, finish in runs:
        pl.when(here)(finish)

    @pl.when(jnp.logical_not(lower))
    def _():
        spread.arrive()
        drain(dx_steps())

    spread.finish()
    spread.close()

    pl.when(stage == 1)(hop.wait_send)


def add_kernel(pieces, order, dx_ref, de_ref, one_ref, two_ref, de_out, table_out, one_out, two_out, wide, sem):
    saves = [local(one_ref, one_out, sem.at[0]), local(two_ref, two_out, sem.at[1])]
    for save in saves:
        save.start()
    wide[:] = dx_ref[:].astype(F32)

    @pl.loop(0, order[2, 0])
    def _(j):
        row = pl.ds(order[1, j], 1)
        de_out[row, :] = de_out[row, :] + wide[pl.ds(order[0, j], 1), :]

    rows = de_ref.shape[0]
    size = -(-rows // (8 * pieces)) * 8
    for c in range(pieces):
        part = pl.ds(c * size, min(size, rows - c * size))
        saves.append(local(de_out.at[part], table_out.at[part], sem.at[2 + c]))
        saves[-1].start()
    for save in saves:
        save.wait()


def vmem():
    return pl.BlockSpec(memory_space=pltpu.VMEM)


def anywhere():
    return pl.BlockSpec(memory_space=pl.ANY)


def params(cid, mib):
    return pltpu.CompilerParams(collective_id=cid, has_side_effects=True, vmem_limit_bytes=mib << 20)


DMA = pltpu.SemaphoreType.DMA


def solution(mesh):
    pp_size = mesh.shape['pp']
    tp_size = mesh.shape['tp']
    last = pp_size - 1

    def device_fn(tokens, labels, emb_table, w_in, w_out):
        num_tokens = tokens.shape[0] * tokens.shape[1]
        vocab_rows, width = emb_table.shape
        w_one, w_two = w_in[0], w_out[0]
        cols = w_one.shape[1]
        unit = num_tokens // (pp_size * tp_size)
        block = pp_size * unit
        group = tp_size * unit
        half = width // 2
        chunk = vocab_rows // 3
        step = 512
        pair = 2 * group
        shape = jax.ShapeDtypeStruct
        VM = pltpu.VMEM

        def reduce_scratch(dtype):
            return [VM((SIDE, SIDE, unit, width), dtype), VM((6, SIDE, unit, half), dtype), VM((2, SIDE, unit, half), dtype), VM((6, unit, half), dtype), VM((unit, width), BF16)]

        reduce_sems = [DMA, DMA((2,)), DMA, DMA((2,)), DMA, DMA]
        many = shape((tp_size, block, width), BF16)
        many_buf = VM((tp_size, block, width), BF16)
        two_sums = 2 * SLOTS

        y_act, order, hidden, one_t, two_t, x_all = pl.pallas_call(
            functools.partial(forward_kernel, last),
            out_shape=(shape((block, width), BF16), shape((3, num_tokens), jnp.int32), shape((tp_size, block, cols), F32), shape((tp_size, cols, width), BF16), shape((tp_size, width, cols), BF16), many),
            in_specs=[vmem()] + [anywhere()] * 3,
            out_specs=[vmem()] * 2 + [anywhere()] * 4,
            scratch_shapes=[VM((tp_size, width, cols), BF16), VM((tp_size, cols, width), BF16), VM((tp_size, cols, width), BF16), VM((tp_size, width, cols), BF16),
                            VM((vocab_rows, width), BF16), VM((vocab_rows, group), BF16), *reduce_scratch(BF16),
                            VM((block, width), BF16), VM((block, width), BF16), VM((block, tp_size * cols), BF16), VM((tp_size, block, cols), F32), many_buf, VM((1, group), jnp.int32),
                            VM((num_tokens // 128, 128), jnp.int32), VM((2, num_tokens), jnp.int32),
                            DMA((3,)), DMA((3 * two_sums,)), *reduce_sems, DMA, DMA, DMA((7,))],
            compiler_params=params(1, 58), name='forward_chain',
        )(tokens, emb_table, w_one, w_two)

        spread_sems = [DMA, DMA, DMA, DMA]
        middle = pp_size // 2
        loss, g_top, g_all, n_all, x_mid = pl.pallas_call(
            functools.partial(head_kernel, last, pp_size, middle, chunk),
            out_shape=(shape((1, 1), F32), shape((pp_size, unit, width), BF16), shape((vocab_rows, num_tokens), BF16), shape((num_tokens, width), BF16), many),
            in_specs=[anywhere(), vmem(), vmem(), anywhere()],
            out_specs=[vmem()] * 2 + [anywhere()] * 3,
            scratch_shapes=[VM((vocab_rows, width), BF16), many_buf, VM((unit, width), BF16), VM((block, width), BF16), VM((num_tokens, width), BF16),
                            many_buf, VM((pp_size, group), jnp.int32), VM((3, vocab_rows, group), BF16),
                            VM((pp_size, group), F32), VM((2, pp_size, group), F32), VM((2, tp_size, pp_size, group), F32), VM((pp_size, group), F32), *reduce_scratch(F32),
                            DMA((2,)), DMA((2 * two_sums,)), DMA((2,)), DMA((2,)), DMA, DMA, *spread_sems, *reduce_sems, DMA((5,)),
                            *[VM((vocab_rows, pair), F32) for _ in range(num_tokens // pair)]],
            compiler_params=params(2, 60), name='head',
        )(emb_table, y_act, labels, x_all)

        de_head, dx_first, grad_one, grad_two = pl.pallas_call(
            functools.partial(backward_kernel, last, middle, step),
            out_shape=(VM((vocab_rows, width), F32), many_buf, VM((width, cols), F32), VM((cols, width), F32)),
            in_specs=[vmem()] + [anywhere()] * 9, out_specs=[vmem()] * 4,
            scratch_shapes=[VM((tp_size, cols, width), BF16), VM((tp_size, width, cols), BF16), VM((tp_size, block, cols), F32), VM((2, step, num_tokens), BF16), VM((num_tokens, width), BF16),
                            many_buf, VM((width, cols), BF16), VM((cols, width), BF16), many_buf,
                            VM((block, width), BF16), VM((block, width), BF16), VM((block, tp_size * cols), BF16),
                            DMA((3,)), DMA((3 * two_sums,)), *spread_sems, DMA, DMA, pltpu.SemaphoreType.REGULAR, pltpu.SemaphoreType.REGULAR, DMA((2,)), DMA((7,))],
            compiler_params=params(3, 44), name='backward_chain',
        )(g_top.reshape(block, width), hidden, one_t, two_t, g_all, n_all, x_all, x_mid, w_one, w_two)

        smem = pl.BlockSpec(memory_space=pltpu.SMEM)
        _, grad_table, grad_one, grad_two = pl.pallas_call(
            functools.partial(add_kernel, 12),
            out_shape=(VM((vocab_rows, width), F32), shape((vocab_rows, width), F32), shape((width, cols), F32), shape((cols, width), F32)),
            in_specs=[smem] + [vmem()] * 4, out_specs=[vmem()] + [anywhere()] * 3,
            scratch_shapes=[VM((num_tokens, width), F32), DMA((14,))], input_output_aliases={2: 0},
            compiler_params=pltpu.CompilerParams(vmem_limit_bytes=24 << 20), name='add_rows',
        )(order, dx_first.reshape(num_tokens, width), de_head, grad_one, grad_two)
        return loss.reshape(1), grad_one[None], grad_two[None], grad_table

    return jax.shard_map(device_fn, mesh=mesh, in_specs=(P('dp', None), P('dp', None), P('tp', None), P('pp', None, 'tp'), P('pp', 'tp', None)), out_specs=(P('dp'), P(('dp', 'pp'), None, 'tp'), P(('dp', 'pp'), 'tp', None), P(('dp', 'tp'), None)), check_vma=False)
```

```python
import functools

import jax
import jax.numpy as jnp
from jax import lax
from jax.experimental import pallas as pl
from jax.experimental.pallas import tpu as pltpu
from jax.sharding import PartitionSpec as P

NORM_EPS = 1e-6
SIDE = 4
MESH = pl.DeviceIdType.MESH
F32 = jnp.float32
BF16 = jnp.bfloat16
CUBE = 0.044715
ROOT = 0.7978845608028654


def dot(lhs, rhs):
    return jnp.dot(lhs, rhs, preferred_element_type=F32)


def rows_dot(lhs, rhs):
    return lax.dot_general(lhs, rhs, (((0,), (0,)), ((), ())), preferred_element_type=F32)


def cols_dot(lhs, rhs):
    return lax.dot_general(lhs, rhs, (((1,), (1,)), ((), ())), preferred_element_type=F32)


def gelu(h):
    return h * (0.5 * (1.0 + jnp.tanh(ROOT * (h + CUBE * (h * h * h)))))


def gelu_slope(h):
    sq = h * h
    t = jnp.tanh(ROOT * (h + CUBE * (sq * h)))
    return 0.5 * (1.0 + t) + (0.5 * h) * (1.0 - t * t) * (ROOT * (1.0 + (3.0 * CUBE) * sq))


def remote(src, dst, send, recv, where):
    return pltpu.make_async_remote_copy(src_ref=src, dst_ref=dst, send_sem=send, recv_sem=recv, device_id=where, device_id_type=MESH)


def signal(peer):
    pl.semaphore_signal(pltpu.get_barrier_semaphore(), inc=1, device_id=peer, device_id_type=MESH)


class Plane:
    def __init__(self):
        self.tp = lax.axis_index('tp')
        self.y = lax.rem(self.tp, SIDE)
        self.z = self.tp // SIDE

    def at(self, dy, dz):
        return lax.rem(self.z + dz + SIDE, SIDE) * SIDE + lax.rem(self.y + dy + SIDE, SIDE)

    def blk(self, half, df, ds):
        return self.at(df, ds) if half == 0 else self.at(ds, df)

    def near(self):
        return [{'tp': self.at(1, 0)}, {'tp': self.at(-1, 0)}, {'tp': self.at(0, 1)}, {'tp': self.at(0, -1)}]

    def rings(self):
        return [{'tp': self.at(d, 0)} for d in (1, 2, 3)] + [{'tp': self.at(0, d)} for d in (1, 2, 3)]


HOPS = (0, -1, 1, 2)
WALK = ((0, -1, None, 1), (0, 1, None, -1), (-1, 2, 0, 1), (1, 2, 1, -1))
BOTH = (0, 1)
TILE = 256
SLOTS = 15


def plane_gather(plane, bufs, send_sem, recv_sem, on_block=lambda *_: None, base=0, begun=False):
    def msg(a, half, slot, block, part, to):
        buf, start, size = bufs[a]
        size = size // 2
        start = start + half * size
        if part is not None:
            size = size // 2
            start = start + part * size
        ref = buf.at[plane.blk(half, *block), pl.ds(start, size)]
        return remote(ref, ref, send_sem.at[base + a], recv_sem.at[((base + a) * 2 + half) * SLOTS + slot], {'tp': plane.blk(half, *to)})

    def f(a, half, k, end):
        step = WALK[k]
        return msg(a, half, min(k, 2), (step[end], 0), None if end and k > 1 else step[2], (step[3], 0))

    def s(a, half, j, k, end):
        step = WALK[k]
        return msg(a, half, 3 * (j + 1) + min(k, 2), (HOPS[j], step[end]), None if end and k > 1 else step[2], (0, step[3]))

    send, recv = BOTH
    pairs = [(a, half) for a in range(len(bufs)) for half in BOTH]

    def across(a, half, j):
        for k in BOTH:
            s(a, half, j, k, send).start()
        on_block(a, half, j, 0)

    def onward(a, half, j):
        for k in BOTH:
            s(a, half, j, k, recv).wait_recv()
            s(a, half, j, k + 2, send).start()
            on_block(a, half, j, k + 1)

    if not begun:
        for pair in pairs:
            for k in BOTH:
                f(*pair, k, send).start()
            across(*pair, 0)
        yield
    for pair in pairs:
        for k in BOTH:
            f(*pair, k, recv).wait_recv()
            f(*pair, k + 2, send).start()
            across(*pair, k + 1)
    yield
    for pair in pairs:
        onward(*pair, 0)
    yield
    for pair in pairs:
        f(*pair, 2, recv).wait_recv()
        across(*pair, SIDE - 1)
    yield
    for j in range(1, SIDE):
        for pair in pairs:
            onward(*pair, j)
        yield
    for j in range(SIDE):
        for pair in pairs:
            s(*pair, j, 2, recv).wait_recv()
            on_block(*pair, j, SIDE - 1)
    for a, (buf, start, size) in enumerate(bufs):
        sent = buf.at[pl.ds(0, SIDE * SIDE - 1), pl.ds(start, size)]
        remote(sent, sent, send_sem.at[base + a], recv_sem.at[0], {'tp': plane.at(1, 0)}).wait_send()


def tiles(width):
    return [slice(n, n + TILE) for n in range(0, width, TILE)]


def drain(steps):
    for _ in steps:
        pass


def local(src, dst, sem):
    return pltpu.make_async_copy(src, dst, sem)


class Reduce:
    def __init__(self, plane, parts, got_one, sum_one, got_two, one_send, one_recv, two_send, two_recv):
        self.plane, self.parts, self.got_one, self.sum_one, self.got_two = plane, parts, got_one, sum_one, got_two
        self.one_send, self.one_recv, self.two_send, self.two_recv = one_send, one_recv, two_send, two_recv

    def row(self, half, index):
        size = self.parts.shape[3] // 2
        cols = pl.ds(half * size, size)
        return self.parts.at[:, index, :, cols] if half == 0 else self.parts.at[index, :, :, cols]

    def here(self, half):
        return (self.plane.y, self.plane.z) if half == 0 else (self.plane.z, self.plane.y)

    def first(self, half, d):
        n = half * 3 + d - 1
        dest = lax.rem(self.here(half)[0] + d, SIDE)
        return remote(self.row(half, dest), self.got_one.at[n], self.one_send, self.one_recv.at[half], {'tp': self.plane.blk(half, d, 0)})

    def second(self, half, d):
        n = half * 3 + d - 1
        dest = lax.rem(self.here(half)[1] + d, SIDE)
        return remote(self.sum_one.at[half, dest], self.got_two.at[n], self.two_send, self.two_recv.at[half], {'tp': self.plane.blk(half, 0, d)})

    def whole(self, got, send, recv, half=None):
        ref = got if half is None else got.at[pl.ds(half * 3, 3)]
        return remote(ref, ref, send, recv.at[half or 0], {'tp': self.plane.at(1, 0)})

    def begin(self, half):
        for d in (2, 1, 3):
            self.first(half, d).start()

    def middle(self):
        for half in BOTH:
            total = self.row(half, self.here(half)[0])[:].astype(F32)
            self.whole(self.got_one, self.one_send, self.one_recv, half).wait_recv()
            for d in (1, 3, 2):
                total = total + self.got_one[half * 3 + d - 1].astype(F32)
            self.sum_one[half] = total.astype(self.sum_one.dtype)
            for d in (2, 1, 3):
                self.second(half, d).start()

    def end(self):
        sums = []
        for half in BOTH:
            total = self.sum_one[half, self.here(half)[1]].astype(F32)
            self.whole(self.got_two, self.two_send, self.two_recv, half).wait_recv()
            for d in (1, 3, 2):
                total = total + self.got_two[half * 3 + d - 1].astype(F32)
            sums.append(total)
        return sums

    def close(self):
        self.whole(self.got_one, self.one_send, self.one_recv).wait_send()
        self.whole(self.got_two, self.two_send, self.two_recv).wait_send()


def fold(op, value):
    rows, cols = value.shape
    return op(value.reshape(rows // 8, 8, cols), axis=0)


def flatten(ids, flat):
    size, cols = ids.shape[1], flat.shape[1]
    for r in range(ids.shape[0]):
        at = r * size
        flat[at // cols:at // cols + 1, at % cols:at % cols + size] = ids[r:r + 1, :]


def list_rows(tokens, base, rows, group, unit, flat, slot, out):
    lines, lanes = flat.shape
    count = lines * lanes
    flatten(tokens, flat)
    row = flat[:] - base
    mine = (row >= 0) & (row < rows)
    upper = lax.broadcasted_iota(jnp.int32, (lanes, lanes), 0) <= lax.broadcasted_iota(jnp.int32, (lanes, lanes), 1)
    ones = [jnp.where(mask, 1.0, 0.0).astype(BF16) for mask in (mine, upper)]
    seen = dot(*ones)
    total = jnp.zeros((1, 1), F32)
    for r in range(lines):
        line = slice(r, r + 1)
        here = slice(r * lanes, (r + 1) * lanes)
        slot[:1, here] = jnp.where(mine[line], seen[line] + (total - 1.0), -1.0).astype(jnp.int32)
        slot[1:, here] = row[line]
        total = total + seen[line, lanes - 1:]
    number = lax.broadcasted_iota(jnp.int32, (1, count), 1)
    inner = lax.rem(number, group)
    place = inner // unit * (count // group * unit) + number // group * unit + lax.rem(number, unit)
    digits = [part for value in (place, slot[1:, :]) for part in (value // 256, lax.rem(value, 256))]
    which = lax.broadcasted_iota(jnp.int32, (16, count), 0)
    values = sum(jnp.where(which == i, digit, 0) for i, digit in enumerate(digits)).astype(F32).astype(BF16)

    @pl.loop(0, count // group)
    def _(c):
        start = pl.multiple_of(c * group, group)
        pick = jnp.where(slot[:1, :] == start + lax.broadcasted_iota(jnp.int32, (group, count), 0), 1.0, 0.0).astype(BF16)
        found = cols_dot(values, pick)
        for i in BOTH:
            out[i:i + 1, pl.ds(start, group)] = (found[2 * i:2 * i + 1] * 256.0 + found[2 * i + 1:2 * i + 2]).astype(jnp.int32)

    out[2:, :] = jnp.broadcast_to(total, (1, count)).astype(jnp.int32)


def forward_kernel(last, tokens, emb, w_one, w_two, y_out, order_out, hid_out, one_out, two_out, x_out, ones, twos, one_t, two_t, table, hot, parts,
                   got_one, sum_one, got_two, piece, x_buf, y_buf, a_buf, hid_ref, x_all, ids, flat, slot,
                   send_sem, recv_sem, one_send, one_recv, two_send, two_recv, line_send, line_recv, hop_send, hop_recv, lead_sem, loc_sem):
    plane = Plane()
    stage = lax.axis_index('pp')
    tp = plane.tp
    stages = last + 1
    core = lax.rem(stage, 2)
    moves = ((emb, table), (w_one, ones.at[tp]), (w_two, twos.at[tp]), (one_t, one_out), (two_t, two_out), (hid_ref, hid_out), (x_all, x_out))
    load, own_one, own_two, *saves = [local(src, dst, loc_sem.at[i]) for i, (src, dst) in enumerate(moves)]
    save_one, save_two, save_hid, save_x = saves
    load.start()
    own_one.start()
    own_two.start()
    for peer in plane.rings() + [{'pp': lax.rem(stage + d, stages)} for d in range(1, stages)]:
        signal(peer)

    own_one.wait()
    own_two.wait()
    pl.semaphore_wait(pltpu.get_barrier_semaphore(), 6 + last)
    def weight_steps(begun=False):
        return plane_gather(plane, [(ones, 0, ones.shape[1]), (twos, 0, twos.shape[1])], send_sem, recv_sem, begun=begun)

    @pl.when(core == 0)
    def _():
        next(weight_steps())

    rows, width = table.shape
    group = ids.shape[1]
    unit = piece.shape[0]
    count = group // tokens.shape[1]
    flatten(tokens.at[pl.ds(pl.multiple_of(stage * count, count), count)], ids)
    hot[:] = jnp.where(ids[:] - tp * rows == lax.broadcasted_iota(jnp.int32, hot.shape, 0), 1.0, 0.0).astype(BF16)
    load.wait()
    cut = rows // group * group
    for cols in tiles(width):
        picked = rows_dot(hot[:cut], table[:cut, cols]) + rows_dot(hot[cut:], table[cut:, cols])
        parts[:, :, :, cols] = picked.astype(BF16).reshape(*parts.shape[:-1], TILE)
    red = Reduce(plane, parts, got_one, sum_one, got_two, one_send, one_recv, two_send, two_recv)
    for half in BOTH:
        red.begin(half)

    @pl.when(core == 1)
    def _():
        pl.semaphore_wait(lead_sem, 1)
        next(weight_steps())

    gather = weight_steps(True)
    next(gather)

    @pl.when(core == 0)
    def _():
        pl.semaphore_signal(lead_sem, inc=1, device_id={'pp': stage + 1}, device_id_type=MESH)

    next(gather)
    red.middle()
    next(gather)
    next(gather)
    for half, total in enumerate(red.end()):
        piece[:, half * (width // 2):(half + 1) * (width // 2)] = total.astype(BF16)

    def line(p):
        return remote(piece, x_buf.at[pl.ds(pl.multiple_of(p * unit, unit), unit)], line_send, line_recv, {'pp': 0})

    @pl.when(stage != 0)
    def _():
        line(stage).start()

    @pl.when(stage == 0)
    def _():
        x_buf[:unit] = piece[:]

    drain(gather)

    @pl.when(stage == 1)
    def _():
        pl.semaphore_signal(lead_sem, inc=1, device_id={'pp': 0}, device_id_type=MESH)

    blocks, _, cols = ones.shape

    def spare_time():
        @pl.loop(0, blocks)
        def _(k):
            one_t[k] = ones[k].T
            two_t[k] = twos[k].T

        save_one.start()
        save_two.start()
        list_rows(tokens, tp * rows, rows, group, unit, flat, slot, order_out)

    pl.when(stage > 1)(spare_time)
    hop = remote(y_buf, x_buf, hop_send, hop_recv, {'pp': lax.rem(stage + 1, stages)})

    @pl.when(stage == 0)
    def _():
        got = x_buf.at[pl.ds(0, last * unit)]
        remote(got, got, line_send, line_recv, {'pp': last}).wait_recv()

    pl.when(stage > 0)(hop.wait_recv)
    x_act = x_buf[:]
    for k in range(blocks):
        hidden = dot(x_act, ones[k])
        hid_ref[k] = hidden
        a_buf[:, k * cols:(k + 1) * cols] = gelu(hidden).astype(BF16)
    save_hid.start()
    gate = a_buf[:]
    for tile in tiles(width):
        branch = dot(gate, twos[:, :, tile].reshape(blocks * cols, TILE))
        y_buf[:, tile] = (x_buf[:, tile].astype(F32) + branch).astype(BF16)

    pl.when(stage < last)(hop.start)
    y_out[:] = y_buf[:]
    x_all[tp] = x_buf[:]

    @pl.when(stage < SIDE)
    def _():
        pl.when(stage <= 1)(spare_time)

        @pl.when(stage == 0)
        def _():
            pl.semaphore_wait(lead_sem, 1)

        steps = plane_gather(plane, [(x_all, 0, x_all.shape[1])], send_sem, recv_sem, base=2)
        drain(steps)

    own_save = local(x_all.at[tp], x_out.at[tp], loc_sem.at[6])
    pl.when(stage < SIDE)(save_x.start)
    pl.when(stage >= SIDE)(own_save.start)
    red.close()

    @pl.when(stage != 0)
    def _():
        line(stage).wait_send()

    pl.when(stage < last)(hop.wait_send)
    for save in saves[:-1]:
        save.wait()
    pl.when(stage < SIDE)(save_x.wait)
    pl.when(stage >= SIDE)(own_save.wait)


def norm_of(x):
    wide = x.astype(F32)
    inv_rms = lax.rsqrt(jnp.mean(wide * wide, axis=-1, keepdims=True) + NORM_EPS)
    return inv_rms, wide * inv_rms


class Spread:
    def __init__(self, plane, source, stages, src, out, line_send, line_recv, die_send, die_recv):
        self.plane, self.source, self.stages, self.src, self.out = plane, source, stages, src, out
        self.line_send, self.line_recv, self.die_send, self.die_recv = line_send, line_recv, die_send, die_recv
        self.stage = lax.axis_index('pp')
        self.core = lax.rem(self.stage, 2)
        self.mate = {'pp': self.stage + 1 - 2 * self.core}
        self.rows = out.shape[1] // 2
        self.lo = pl.multiple_of(self.core * self.rows, self.rows)
        self.others = [p for p in range(stages) if p != source]

    def greet(self, back):
        source = self.stage == self.source
        twin = self.stage == self.source ^ 1

        @pl.when(source)
        def _():
            for p in self.others if back else [self.source ^ 1]:
                signal({'pp': p})

        @pl.when(jnp.logical_not(source))
        def _():
            signal({'pp': self.source})

        pl.when(jnp.logical_not(source | twin))(functools.partial(signal, self.mate))
        return jnp.where(source, len(self.others), jnp.where(twin, 1, 1 + back))

    def line(self, p):
        part = pl.ds((p % 2) * self.rows, self.rows)
        return remote(self.src.at[part], self.out.at[self.plane.tp, part], self.line_send, self.line_recv, {'pp': p})

    def send(self):
        for p in self.others:
            self.line(p).start()
        part = pl.ds(self.lo, self.rows)
        self.out[self.plane.tp, part] = self.src[part]

    def arrive(self):
        mine = self.out.at[self.plane.tp, pl.ds(self.lo, self.rows)]
        remote(mine, mine, self.line_recv, self.line_recv, self.mate).wait_recv()

    def on_block(self, a, half, j, k):
        if a == 0:
            size = self.rows // 2
            ref = self.out.at[self.plane.blk(half, HOPS[j], HOPS[k]), pl.ds(self.lo + half * size, size)]
            remote(ref, ref, self.die_send, self.die_recv, self.mate).start()

    def half(self, lo):
        ref = self.out.at[:, pl.ds(lo, self.rows)]
        return remote(ref, ref, self.die_send, self.die_recv, self.mate)

    def finish(self):
        self.half(pl.multiple_of((1 - self.core) * self.rows, self.rows)).wait_recv()

    def close(self):
        self.half(self.lo).wait_send()

        @pl.when(self.stage == self.source)
        def _():
            sent = self.out.at[pl.ds(0, len(self.others)), pl.ds(self.lo, self.rows)]
            remote(sent, sent, self.line_send, self.line_recv, self.mate).wait_send()


def head_kernel(target, stages, chunk, emb, y_ref, labels, loss_out, g_top, g_out, n_out,
                table, top, own_x, n_src, n_buf, lab, g_buf, peak, stat, shared, scale_ref, parts, got_one, sum_one, got_two, piece,
                send_sem, recv_sem, share_send, share_recv, own_send, own_recv, spread_send, spread_recv, die_send, die_recv,
                one_send, one_recv, two_send, two_recv, line_send, line_recv, loc_sem, *e_bufs):
    plane = Plane()
    stage = lax.axis_index('pp')
    tp = plane.tp
    size = shared.shape[1]
    others = [p for p in range(stages) if p != target]
    load = local(emb, table, loc_sem.at[0])
    load.start()
    spread = Spread(plane, target, stages, n_src, top, spread_send, spread_recv, die_send, die_recv)
    for d in range(1, size):
        signal({'tp': lax.rem(tp + d, size)})
    extra = spread.greet(1)
    n_src[:] = norm_of(y_ref[:])[1].astype(BF16)
    each, group = peak.shape[1:]
    unit = group // size
    pl.semaphore_wait(pltpu.get_barrier_semaphore(), size - 1 + extra)

    def own(p):
        return remote(y_ref.at[pl.ds(p * unit, unit)], own_x, own_send, own_recv, {'pp': p})

    @pl.when(stage == target)
    def _():
        spread.send()
        for p in others:
            own(p).start()
        own_x[:] = y_ref[target * unit:(target + 1) * unit]

    pl.when(stage != target)(spread.arrive)
    drain(plane_gather(plane, [(top, spread.lo, spread.rows)], send_sem, recv_sem, spread.on_block))
    spread.finish()
    for p in range(stages):
        n_buf[p * group:(p + 1) * group] = top[:, p * unit:(p + 1) * unit, :].reshape(group, top.shape[2])
    save_n = local(n_buf, n_out, loc_sem.at[1])
    save_n.start()
    load.wait()

    rows, width = table.shape
    flatten(labels, lab)
    lab[:] = lab[:] - tp * rows
    pieces = len(e_bufs)
    pair = each * group

    def group_at(b, i):
        return lax.rem(stage // each + b, pieces) * each + i

    def label_of(p):
        return lab[pl.ds(p, 1), :]

    def down(value, start):
        return start + lax.broadcasted_iota(jnp.int32, value.shape, 0)

    def logit_chunk(b, start):
        tokens = n_buf[pl.ds(pl.multiple_of(group_at(b, 0) * group, pair), pair), :]
        logits = cols_dot(table[pl.ds(start, chunk), :], tokens)
        e_bufs[b][pl.ds(start, chunk), :] = logits
        return fold(jnp.max, logits)

    def exp_chunk(b, start, label, top_b, total, hits):
        logits = e_bufs[b][pl.ds(start, chunk), :]
        e = jnp.exp(logits - top_b)
        e_bufs[b][pl.ds(start, chunk), :] = e
        return total + fold(jnp.sum, e), hits + fold(jnp.sum, jnp.where(label == down(logits, start), logits, 0.0))

    def chunks(body, carry):
        return lax.fori_loop(0, rows // chunk, lambda c, carry: body(pl.multiple_of(c * chunk, 8), carry), carry)

    def msg(d, k):
        some = pl.ds(k, 1 + k * (pieces - 2))
        return remote(stat.at[some], shared.at[some, tp], share_send.at[k], share_recv.at[k], {'tp': lax.rem(tp + d, size)})

    def shares(k):
        ref = shared.at[pl.ds(k, 1 + k * (pieces - 2)), pl.ds(0, size - 1)]
        return remote(ref, ref, share_send.at[k], share_recv.at[k], {'tp': plane.at(1, 0)})

    def share(k):
        for d in range(1, size):
            msg(d, k).start()

    losses = []

    def normalise(k):
        shares(k).wait_recv()
        for b in (range(1, pieces) if k else range(1)):
            every = shared[b, :, 0]
            most = jnp.max(every, axis=0)
            log_norm = most + jnp.log(jnp.sum(jnp.exp(every - most[None]), axis=0))
            losses.append(jnp.sum(log_norm - jnp.sum(shared[b, :, 1], axis=0), keepdims=True))
            scale_ref[b] = jnp.exp(peak[b] - log_norm)

    def grad_block(b, i, slot):
        cols = pl.ds(pl.multiple_of(i * group, group), group)
        label = label_of(group_at(b, i))
        factor = scale_ref[b, pl.ds(i, 1), :]

        def part(start, _):
            e = e_bufs[b][pl.ds(start, chunk), cols]
            hit = label == down(e, start)
            g_buf[slot, pl.ds(start, chunk), :] = (e * factor - jnp.where(hit, 1.0, 0.0)).astype(BF16)

        chunks(part, None)

    def save(k):
        slot = 1 + k % 2
        at = pl.multiple_of(group_at(k // each, k % each) * group, group)
        return local(g_buf.at[slot], g_out.at[:, pl.ds(at, group)], loc_sem.at[2 + slot])

    def gradient(k):
        if k >= 2:
            save(k - 2).wait()
        grad_block(k // each, k % each, 1 + k % 2)
        save(k).start()

    cut = rows // group * group
    half = width // 2
    red = Reduce(plane, parts, got_one, sum_one, got_two, one_send, one_recv, two_send, two_recv)

    def own_gradient():
        grad_block(0, lax.rem(stage, each), 0)
        mine_g = g_buf.at[0]
        for cols in tiles(width):
            back = rows_dot(mine_g[:cut, :], table[:cut, cols]) + rows_dot(mine_g[cut:, :], table[cut:, cols])
            parts[:, :, :, cols] = back.reshape(*parts.shape[:-1], TILE)
            if cols.stop % half == 0:
                red.begin(cols.start // half)

    tops = []
    zero = jnp.zeros((8, pair), F32)
    for now, done in ((0, None), (None, 0), (1, None), *((b, b - 1) for b in range(2, pieces)), (None, pieces - 1)):
        label = None if done is None else jnp.concatenate([label_of(group_at(done, i)) for i in range(each)], axis=1)
        top_b = None if done is None else tops[done]

        def both(start, carry, now=now, done=done, top_b=top_b, label=label):
            best, total, hits = carry
            if now is not None:
                best = jnp.maximum(best, logit_chunk(now, start))
            if done is not None:
                total, hits = exp_chunk(done, start, label, top_b, total, hits)
            return best, total, hits

        best, total, hits = chunks(both, (jnp.full((8, pair), -jnp.inf, F32), zero, zero))
        if done is not None:
            found = (top_b + jnp.log(jnp.sum(total, axis=0, keepdims=True)), jnp.sum(hits, axis=0, keepdims=True), top_b)
            for i in range(each):
                cols = slice(i * group, (i + 1) * group)
                for kind in BOTH:
                    stat[done, kind, i:i + 1, :] = found[kind][:, cols]
                peak[done, i:i + 1, :] = found[2][:, cols]
            shared[done, tp] = stat[done]
        if now is None:
            share(1 if done else 0)
        else:
            tops.append(jnp.max(best, axis=0, keepdims=True))
        if now == 1:
            normalise(0)
            own_gradient()
        if now == pieces - 1:
            red.middle()

    gradient(0)
    gradient(1)
    sums = red.end()

    @pl.when(stage != target)
    def _():
        remote(own_x, own_x, own_recv, own_recv, spread.mate).wait_recv()

    inv_rms, normed = norm_of(own_x[:])
    mean = (jnp.sum(normed[:, :half] * sums[0], axis=-1, keepdims=True) + jnp.sum(normed[:, half:] * sums[1], axis=-1, keepdims=True)) / width
    for h in BOTH:
        cols = slice(h * half, (h + 1) * half)
        piece[:, cols] = (inv_rms * (sums[h] - normed[:, cols] * mean)).astype(BF16)

    def line(p):
        return remote(piece, g_top.at[p], line_send, line_recv, {'pp': target})

    @pl.when(stage != target)
    def _():
        line(stage).start()

    normalise(1)
    for k in range(2, stages):
        gradient(k)
    loss_out[:] = sum(losses) / (stages * group)
    @pl.when(stage == target)
    def _():
        g_top[target] = piece[:]
        got = g_top.at[pl.ds(0, len(others))]
        remote(got, got, line_send, line_recv, spread.mate).wait_recv()

    red.close()
    for k in BOTH:
        shares(k).wait_send()
    save_n.wait()
    save(stages - 2).wait()
    save(stages - 1).wait()
    spread.close()

    @pl.when(stage == target)
    def _():
        sent = y_ref.at[pl.ds(0, len(others) * unit)]
        remote(sent, sent, own_send, own_recv, spread.mate).wait_send()

    @pl.when(stage != target)
    def _():
        line(stage).wait_send()


def backward_kernel(last, chunk, g_top, hid_in, two_all, one_all, g_all, n_all, x_in, w_one, w_two, de_buf, dx_all, grad_one, grad_two,
                    ones, twos, slope_ref, g_buf, n_buf, x_all, w_one_buf, w_two_buf, dy_all, dy_buf, dx_buf, d_buf,
                    send_sem, recv_sem, spread_send, spread_recv, die_send, die_recv, hop_send, hop_recv, go_sem, ready_sem, g_sem, loc_sem):
    plane = Plane()
    stage = lax.axis_index('pp')
    stages = last + 1
    blocks, cols, width = one_all.shape
    pairs = ((hid_in, slope_ref), (two_all, twos), (one_all, ones), (n_all, n_buf), (w_one, w_one_buf), (w_two, w_two_buf))
    loads = [local(src, dst, loc_sem.at[i]) for i, (src, dst) in enumerate(pairs)]
    lower = stage < SIDE
    upper = stage >= SIDE
    own = plane.tp
    load_x = [local(*pair, loc_sem.at[6]) for pair in ((x_in, x_all), (x_in.at[own], x_all.at[own]))]

    mid = upper & (stage < last - 1)

    def start(some):
        for load in some:
            load.start()

    pl.when(upper)(functools.partial(start, loads[:3]))
    pl.when(lower)(functools.partial(start, loads[3:4]))
    own_load = load_x[1]
    pl.when(mid)(own_load.start)
    spread = Spread(plane, 0, stages, dx_buf, dx_all, spread_send, spread_recv, die_send, die_recv)
    near = plane.near()
    for peer in near:
        signal(peer)
    extra = spread.greet(0)
    before = {'pp': lax.rem(stage + last, stages)}
    pl.when(stage > 0)(functools.partial(signal, before))
    hop = remote(dx_buf, dy_buf, hop_send, hop_recv, before)
    rows = de_buf.shape[0]
    pieces = -(-rows // chunk)

    def piece_at(c):
        return pl.ds(pl.multiple_of(jnp.minimum(c * chunk, rows - chunk), 8), chunk)

    def fetch(c):
        slot = lax.rem(c, 2)
        return local(g_all.at[piece_at(c)], g_buf.at[slot], g_sem.at[slot])

    def table(lo, hi):
        if lo == 0:
            fetch(0).start()
            loads[3].wait()

        @pl.loop(lo, hi)
        def _(c):
            @pl.when(c < pieces - 1)
            def _():
                fetch(c + 1).start()

            for i, some in enumerate((loads[:2], loads[2:3], loads[4:] + load_x[:1])):
                pl.when(lower & (c == i + 1))(functools.partial(start, some))

            fetch(c).wait()
            de_buf[piece_at(c), :] = dot(g_buf[lax.rem(c, 2)], n_buf[:])

    pl.semaphore_wait(pltpu.get_barrier_semaphore(), len(near) + extra + jnp.where(stage < last, 1, 0))

    @pl.when(stage < last)
    def _():
        pl.semaphore_signal(ready_sem, inc=1, device_id={'pp': lax.rem(stage + 1, stages)}, device_id_type=MESH)

    pl.when(lower)(functools.partial(table, 0, pieces))
    loads[0].wait()
    for k in range(blocks):
        slope_ref[k] = gelu_slope(slope_ref[k])
    loads[1].wait()

    def a_steps(begun=False):
        return plane_gather(plane, [(x_all, 0, x_all.shape[1])], send_sem, recv_sem, base=2, begun=begun)

    mid_steps = a_steps()

    @pl.when(mid)
    def _():
        own_load.wait()
        for _ in range(3):
            next(mid_steps)

    @pl.when(stage == last)
    def _():
        dy_buf[:] = g_top[:]

    pl.when(stage < last)(hop.wait_recv)
    dy_all[plane.tp] = dy_buf[:]
    whole = (dy_all, 0, dy_all.shape[1])
    part = (dx_all, spread.lo, spread.rows)

    def dy_steps(begun):
        return plane_gather(plane, [whole], send_sem, recv_sem, base=1, begun=begun)

    @pl.when(stage <= 1)
    def _():
        next(dy_steps(False))

    grad_y = dy_buf[:]
    for k in range(blocks):
        grad_gate = dot(grad_y, twos[k])
        d_buf[:, k * cols:(k + 1) * cols] = (slope_ref[k] * grad_gate).astype(BF16)
    loads[2].wait()
    grad_hidden = d_buf[:]
    for tile in tiles(width):
        back = dot(grad_hidden, ones[:, :, tile].reshape(blocks * cols, TILE))
        dx_buf[:, tile] = (dy_buf[:, tile].astype(F32) + back).astype(BF16)

    @pl.when(stage > 0)
    def _():
        pl.semaphore_wait(ready_sem, 1)
        hop.start()

    pl.when(stage == 0)(spread.send)
    pl.when(upper)(functools.partial(start, loads[3:]))
    pl.when(upper & jnp.logical_not(mid))(own_load.start)
    for load in loads[4:]:
        load.wait()
    pl.when(lower)(load_x[0].wait)
    pl.when(upper & jnp.logical_not(mid))(own_load.wait)

    grad_one[:] = jnp.zeros_like(grad_one)
    grad_two[:] = jnp.zeros_like(grad_two)

    def weights(lo, hi):
        step = SIDE

        @pl.loop(lo, hi)
        def _(c):
            part = pl.ds(c * step, step)
            x_act = x_all[part].reshape(step * x_all.shape[1], width)
            grad_y = dy_all[part].reshape(step * x_all.shape[1], width)
            hidden = dot(x_act, w_one_buf[:])
            grad_gate = cols_dot(grad_y, w_two_buf[:])
            grad_hidden = (gelu_slope(hidden) * grad_gate).astype(BF16)
            grad_one[:] += rows_dot(x_act, grad_hidden)
            grad_two[:] += rows_dot(gelu(hidden).astype(BF16), grad_y)

    def dx_steps():
        return plane_gather(plane, [part], send_sem, recv_sem, spread.on_block)

    @pl.when(stage > 1)
    def _():
        hop.wait_send()

        @pl.when(spread.core == 0)
        def _():
            pl.semaphore_signal(go_sem, inc=1, device_id=spread.mate, device_id_type=MESH)

        @pl.when(spread.core == 1)
        def _():
            pl.semaphore_wait(go_sem, 1)

    @pl.when(stage > 1)
    def _():
        next(dy_steps(False))

    @pl.when(upper & jnp.logical_not(mid))
    def _():
        next(a_steps())

    planes = [(stage <= 1, None, 'dxddxdxdxdx', 'xx'), ((stage > 1) & lower, None, 'dddxdxdxdx', 'xxx'),
              (mid, mid_steps, 'dtdadatdaxdaxdx', 'xxx'), (upper & jnp.logical_not(mid), a_steps(True), 'datdadatdaxdaxdax', 'xxx')]
    runs = []
    for here, more, order, rest in planes:
        steps = {'d': dy_steps(True), 'x': dx_steps(), 'a': more}

        def arrived(order=order, steps=steps):
            part = -(-pieces // 2)
            for i, kind in enumerate(order):
                if kind == 't':
                    lo = order[:i].count('t') * part
                    table(lo, min(lo + part, pieces))
                    continue
                if kind == 'x' and 'x' not in order[:i]:
                    pl.when(stage > 0)(spread.arrive)
                next(steps[kind])
            drain(steps['d'])
            drain(steps['a'] or ())

        def onward(rest=rest, steps=steps):
            for kind in rest:
                next(steps[kind])

        pl.when(here)(arrived)
        runs.append((here, onward, functools.partial(drain, steps['x'])))

    weights(0, 2)
    for here, onward, _ in runs:
        pl.when(here)(onward)
    weights(2, SIDE)
    for here, _, finish in runs:
        pl.when(here)(finish)

    spread.finish()
    spread.close()

    pl.when(stage == 1)(hop.wait_send)


def add_kernel(pieces, order, dx_ref, de_ref, one_ref, two_ref, de_out, table_out, one_out, two_out, wide, sem):
    saves = [local(one_ref, one_out, sem.at[0]), local(two_ref, two_out, sem.at[1])]
    for save in saves:
        save.start()
    wide[:] = dx_ref[:].astype(F32)

    @pl.loop(0, order[2, 0])
    def _(j):
        row = pl.ds(order[1, j], 1)
        de_out[row, :] = de_out[row, :] + wide[pl.ds(order[0, j], 1), :]

    rows = de_ref.shape[0]
    size = -(-rows // (8 * pieces)) * 8
    for c in range(pieces):
        part = pl.ds(c * size, min(size, rows - c * size))
        saves.append(local(de_out.at[part], table_out.at[part], sem.at[2 + c]))
        saves[-1].start()
    for save in saves:
        save.wait()


def vmem():
    return pl.BlockSpec(memory_space=pltpu.VMEM)


def anywhere():
    return pl.BlockSpec(memory_space=pl.ANY)


def params(cid, mib):
    return pltpu.CompilerParams(collective_id=cid, has_side_effects=True, vmem_limit_bytes=mib << 20)


DMA = pltpu.SemaphoreType.DMA


def solution(mesh):
    pp_size = mesh.shape['pp']
    tp_size = mesh.shape['tp']
    last = pp_size - 1

    def device_fn(tokens, labels, emb_table, w_in, w_out):
        num_tokens = tokens.shape[0] * tokens.shape[1]
        vocab_rows, width = emb_table.shape
        w_one, w_two = w_in[0], w_out[0]
        cols = w_one.shape[1]
        unit = num_tokens // (pp_size * tp_size)
        block = pp_size * unit
        group = tp_size * unit
        half = width // 2
        chunk = vocab_rows // 3
        step = 512
        pair = 2 * group
        shape = jax.ShapeDtypeStruct
        VM = pltpu.VMEM

        def reduce_scratch(dtype):
            return [VM((SIDE, SIDE, unit, width), dtype), VM((6, SIDE, unit, half), dtype), VM((2, SIDE, unit, half), dtype), VM((6, unit, half), dtype), VM((unit, width), BF16)]

        duo = DMA((2,))
        reduce_sems = [DMA, duo, DMA, duo, DMA, DMA]
        many = shape((tp_size, block, width), BF16)
        many_buf = VM((tp_size, block, width), BF16)
        two_sums = 2 * SLOTS
        gather_sems = [DMA((3,)), DMA((3 * two_sums,))]

        y_act, order, hidden, one_t, two_t, x_all = pl.pallas_call(
            functools.partial(forward_kernel, last),
            out_shape=(shape((block, width), BF16), shape((3, num_tokens), jnp.int32), shape((tp_size, block, cols), F32), shape((tp_size, cols, width), BF16), shape((tp_size, width, cols), BF16), many),
            in_specs=[vmem()] + [anywhere()] * 3,
            out_specs=[vmem()] * 2 + [anywhere()] * 4,
            scratch_shapes=[VM((tp_size, width, cols), BF16), VM((tp_size, cols, width), BF16), VM((tp_size, cols, width), BF16), VM((tp_size, width, cols), BF16),
                            VM((vocab_rows, width), BF16), VM((vocab_rows, group), BF16), *reduce_scratch(BF16),
                            VM((block, width), BF16), VM((block, width), BF16), VM((block, tp_size * cols), BF16), VM((tp_size, block, cols), F32), many_buf, VM((1, group), jnp.int32),
                            VM((num_tokens // 128, 128), jnp.int32), VM((2, num_tokens), jnp.int32),
                            *gather_sems, *reduce_sems, DMA, DMA, pltpu.SemaphoreType.REGULAR, DMA((7,))],
            compiler_params=params(1, 58), name='forward_chain',
        )(tokens, emb_table, w_one, w_two)

        spread_sems = [DMA, DMA, DMA, DMA]
        by_pair = (num_tokens // pair, pair // group, group)
        loss, g_top, g_all, n_all = pl.pallas_call(
            functools.partial(head_kernel, last, pp_size, chunk),
            out_shape=(shape((1, 1), F32), shape((pp_size, unit, width), BF16), shape((vocab_rows, num_tokens), BF16), shape((num_tokens, width), BF16)),
            in_specs=[anywhere(), vmem(), vmem()],
            out_specs=[vmem()] * 2 + [anywhere()] * 2,
            scratch_shapes=[VM((vocab_rows, width), BF16), many_buf, VM((unit, width), BF16), VM((block, width), BF16), VM((num_tokens, width), BF16),
                            VM((pp_size, group), jnp.int32), VM((3, vocab_rows, group), BF16),
                            VM(by_pair, F32), VM((by_pair[0], 2, *by_pair[1:]), F32), VM((by_pair[0], tp_size, 2, *by_pair[1:]), F32), VM(by_pair, F32), *reduce_scratch(F32),
                            *gather_sems, duo, duo, DMA, DMA, *spread_sems, *reduce_sems, DMA((5,)),
                            *[VM((vocab_rows, pair), F32) for _ in range(num_tokens // pair)]],
            compiler_params=params(2, 60), name='head',
        )(emb_table, y_act, labels)

        de_head, dx_first, grad_one, grad_two = pl.pallas_call(
            functools.partial(backward_kernel, last, step),
            out_shape=(VM((vocab_rows, width), F32), many_buf, VM((width, cols), F32), VM((cols, width), F32)),
            in_specs=[vmem()] + [anywhere()] * 8, out_specs=[vmem()] * 4,
            scratch_shapes=[VM((tp_size, cols, width), BF16), VM((tp_size, width, cols), BF16), VM((tp_size, block, cols), F32), VM((2, step, num_tokens), BF16), VM((num_tokens, width), BF16),
                            many_buf, VM((width, cols), BF16), VM((cols, width), BF16), many_buf,
                            VM((block, width), BF16), VM((block, width), BF16), VM((block, tp_size * cols), BF16),
                            *gather_sems, *spread_sems, DMA, DMA, pltpu.SemaphoreType.REGULAR, pltpu.SemaphoreType.REGULAR, duo, DMA((7,))],
            compiler_params=params(3, 45), name='backward_chain',
        )(g_top.reshape(block, width), hidden, two_t, one_t, g_all, n_all, x_all, w_one, w_two)

        smem = pl.BlockSpec(memory_space=pltpu.SMEM)
        _, grad_table, grad_one, grad_two = pl.pallas_call(
            functools.partial(add_kernel, 12),
            out_shape=(VM((vocab_rows, width), F32), shape((vocab_rows, width), F32), shape((width, cols), F32), shape((cols, width), F32)),
            in_specs=[smem] + [vmem()] * 4, out_specs=[vmem()] + [anywhere()] * 3,
            scratch_shapes=[VM((num_tokens, width), F32), DMA((14,))], input_output_aliases={2: 0},
            compiler_params=pltpu.CompilerParams(vmem_limit_bytes=24 << 20), name='add_rows',
        )(order, dx_first.reshape(num_tokens, width), de_head, grad_one, grad_two)
        return loss.reshape(1), grad_one[None], grad_two[None], grad_table

    return jax.shard_map(device_fn, mesh=mesh, in_specs=(P('dp', None), P('dp', None), P('tp', None), P('pp', None, 'tp'), P('pp', 'tp', None)), out_specs=(P('dp'), P(('dp', 'pp'), None, 'tp'), P(('dp', 'pp'), 'tp', None), P(('dp', 'tp'), None)), check_vma=False)
```

```python
import functools

import jax
import jax.numpy as jnp
from jax import lax
from jax.experimental import pallas as pl
from jax.experimental.pallas import tpu as pltpu
from jax.sharding import PartitionSpec as P

NORM_EPS = 1e-6
SIDE = 4
MESH = pl.DeviceIdType.MESH
F32 = jnp.float32
BF16 = jnp.bfloat16
CUBE = 0.044715
ROOT = 0.7978845608028654


def dot(lhs, rhs):
    return jnp.dot(lhs, rhs, preferred_element_type=F32)


def rows_dot(lhs, rhs):
    return lax.dot_general(lhs, rhs, (((0,), (0,)), ((), ())), preferred_element_type=F32)


def cols_dot(lhs, rhs):
    return lax.dot_general(lhs, rhs, (((1,), (1,)), ((), ())), preferred_element_type=F32)


def gelu(h):
    return h * (0.5 * (1.0 + jnp.tanh(ROOT * (h + CUBE * (h * h * h)))))


def gelu_slope(h):
    sq = h * h
    t = jnp.tanh(ROOT * (h + CUBE * (sq * h)))
    return 0.5 * (1.0 + t) + (0.5 * h) * (1.0 - t * t) * (ROOT * (1.0 + (3.0 * CUBE) * sq))


def remote(src, dst, send, recv, where):
    return pltpu.make_async_remote_copy(src_ref=src, dst_ref=dst, send_sem=send, recv_sem=recv, device_id=where, device_id_type=MESH)


def signal(peer):
    pl.semaphore_signal(pltpu.get_barrier_semaphore(), inc=1, device_id=peer, device_id_type=MESH)


class Plane:
    def __init__(self):
        self.tp = lax.axis_index('tp')
        self.y = lax.rem(self.tp, SIDE)
        self.z = self.tp // SIDE

    def at(self, dy, dz):
        return lax.rem(self.z + dz + SIDE, SIDE) * SIDE + lax.rem(self.y + dy + SIDE, SIDE)

    def blk(self, half, df, ds):
        return self.at(df, ds) if half == 0 else self.at(ds, df)

    def near(self):
        return [{'tp': self.at(1, 0)}, {'tp': self.at(-1, 0)}, {'tp': self.at(0, 1)}, {'tp': self.at(0, -1)}]

    def rings(self):
        return [{'tp': self.at(d, 0)} for d in (1, 2, 3)] + [{'tp': self.at(0, d)} for d in (1, 2, 3)]


HOPS = (0, -1, 1, 2)
WALK = ((0, -1, None, 1), (0, 1, None, -1), (-1, 2, 0, 1), (1, 2, 1, -1))
BOTH = (0, 1)
TILE = 256
SLOTS = 15


def plane_gather(plane, bufs, send_sem, recv_sem, on_block=lambda *_: None, base=0, begun=False):
    def msg(a, half, slot, block, part, to):
        buf, start, size = bufs[a]
        size = size // 2
        start = start + half * size
        if part is not None:
            size = size // 2
            start = start + part * size
        ref = buf.at[plane.blk(half, *block), pl.ds(start, size)]
        return remote(ref, ref, send_sem.at[base + a], recv_sem.at[((base + a) * 2 + half) * SLOTS + slot], {'tp': plane.blk(half, *to)})

    def f(a, half, k, end):
        step = WALK[k]
        return msg(a, half, min(k, 2), (step[end], 0), None if end and k > 1 else step[2], (step[3], 0))

    def s(a, half, j, k, end):
        step = WALK[k]
        return msg(a, half, 3 * (j + 1) + min(k, 2), (HOPS[j], step[end]), None if end and k > 1 else step[2], (0, step[3]))

    send, recv = BOTH
    pairs = [(a, half) for a in range(len(bufs)) for half in BOTH]

    def across(a, half, j):
        for k in BOTH:
            s(a, half, j, k, send).start()
        on_block(a, half, j, 0)

    def onward(a, half, j):
        for k in BOTH:
            s(a, half, j, k, recv).wait_recv()
            s(a, half, j, k + 2, send).start()
            on_block(a, half, j, k + 1)

    if not begun:
        for pair in pairs:
            for k in BOTH:
                f(*pair, k, send).start()
            across(*pair, 0)
        yield
    for pair in pairs:
        for k in BOTH:
            f(*pair, k, recv).wait_recv()
            f(*pair, k + 2, send).start()
            across(*pair, k + 1)
    yield
    for pair in pairs:
        onward(*pair, 0)
    yield
    for pair in pairs:
        f(*pair, 2, recv).wait_recv()
        across(*pair, SIDE - 1)
    yield
    for j in range(1, SIDE):
        for pair in pairs:
            onward(*pair, j)
        yield
    for j in range(SIDE):
        for pair in pairs:
            s(*pair, j, 2, recv).wait_recv()
            on_block(*pair, j, SIDE - 1)
    for a, (buf, start, size) in enumerate(bufs):
        sent = buf.at[pl.ds(0, SIDE * SIDE - 1), pl.ds(start, size)]
        remote(sent, sent, send_sem.at[base + a], recv_sem.at[0], {'tp': plane.at(1, 0)}).wait_send()


def tiles(width):
    return [slice(n, n + TILE) for n in range(0, width, TILE)]


def drain(steps):
    for _ in steps:
        pass


def local(src, dst, sem):
    return pltpu.make_async_copy(src, dst, sem)


class Reduce:
    def __init__(self, plane, parts, got_one, sum_one, got_two, one_send, one_recv, two_send, two_recv):
        self.plane, self.parts, self.got_one, self.sum_one, self.got_two = plane, parts, got_one, sum_one, got_two
        self.one_send, self.one_recv, self.two_send, self.two_recv = one_send, one_recv, two_send, two_recv

    def row(self, half, index):
        size = self.parts.shape[3] // 2
        cols = pl.ds(half * size, size)
        return self.parts.at[:, index, :, cols] if half == 0 else self.parts.at[index, :, :, cols]

    def here(self, half):
        return (self.plane.y, self.plane.z) if half == 0 else (self.plane.z, self.plane.y)

    def first(self, half, d):
        n = half * 3 + d - 1
        dest = lax.rem(self.here(half)[0] + d, SIDE)
        return remote(self.row(half, dest), self.got_one.at[n], self.one_send, self.one_recv.at[half], {'tp': self.plane.blk(half, d, 0)})

    def second(self, half, d):
        n = half * 3 + d - 1
        dest = lax.rem(self.here(half)[1] + d, SIDE)
        return remote(self.sum_one.at[half, dest], self.got_two.at[n], self.two_send, self.two_recv.at[half], {'tp': self.plane.blk(half, 0, d)})

    def whole(self, got, send, recv, half=None):
        ref = got if half is None else got.at[pl.ds(half * 3, 3)]
        return remote(ref, ref, send, recv.at[half or 0], {'tp': self.plane.at(1, 0)})

    def begin(self, half):
        for d in (2, 1, 3):
            self.first(half, d).start()

    def middle(self):
        for half in BOTH:
            total = self.row(half, self.here(half)[0])[:].astype(F32)
            self.whole(self.got_one, self.one_send, self.one_recv, half).wait_recv()
            for d in (1, 3, 2):
                total = total + self.got_one[half * 3 + d - 1].astype(F32)
            self.sum_one[half] = total.astype(self.sum_one.dtype)
            for d in (2, 1, 3):
                self.second(half, d).start()

    def end(self):
        sums = []
        for half in BOTH:
            total = self.sum_one[half, self.here(half)[1]].astype(F32)
            self.whole(self.got_two, self.two_send, self.two_recv, half).wait_recv()
            for d in (1, 3, 2):
                total = total + self.got_two[half * 3 + d - 1].astype(F32)
            sums.append(total)
        return sums

    def close(self):
        self.whole(self.got_one, self.one_send, self.one_recv).wait_send()
        self.whole(self.got_two, self.two_send, self.two_recv).wait_send()


def fold(op, value):
    rows, cols = value.shape
    return op(value.reshape(rows // 8, 8, cols), axis=0)


def flatten(ids, flat):
    size, cols = ids.shape[1], flat.shape[1]
    for r in range(ids.shape[0]):
        at = r * size
        flat[at // cols:at // cols + 1, at % cols:at % cols + size] = ids[r:r + 1, :]


def list_rows(tokens, base, rows, group, unit, flat, slot, out):
    lines, lanes = flat.shape
    count = lines * lanes
    flatten(tokens, flat)
    row = flat[:] - base
    mine = (row >= 0) & (row < rows)
    upper = lax.broadcasted_iota(jnp.int32, (lanes, lanes), 0) <= lax.broadcasted_iota(jnp.int32, (lanes, lanes), 1)
    ones = [jnp.where(mask, 1.0, 0.0).astype(BF16) for mask in (mine, upper)]
    seen = dot(*ones)
    total = jnp.zeros((1, 1), F32)
    for r in range(lines):
        line = slice(r, r + 1)
        here = slice(r * lanes, (r + 1) * lanes)
        slot[:1, here] = jnp.where(mine[line], seen[line] + (total - 1.0), -1.0).astype(jnp.int32)
        slot[1:, here] = row[line]
        total = total + seen[line, lanes - 1:]
    number = lax.broadcasted_iota(jnp.int32, (1, count), 1)
    inner = lax.rem(number, group)
    place = inner // unit * (count // group * unit) + number // group * unit + lax.rem(number, unit)
    digits = [part for value in (place, slot[1:, :]) for part in (value // 256, lax.rem(value, 256))]
    which = lax.broadcasted_iota(jnp.int32, (16, count), 0)
    values = sum(jnp.where(which == i, digit, 0) for i, digit in enumerate(digits)).astype(F32).astype(BF16)

    @pl.loop(0, count // group)
    def _(c):
        start = pl.multiple_of(c * group, group)
        pick = jnp.where(slot[:1, :] == start + lax.broadcasted_iota(jnp.int32, (group, count), 0), 1.0, 0.0).astype(BF16)
        found = cols_dot(values, pick)
        for i in BOTH:
            out[i:i + 1, pl.ds(start, group)] = (found[2 * i:2 * i + 1] * 256.0 + found[2 * i + 1:2 * i + 2]).astype(jnp.int32)

    out[2:, :] = jnp.broadcast_to(total, (1, count)).astype(jnp.int32)


def norm_of(x):
    wide = x.astype(F32)
    inv_rms = lax.rsqrt(jnp.mean(wide * wide, axis=-1, keepdims=True) + NORM_EPS)
    return inv_rms, wide * inv_rms


class Spread:
    def __init__(self, plane, source, stages, src, out, line_send, line_recv, die_send, die_recv):
        self.plane, self.source, self.stages, self.src, self.out = plane, source, stages, src, out
        self.line_send, self.line_recv, self.die_send, self.die_recv = line_send, line_recv, die_send, die_recv
        self.stage = lax.axis_index('pp')
        self.core = lax.rem(self.stage, 2)
        self.mate = {'pp': self.stage + 1 - 2 * self.core}
        self.rows = out.shape[1] // 2
        self.lo = pl.multiple_of(self.core * self.rows, self.rows)
        self.others = [p for p in range(stages) if p != source]

    def greet(self):
        source = self.stage == self.source
        twin = self.stage == self.source ^ 1
        pl.when(source)(functools.partial(signal, {'pp': self.source ^ 1}))
        pl.when(jnp.logical_not(source))(functools.partial(signal, {'pp': self.source}))
        pl.when(jnp.logical_not(source | twin))(functools.partial(signal, self.mate))
        return jnp.where(source, len(self.others), 1)

    def line(self, p):
        part = pl.ds((p % 2) * self.rows, self.rows)
        return remote(self.src.at[part], self.out.at[self.plane.tp, part], self.line_send, self.line_recv, {'pp': p})

    def send(self):
        for p in self.others:
            self.line(p).start()
        part = pl.ds(self.lo, self.rows)
        self.out[self.plane.tp, part] = self.src[part]

    def arrive(self):
        mine = self.out.at[self.plane.tp, pl.ds(self.lo, self.rows)]
        remote(mine, mine, self.line_recv, self.line_recv, self.mate).wait_recv()

    def on_block(self, a, half, j, k):
        if a == 0:
            size = self.rows // 2
            ref = self.out.at[self.plane.blk(half, HOPS[j], HOPS[k]), pl.ds(self.lo + half * size, size)]
            remote(ref, ref, self.die_send, self.die_recv, self.mate).start()

    def half(self, lo):
        ref = self.out.at[:, pl.ds(lo, self.rows)]
        return remote(ref, ref, self.die_send, self.die_recv, self.mate)

    def finish(self):
        self.half(pl.multiple_of((1 - self.core) * self.rows, self.rows)).wait_recv()

    def close(self):
        self.half(self.lo).wait_send()

        @pl.when(self.stage == self.source)
        def _():
            sent = self.out.at[pl.ds(0, len(self.others)), pl.ds(self.lo, self.rows)]
            remote(sent, sent, self.line_send, self.line_recv, self.mate).wait_send()


def forward_kernel(last, tokens, emb, w_one, w_two, top, own_x, table, order_out, hid_out, one_out, two_out, x_out, ones, twos, one_t, two_t, hot, parts,
                   got_one, sum_one, got_two, piece, x_buf, y_buf, n_src, a_buf, hid_ref, x_all, ids, flat, slot,
                   send_sem, recv_sem, one_send, one_recv, two_send, two_recv, line_send, line_recv, own_send, own_recv, spread_send, spread_recv, die_send, die_recv,
                   hop_send, hop_recv, lead_sem, loc_sem):
    plane = Plane()
    stage = lax.axis_index('pp')
    tp = plane.tp
    stages = last + 1
    core = lax.rem(stage, 2)
    moves = ((emb, table), (w_one, ones.at[tp]), (w_two, twos.at[tp]), (one_t, one_out), (two_t, two_out), (hid_ref, hid_out), (x_all, x_out))
    load, own_one, own_two, *saves = [local(src, dst, loc_sem.at[i]) for i, (src, dst) in enumerate(moves)]
    save_one, save_two, save_hid, save_x = saves
    load.start()
    own_one.start()
    own_two.start()
    for peer in plane.rings() + [{'pp': lax.rem(stage + d, stages)} for d in range(1, stages)]:
        signal(peer)

    own_one.wait()
    own_two.wait()
    pl.semaphore_wait(pltpu.get_barrier_semaphore(), 6 + last)
    def weight_steps(begun=False):
        return plane_gather(plane, [(ones, 0, ones.shape[1]), (twos, 0, twos.shape[1])], send_sem, recv_sem, begun=begun)

    @pl.when(core == 0)
    def _():
        next(weight_steps())

    rows, width = table.shape
    group = ids.shape[1]
    unit = piece.shape[0]
    count = group // tokens.shape[1]
    flatten(tokens.at[pl.ds(pl.multiple_of(stage * count, count), count)], ids)
    hot[:] = jnp.where(ids[:] - tp * rows == lax.broadcasted_iota(jnp.int32, hot.shape, 0), 1.0, 0.0).astype(BF16)
    load.wait()
    cut = rows // group * group
    for cols in tiles(width):
        picked = rows_dot(hot[:cut], table[:cut, cols]) + rows_dot(hot[cut:], table[cut:, cols])
        parts[:, :, :, cols] = picked.astype(BF16).reshape(*parts.shape[:-1], TILE)
    red = Reduce(plane, parts, got_one, sum_one, got_two, one_send, one_recv, two_send, two_recv)
    for half in BOTH:
        red.begin(half)

    @pl.when(core == 1)
    def _():
        pl.semaphore_wait(lead_sem, 1)
        next(weight_steps())

    gather = weight_steps(True)
    next(gather)

    @pl.when(core == 0)
    def _():
        pl.semaphore_signal(lead_sem, inc=1, device_id={'pp': stage + 1}, device_id_type=MESH)

    next(gather)
    red.middle()
    next(gather)
    next(gather)
    for half, total in enumerate(red.end()):
        piece[:, half * (width // 2):(half + 1) * (width // 2)] = total.astype(BF16)

    def line(p):
        return remote(piece, x_buf.at[pl.ds(pl.multiple_of(p * unit, unit), unit)], line_send, line_recv, {'pp': 0})

    @pl.when(stage != 0)
    def _():
        line(stage).start()

    @pl.when(stage == 0)
    def _():
        x_buf[:unit] = piece[:]

    drain(gather)

    @pl.when(stage == 1)
    def _():
        pl.semaphore_signal(lead_sem, inc=1, device_id={'pp': 0}, device_id_type=MESH)

    blocks, _, cols = ones.shape

    def spare_time():
        @pl.loop(0, blocks)
        def _(k):
            one_t[k] = ones[k].T
            two_t[k] = twos[k].T

        save_one.start()
        save_two.start()
        list_rows(tokens, tp * rows, rows, group, unit, flat, slot, order_out)

    pl.when(stage > 1)(spare_time)
    hop = remote(y_buf, x_buf, hop_send, hop_recv, {'pp': lax.rem(stage + 1, stages)})

    @pl.when(stage == 0)
    def _():
        got = x_buf.at[pl.ds(0, last * unit)]
        remote(got, got, line_send, line_recv, {'pp': last}).wait_recv()

    pl.when(stage > 0)(hop.wait_recv)
    x_act = x_buf[:]
    for k in range(blocks):
        hidden = dot(x_act, ones[k])
        hid_ref[k] = hidden
        a_buf[:, k * cols:(k + 1) * cols] = gelu(hidden).astype(BF16)
    save_hid.start()
    gate = a_buf[:]
    for tile in tiles(width):
        branch = dot(gate, twos[:, :, tile].reshape(blocks * cols, TILE))
        y_buf[:, tile] = (x_buf[:, tile].astype(F32) + branch).astype(BF16)

    pl.when(stage < last)(hop.start)
    x_all[tp] = x_buf[:]

    @pl.when(stage < SIDE)
    def _():
        pl.when(stage <= 1)(spare_time)

        @pl.when(stage == 0)
        def _():
            pl.semaphore_wait(lead_sem, 1)

        steps = plane_gather(plane, [(x_all, 0, x_all.shape[1])], send_sem, recv_sem, base=2)
        drain(steps)

    own_save = local(x_all.at[tp], x_out.at[tp], loc_sem.at[6])
    pl.when(stage < SIDE)(save_x.start)
    pl.when(stage >= SIDE)(own_save.start)

    spread = Spread(plane, last, stages, n_src, top, spread_send, spread_recv, die_send, die_recv)

    def own(p):
        return remote(y_buf.at[pl.ds(p * unit, unit)], own_x, own_send, own_recv, {'pp': p})

    @pl.when(stage == last)
    def _():
        n_src[:] = norm_of(y_buf[:])[1].astype(BF16)
        spread.send()
        for p in spread.others:
            own(p).start()
        own_x[:] = y_buf[last * unit:]

    pl.when(stage < last)(spread.arrive)
    drain(plane_gather(plane, [(top, spread.lo, spread.rows)], send_sem, recv_sem, spread.on_block, base=3))
    spread.finish()
    pl.when(stage < last)(own(last).wait_recv)
    spread.close()

    @pl.when(stage == last)
    def _():
        sent = y_buf.at[pl.ds(0, last * unit)]
        remote(sent, sent, own_send, own_recv, spread.mate).wait_send()

    red.close()

    @pl.when(stage != 0)
    def _():
        line(stage).wait_send()

    pl.when(stage < last)(hop.wait_send)
    for save in saves[:-1]:
        save.wait()
    pl.when(stage < SIDE)(save_x.wait)
    pl.when(stage >= SIDE)(own_save.wait)


def head_kernel(target, stages, chunk, table, top, own_x, labels, loss_out, g_top, g_out, n_out,
                n_buf, lab, g_buf, peak, stat, shared, scale_ref, parts, got_one, sum_one, got_two, piece,
                share_send, share_recv, one_send, one_recv, two_send, two_recv, line_send, line_recv, loc_sem, *e_bufs):
    plane = Plane()
    stage = lax.axis_index('pp')
    tp = plane.tp
    size = shared.shape[1]
    others = [p for p in range(stages) if p != target]
    each, group = peak.shape[1:]
    unit = group // size
    for d in range(1, size):
        signal({'tp': lax.rem(tp + d, size)})

    @pl.when(stage == target)
    def _():
        for p in others:
            signal({'pp': p})

    pl.when(stage != target)(functools.partial(signal, {'pp': target}))
    for p in range(stages):
        n_buf[p * group:(p + 1) * group] = top[:, p * unit:(p + 1) * unit, :].reshape(group, top.shape[2])
    save_n = local(n_buf, n_out, loc_sem.at[1])
    save_n.start()

    rows, width = table.shape
    flatten(labels, lab)
    lab[:] = lab[:] - tp * rows
    pieces = len(e_bufs)
    pair = each * group

    def group_at(b, i):
        return lax.rem(stage // each + b, pieces) * each + i

    def label_of(p):
        return lab[pl.ds(p, 1), :]

    def down(value, start):
        return start + lax.broadcasted_iota(jnp.int32, value.shape, 0)

    def logit_chunk(b, start):
        tokens = n_buf[pl.ds(pl.multiple_of(group_at(b, 0) * group, pair), pair), :]
        logits = cols_dot(table[pl.ds(start, chunk), :], tokens)
        e_bufs[b][pl.ds(start, chunk), :] = logits
        return fold(jnp.max, logits)

    def exp_chunk(b, start, label, top_b, total, hits):
        logits = e_bufs[b][pl.ds(start, chunk), :]
        e = jnp.exp(logits - top_b)
        e_bufs[b][pl.ds(start, chunk), :] = e
        return total + fold(jnp.sum, e), hits + fold(jnp.sum, jnp.where(label == down(logits, start), logits, 0.0))

    def chunks(body, carry):
        return lax.fori_loop(0, rows // chunk, lambda c, carry: body(pl.multiple_of(c * chunk, 8), carry), carry)

    def msg(d, k):
        some = pl.ds(k, 1 + k * (pieces - 2))
        return remote(stat.at[some], shared.at[some, tp], share_send.at[k], share_recv.at[k], {'tp': lax.rem(tp + d, size)})

    def shares(k):
        ref = shared.at[pl.ds(k, 1 + k * (pieces - 2)), pl.ds(0, size - 1)]
        return remote(ref, ref, share_send.at[k], share_recv.at[k], {'tp': plane.at(1, 0)})

    def share(k):
        for d in range(1, size):
            msg(d, k).start()

    losses = []

    def normalise(k):
        shares(k).wait_recv()
        for b in (range(1, pieces) if k else range(1)):
            every = shared[b, :, 0]
            most = jnp.max(every, axis=0)
            log_norm = most + jnp.log(jnp.sum(jnp.exp(every - most[None]), axis=0))
            losses.append(jnp.sum(log_norm - jnp.sum(shared[b, :, 1], axis=0), keepdims=True))
            scale_ref[b] = jnp.exp(peak[b] - log_norm)

    def grad_block(b, i, slot):
        cols = pl.ds(pl.multiple_of(i * group, group), group)
        label = label_of(group_at(b, i))
        factor = scale_ref[b, pl.ds(i, 1), :]

        def part(start, _):
            e = e_bufs[b][pl.ds(start, chunk), cols]
            hit = label == down(e, start)
            g_buf[slot, pl.ds(start, chunk), :] = (e * factor - jnp.where(hit, 1.0, 0.0)).astype(BF16)

        chunks(part, None)

    def save(k):
        slot = 1 + k % 2
        at = pl.multiple_of(group_at(k // each, k % each) * group, group)
        return local(g_buf.at[slot], g_out.at[:, pl.ds(at, group)], loc_sem.at[2 + slot])

    def gradient(k):
        if k >= 2:
            save(k - 2).wait()
        grad_block(k // each, k % each, 1 + k % 2)
        save(k).start()

    cut = rows // group * group
    half = width // 2
    red = Reduce(plane, parts, got_one, sum_one, got_two, one_send, one_recv, two_send, two_recv)

    def own_gradient():
        grad_block(0, lax.rem(stage, each), 0)
        mine_g = g_buf.at[0]
        for cols in tiles(width):
            back = rows_dot(mine_g[:cut, :], table[:cut, cols]) + rows_dot(mine_g[cut:, :], table[cut:, cols])
            parts[:, :, :, cols] = back.reshape(*parts.shape[:-1], TILE)
            if cols.stop % half == 0:
                red.begin(cols.start // half)

    tops = []
    zero = jnp.zeros((8, pair), F32)
    for now, done in ((0, None), (None, 0), (1, None), *((b, b - 1) for b in range(2, pieces)), (None, pieces - 1)):
        label = None if done is None else jnp.concatenate([label_of(group_at(done, i)) for i in range(each)], axis=1)
        top_b = None if done is None else tops[done]

        def both(start, carry, now=now, done=done, top_b=top_b, label=label):
            best, total, hits = carry
            if now is not None:
                best = jnp.maximum(best, logit_chunk(now, start))
            if done is not None:
                total, hits = exp_chunk(done, start, label, top_b, total, hits)
            return best, total, hits

        best, total, hits = chunks(both, (jnp.full((8, pair), -jnp.inf, F32), zero, zero))
        if done is not None:
            found = (top_b + jnp.log(jnp.sum(total, axis=0, keepdims=True)), jnp.sum(hits, axis=0, keepdims=True), top_b)
            for i in range(each):
                cols = slice(i * group, (i + 1) * group)
                for kind in BOTH:
                    stat[done, kind, i:i + 1, :] = found[kind][:, cols]
                peak[done, i:i + 1, :] = found[2][:, cols]
            shared[done, tp] = stat[done]
        if done == 0:
            pl.semaphore_wait(pltpu.get_barrier_semaphore(), size - 1 + jnp.where(stage == target, len(others), 1))
        if now is None:
            share(1 if done else 0)
        else:
            tops.append(jnp.max(best, axis=0, keepdims=True))
        if now == 1:
            normalise(0)
            own_gradient()
        if now == pieces - 1:
            red.middle()

    gradient(0)
    gradient(1)
    sums = red.end()

    inv_rms, normed = norm_of(own_x[:])
    mean = (jnp.sum(normed[:, :half] * sums[0], axis=-1, keepdims=True) + jnp.sum(normed[:, half:] * sums[1], axis=-1, keepdims=True)) / width
    for h in BOTH:
        cols = slice(h * half, (h + 1) * half)
        piece[:, cols] = (inv_rms * (sums[h] - normed[:, cols] * mean)).astype(BF16)

    def line(p):
        return remote(piece, g_top.at[p], line_send, line_recv, {'pp': target})

    @pl.when(stage != target)
    def _():
        line(stage).start()

    normalise(1)
    for k in range(2, stages):
        gradient(k)
    loss_out[:] = sum(losses) / (stages * group)
    @pl.when(stage == target)
    def _():
        g_top[target] = piece[:]
        got = g_top.at[pl.ds(0, len(others))]
        remote(got, got, line_send, line_recv, {'pp': 0}).wait_recv()

    red.close()
    for k in BOTH:
        shares(k).wait_send()
    save_n.wait()
    save(stages - 2).wait()
    save(stages - 1).wait()
    @pl.when(stage != target)
    def _():
        line(stage).wait_send()


def backward_kernel(last, chunk, g_top, hid_in, two_all, one_all, g_all, n_all, x_in, w_one, w_two, de_buf, dx_all, grad_one, grad_two,
                    ones, twos, slope_ref, g_buf, n_buf, x_all, w_one_buf, w_two_buf, dy_all, dy_buf, dx_buf, d_buf,
                    send_sem, recv_sem, spread_send, spread_recv, die_send, die_recv, hop_send, hop_recv, go_sem, ready_sem, g_sem, loc_sem):
    plane = Plane()
    stage = lax.axis_index('pp')
    stages = last + 1
    blocks, cols, width = one_all.shape
    pairs = ((hid_in, slope_ref), (two_all, twos), (one_all, ones), (n_all, n_buf), (w_one, w_one_buf), (w_two, w_two_buf))
    loads = [local(src, dst, loc_sem.at[i]) for i, (src, dst) in enumerate(pairs)]
    lower = stage < SIDE
    upper = stage >= SIDE
    own = plane.tp
    load_x = [local(*pair, loc_sem.at[6]) for pair in ((x_in, x_all), (x_in.at[own], x_all.at[own]))]

    mid = upper & (stage < last - 1)

    def start(some):
        for load in some:
            load.start()

    pl.when(upper)(functools.partial(start, loads[:3]))
    pl.when(lower)(functools.partial(start, loads[3:4]))
    own_load = load_x[1]
    pl.when(mid)(own_load.start)
    spread = Spread(plane, 0, stages, dx_buf, dx_all, spread_send, spread_recv, die_send, die_recv)
    near = plane.near()
    for peer in near:
        signal(peer)
    extra = spread.greet()
    before = {'pp': lax.rem(stage + last, stages)}
    pl.when(stage > 0)(functools.partial(signal, before))
    hop = remote(dx_buf, dy_buf, hop_send, hop_recv, before)
    rows = de_buf.shape[0]
    pieces = -(-rows // chunk)

    def piece_at(c):
        return pl.ds(pl.multiple_of(jnp.minimum(c * chunk, rows - chunk), 8), chunk)

    def fetch(c):
        slot = lax.rem(c, 2)
        return local(g_all.at[piece_at(c)], g_buf.at[slot], g_sem.at[slot])

    def table(lo, hi):
        if lo == 0:
            fetch(0).start()
            loads[3].wait()

        @pl.loop(lo, hi)
        def _(c):
            @pl.when(c < pieces - 1)
            def _():
                fetch(c + 1).start()

            for i, some in enumerate((loads[:2], loads[2:3], loads[4:] + load_x[:1])):
                pl.when(lower & (c == i + 1))(functools.partial(start, some))

            fetch(c).wait()
            de_buf[piece_at(c), :] = dot(g_buf[lax.rem(c, 2)], n_buf[:])

    pl.semaphore_wait(pltpu.get_barrier_semaphore(), len(near) + extra + jnp.where(stage < last, 1, 0))

    @pl.when(stage < last)
    def _():
        pl.semaphore_signal(ready_sem, inc=1, device_id={'pp': lax.rem(stage + 1, stages)}, device_id_type=MESH)

    pl.when(lower)(functools.partial(table, 0, pieces))
    loads[0].wait()
    for k in range(blocks):
        slope_ref[k] = gelu_slope(slope_ref[k])
    loads[1].wait()

    def a_steps(begun=False):
        return plane_gather(plane, [(x_all, 0, x_all.shape[1])], send_sem, recv_sem, base=2, begun=begun)

    mid_steps = a_steps()

    @pl.when(mid)
    def _():
        own_load.wait()
        for _ in range(3):
            next(mid_steps)

    @pl.when(stage == last)
    def _():
        dy_buf[:] = g_top[:]

    pl.when(stage < last)(hop.wait_recv)
    dy_all[plane.tp] = dy_buf[:]
    whole = (dy_all, 0, dy_all.shape[1])
    part = (dx_all, spread.lo, spread.rows)

    def dy_steps(begun):
        return plane_gather(plane, [whole], send_sem, recv_sem, base=1, begun=begun)

    @pl.when(stage <= 1)
    def _():
        next(dy_steps(False))

    grad_y = dy_buf[:]
    for k in range(blocks):
        grad_gate = dot(grad_y, twos[k])
        d_buf[:, k * cols:(k + 1) * cols] = (slope_ref[k] * grad_gate).astype(BF16)
    loads[2].wait()
    grad_hidden = d_buf[:]
    for tile in tiles(width):
        back = dot(grad_hidden, ones[:, :, tile].reshape(blocks * cols, TILE))
        dx_buf[:, tile] = (dy_buf[:, tile].astype(F32) + back).astype(BF16)

    @pl.when(stage > 0)
    def _():
        pl.semaphore_wait(ready_sem, 1)
        hop.start()

    pl.when(stage == 0)(spread.send)
    pl.when(upper)(functools.partial(start, loads[3:]))
    pl.when(upper & jnp.logical_not(mid))(own_load.start)
    for load in loads[4:]:
        load.wait()
    pl.when(lower)(load_x[0].wait)
    pl.when(upper & jnp.logical_not(mid))(own_load.wait)

    grad_one[:] = jnp.zeros_like(grad_one)
    grad_two[:] = jnp.zeros_like(grad_two)

    def weights(lo, hi):
        step = SIDE

        @pl.loop(lo, hi)
        def _(c):
            part = pl.ds(c * step, step)
            x_act = x_all[part].reshape(step * x_all.shape[1], width)
            grad_y = dy_all[part].reshape(step * x_all.shape[1], width)
            hidden = dot(x_act, w_one_buf[:])
            grad_gate = cols_dot(grad_y, w_two_buf[:])
            grad_hidden = (gelu_slope(hidden) * grad_gate).astype(BF16)
            grad_one[:] += rows_dot(x_act, grad_hidden)
            grad_two[:] += rows_dot(gelu(hidden).astype(BF16), grad_y)

    def dx_steps():
        return plane_gather(plane, [part], send_sem, recv_sem, spread.on_block)

    @pl.when(stage > 1)
    def _():
        hop.wait_send()

        @pl.when(spread.core == 0)
        def _():
            pl.semaphore_signal(go_sem, inc=1, device_id=spread.mate, device_id_type=MESH)

        @pl.when(spread.core == 1)
        def _():
            pl.semaphore_wait(go_sem, 1)

    @pl.when(stage > 1)
    def _():
        next(dy_steps(False))

    @pl.when(upper & jnp.logical_not(mid))
    def _():
        next(a_steps())

    planes = [(stage <= 1, None, 'dxddxdxdxdx', 'xx'), ((stage > 1) & lower, None, 'dddxdxdxdx', 'xxx'),
              (mid, mid_steps, 'dtdadatdaxdaxdx', 'xxx'), (upper & jnp.logical_not(mid), a_steps(True), 'datdadatdaxdaxdax', 'xxx')]
    runs = []
    for here, more, order, rest in planes:
        steps = {'d': dy_steps(True), 'x': dx_steps(), 'a': more}

        def arrived(order=order, steps=steps):
            part = -(-pieces // 2)
            for i, kind in enumerate(order):
                if kind == 't':
                    lo = order[:i].count('t') * part
                    table(lo, min(lo + part, pieces))
                    continue
                if kind == 'x' and 'x' not in order[:i]:
                    pl.when(stage > 0)(spread.arrive)
                next(steps[kind])
            drain(steps['d'])
            drain(steps['a'] or ())

        def onward(rest=rest, steps=steps):
            for kind in rest:
                next(steps[kind])

        pl.when(here)(arrived)
        runs.append((here, onward, functools.partial(drain, steps['x'])))

    weights(0, 2)
    for here, onward, _ in runs:
        pl.when(here)(onward)
    weights(2, SIDE)
    for here, _, finish in runs:
        pl.when(here)(finish)

    spread.finish()
    spread.close()

    pl.when(stage == 1)(hop.wait_send)


def add_kernel(pieces, order, dx_ref, de_ref, one_ref, two_ref, de_out, table_out, one_out, two_out, wide, sem):
    saves = [local(one_ref, one_out, sem.at[0]), local(two_ref, two_out, sem.at[1])]
    for save in saves:
        save.start()
    wide[:] = dx_ref[:].astype(F32)

    @pl.loop(0, order[2, 0])
    def _(j):
        row = pl.ds(order[1, j], 1)
        de_out[row, :] = de_out[row, :] + wide[pl.ds(order[0, j], 1), :]

    rows = de_ref.shape[0]
    size = -(-rows // (8 * pieces)) * 8
    for c in range(pieces):
        part = pl.ds(c * size, min(size, rows - c * size))
        saves.append(local(de_out.at[part], table_out.at[part], sem.at[2 + c]))
        saves[-1].start()
    for save in saves:
        save.wait()


def vmem():
    return pl.BlockSpec(memory_space=pltpu.VMEM)


def anywhere():
    return pl.BlockSpec(memory_space=pl.ANY)


def params(cid, mib):
    return pltpu.CompilerParams(collective_id=cid, has_side_effects=True, vmem_limit_bytes=mib << 20)


DMA = pltpu.SemaphoreType.DMA


def solution(mesh):
    pp_size = mesh.shape['pp']
    tp_size = mesh.shape['tp']
    last = pp_size - 1

    def device_fn(tokens, labels, emb_table, w_in, w_out):
        num_tokens = tokens.shape[0] * tokens.shape[1]
        vocab_rows, width = emb_table.shape
        w_one, w_two = w_in[0], w_out[0]
        cols = w_one.shape[1]
        unit = num_tokens // (pp_size * tp_size)
        block = pp_size * unit
        group = tp_size * unit
        half = width // 2
        chunk = vocab_rows // 3
        step = 512
        pair = 2 * group
        shape = jax.ShapeDtypeStruct
        VM = pltpu.VMEM

        def reduce_scratch(dtype):
            return [VM((SIDE, SIDE, unit, width), dtype), VM((6, SIDE, unit, half), dtype), VM((2, SIDE, unit, half), dtype), VM((6, unit, half), dtype), VM((unit, width), BF16)]

        duo = DMA((2,))
        reduce_sems = [DMA, duo, DMA, duo, DMA, DMA]
        many = shape((tp_size, block, width), BF16)
        many_buf = VM((tp_size, block, width), BF16)
        two_sums = 2 * SLOTS
        gather_sems = [DMA((4,)), DMA((4 * two_sums,))]
        spread_sems = [DMA, DMA, DMA, DMA]

        top, own_x, table, order, hidden, one_t, two_t, x_all = pl.pallas_call(
            functools.partial(forward_kernel, last),
            out_shape=(many_buf, VM((unit, width), BF16), VM((vocab_rows, width), BF16), shape((3, num_tokens), jnp.int32), shape((tp_size, block, cols), F32), shape((tp_size, cols, width), BF16), shape((tp_size, width, cols), BF16), many),
            in_specs=[vmem()] + [anywhere()] * 3,
            out_specs=[vmem()] * 4 + [anywhere()] * 4,
            scratch_shapes=[VM((tp_size, width, cols), BF16), VM((tp_size, cols, width), BF16), VM((tp_size, cols, width), BF16), VM((tp_size, width, cols), BF16),
                            VM((vocab_rows, group), BF16), *reduce_scratch(BF16),
                            VM((block, width), BF16), VM((block, width), BF16), VM((block, width), BF16), VM((block, tp_size * cols), BF16), VM((tp_size, block, cols), F32), many_buf, VM((1, group), jnp.int32),
                            VM((num_tokens // 128, 128), jnp.int32), VM((2, num_tokens), jnp.int32),
                            *gather_sems, *reduce_sems, DMA, DMA, *spread_sems, DMA, DMA, pltpu.SemaphoreType.REGULAR, DMA((7,))],
            compiler_params=params(1, 49), name='forward_chain',
        )(tokens, emb_table, w_one, w_two)

        by_pair = (num_tokens // pair, pair // group, group)
        loss, g_top, g_all, n_all = pl.pallas_call(
            functools.partial(head_kernel, last, pp_size, chunk),
            out_shape=(shape((1, 1), F32), pltpu.HBM((pp_size, unit, width), BF16), shape((vocab_rows, num_tokens), BF16), shape((num_tokens, width), BF16)),
            in_specs=[vmem()] * 4,
            out_specs=[vmem()] * 2 + [anywhere()] * 2,
            scratch_shapes=[VM((num_tokens, width), BF16), VM((pp_size, group), jnp.int32), VM((3, vocab_rows, group), BF16),
                            VM(by_pair, F32), VM((by_pair[0], 2, *by_pair[1:]), F32), VM((by_pair[0], tp_size, 2, *by_pair[1:]), F32), VM(by_pair, F32), *reduce_scratch(F32),
                            duo, duo, *reduce_sems, DMA((5,)),
                            *[VM((vocab_rows, pair), F32) for _ in range(num_tokens // pair)]],
            compiler_params=params(2, 49), name='head',
        )(*[pltpu.with_memory_space_constraint(array, pltpu.VMEM) for array in (table, top, own_x)], labels)

        de_head, dx_first, grad_one, grad_two = pl.pallas_call(
            functools.partial(backward_kernel, last, step),
            out_shape=(VM((vocab_rows, width), F32), many_buf, VM((width, cols), F32), VM((cols, width), F32)),
            in_specs=[vmem()] + [anywhere()] * 8, out_specs=[vmem()] * 4,
            scratch_shapes=[VM((tp_size, cols, width), BF16), VM((tp_size, width, cols), BF16), VM((tp_size, block, cols), F32), VM((2, step, num_tokens), BF16), VM((num_tokens, width), BF16),
                            many_buf, VM((width, cols), BF16), VM((cols, width), BF16), many_buf,
                            VM((block, width), BF16), VM((block, width), BF16), VM((block, tp_size * cols), BF16),
                            *gather_sems, *spread_sems, DMA, DMA, pltpu.SemaphoreType.REGULAR, pltpu.SemaphoreType.REGULAR, duo, DMA((7,))],
            compiler_params=params(3, 45), name='backward_chain',
        )(g_top.reshape(block, width), hidden, two_t, one_t, g_all, n_all, x_all, w_one, w_two)

        smem = pl.BlockSpec(memory_space=pltpu.SMEM)
        _, grad_table, grad_one, grad_two = pl.pallas_call(
            functools.partial(add_kernel, 12),
            out_shape=(VM((vocab_rows, width), F32), shape((vocab_rows, width), F32), shape((width, cols), F32), shape((cols, width), F32)),
            in_specs=[smem] + [vmem()] * 4, out_specs=[vmem()] + [anywhere()] * 3,
            scratch_shapes=[VM((num_tokens, width), F32), DMA((14,))], input_output_aliases={2: 0},
            compiler_params=pltpu.CompilerParams(vmem_limit_bytes=24 << 20), name='add_rows',
        )(order, dx_first.reshape(num_tokens, width), de_head, grad_one, grad_two)
        return loss.reshape(1), grad_one[None], grad_two[None], grad_table

    return jax.shard_map(device_fn, mesh=mesh, in_specs=(P('dp', None), P('dp', None), P('tp', None), P('pp', None, 'tp'), P('pp', 'tp', None)), out_specs=(P('dp'), P(('dp', 'pp'), None, 'tp'), P(('dp', 'pp'), 'tp', None), P(('dp', 'tp'), None)), check_vma=False)
```

```python
import functools

import jax
import jax.numpy as jnp
from jax import lax
from jax.experimental import pallas as pl
from jax.experimental.pallas import tpu as pltpu
from jax.sharding import PartitionSpec as P

NORM_EPS = 1e-6
SIDE = 4
MESH = pl.DeviceIdType.MESH
F32 = jnp.float32
BF16 = jnp.bfloat16
CUBE = 0.044715
ROOT = 0.7978845608028654


def dot(lhs, rhs):
    return jnp.dot(lhs, rhs, preferred_element_type=F32)


def rows_dot(lhs, rhs):
    return lax.dot_general(lhs, rhs, (((0,), (0,)), ((), ())), preferred_element_type=F32)


def cols_dot(lhs, rhs):
    return lax.dot_general(lhs, rhs, (((1,), (1,)), ((), ())), preferred_element_type=F32)


def gelu(h):
    return h * (0.5 * (1.0 + jnp.tanh(ROOT * (h + CUBE * (h * h * h)))))


def gelu_slope(h):
    sq = h * h
    t = jnp.tanh(ROOT * (h + CUBE * (sq * h)))
    return 0.5 * (1.0 + t) + (0.5 * h) * (1.0 - t * t) * (ROOT * (1.0 + (3.0 * CUBE) * sq))


def remote(src, dst, send, recv, where):
    return pltpu.make_async_remote_copy(src_ref=src, dst_ref=dst, send_sem=send, recv_sem=recv, device_id=where, device_id_type=MESH)


def signal(peer):
    pl.semaphore_signal(pltpu.get_barrier_semaphore(), inc=1, device_id=peer, device_id_type=MESH)


class Plane:
    def __init__(self):
        self.tp = lax.axis_index('tp')
        self.y = lax.rem(self.tp, SIDE)
        self.z = self.tp // SIDE

    def at(self, dy, dz):
        return lax.rem(self.z + dz + SIDE, SIDE) * SIDE + lax.rem(self.y + dy + SIDE, SIDE)

    def blk(self, half, df, ds):
        return self.at(df, ds) if half == 0 else self.at(ds, df)

    def near(self):
        return [{'tp': self.at(1, 0)}, {'tp': self.at(-1, 0)}, {'tp': self.at(0, 1)}, {'tp': self.at(0, -1)}]

    def rings(self):
        return [{'tp': self.at(d, 0)} for d in (1, 2, 3)] + [{'tp': self.at(0, d)} for d in (1, 2, 3)]


HOPS = (0, -1, 1, 2)
WALK = ((0, -1, None, 1), (0, 1, None, -1), (-1, 2, 0, 1), (1, 2, 1, -1))
BOTH = (0, 1)
TILE = 256
SLOTS = 15


def plane_gather(plane, bufs, send_sem, recv_sem, on_block=lambda *_: None, base=0, begun=False):
    def msg(a, half, slot, block, part, to):
        buf, start, size = bufs[a]
        size = size // 2
        start = start + half * size
        if part is not None:
            size = size // 2
            start = start + part * size
        ref = buf.at[plane.blk(half, *block), pl.ds(start, size)]
        return remote(ref, ref, send_sem.at[base + a], recv_sem.at[((base + a) * 2 + half) * SLOTS + slot], {'tp': plane.blk(half, *to)})

    def f(a, half, k, end):
        step = WALK[k]
        return msg(a, half, min(k, 2), (step[end], 0), None if end and k > 1 else step[2], (step[3], 0))

    def s(a, half, j, k, end):
        step = WALK[k]
        return msg(a, half, 3 * (j + 1) + min(k, 2), (HOPS[j], step[end]), None if end and k > 1 else step[2], (0, step[3]))

    send, recv = BOTH
    pairs = [(a, half) for a in range(len(bufs)) for half in BOTH]

    def across(a, half, j):
        for k in BOTH:
            s(a, half, j, k, send).start()
        on_block(a, half, j, 0)

    def onward(a, half, j):
        for k in BOTH:
            s(a, half, j, k, recv).wait_recv()
            s(a, half, j, k + 2, send).start()
            on_block(a, half, j, k + 1)

    if not begun:
        for pair in pairs:
            for k in BOTH:
                f(*pair, k, send).start()
            across(*pair, 0)
        yield
    for pair in pairs:
        for k in BOTH:
            f(*pair, k, recv).wait_recv()
            f(*pair, k + 2, send).start()
            across(*pair, k + 1)
    yield
    for pair in pairs:
        onward(*pair, 0)
    yield
    for pair in pairs:
        f(*pair, 2, recv).wait_recv()
        across(*pair, SIDE - 1)
    yield
    for j in range(1, SIDE):
        for pair in pairs:
            onward(*pair, j)
        yield
    for j in range(SIDE):
        for pair in pairs:
            s(*pair, j, 2, recv).wait_recv()
            on_block(*pair, j, SIDE - 1)
        if j % 2:
            yield
    for a, (buf, start, size) in enumerate(bufs):
        sent = buf.at[pl.ds(0, SIDE * SIDE - 1), pl.ds(start, size)]
        remote(sent, sent, send_sem.at[base + a], recv_sem.at[0], {'tp': plane.at(1, 0)}).wait_send()


def tiles(width):
    return [slice(n, n + TILE) for n in range(0, width, TILE)]


def drain(steps):
    for _ in steps:
        pass


def local(src, dst, sem):
    return pltpu.make_async_copy(src, dst, sem)


class Reduce:
    def __init__(self, plane, parts, got_one, sum_one, got_two, one_send, one_recv, two_send, two_recv):
        self.plane, self.parts, self.got_one, self.sum_one, self.got_two = plane, parts, got_one, sum_one, got_two
        self.one_send, self.one_recv, self.two_send, self.two_recv = one_send, one_recv, two_send, two_recv

    def row(self, half, index):
        size = self.parts.shape[3] // 2
        cols = pl.ds(half * size, size)
        return self.parts.at[:, index, :, cols] if half == 0 else self.parts.at[index, :, :, cols]

    def here(self, half):
        return (self.plane.y, self.plane.z) if half == 0 else (self.plane.z, self.plane.y)

    def first(self, half, d):
        n = half * 3 + d - 1
        dest = lax.rem(self.here(half)[0] + d, SIDE)
        return remote(self.row(half, dest), self.got_one.at[n], self.one_send, self.one_recv.at[half], {'tp': self.plane.blk(half, d, 0)})

    def second(self, half, d):
        n = half * 3 + d - 1
        dest = lax.rem(self.here(half)[1] + d, SIDE)
        return remote(self.sum_one.at[half, dest], self.got_two.at[n], self.two_send, self.two_recv.at[half], {'tp': self.plane.blk(half, 0, d)})

    def whole(self, got, send, recv, half=None):
        ref = got if half is None else got.at[pl.ds(half * 3, 3)]
        return remote(ref, ref, send, recv.at[half or 0], {'tp': self.plane.at(1, 0)})

    def begin(self, half):
        for d in (2, 1, 3):
            self.first(half, d).start()

    def middle(self):
        for half in BOTH:
            total = self.row(half, self.here(half)[0])[:].astype(F32)
            self.whole(self.got_one, self.one_send, self.one_recv, half).wait_recv()
            for d in (1, 3, 2):
                total = total + self.got_one[half * 3 + d - 1].astype(F32)
            self.sum_one[half] = total.astype(self.sum_one.dtype)
            for d in (2, 1, 3):
                self.second(half, d).start()

    def end(self):
        sums = []
        for half in BOTH:
            total = self.sum_one[half, self.here(half)[1]].astype(F32)
            self.whole(self.got_two, self.two_send, self.two_recv, half).wait_recv()
            for d in (1, 3, 2):
                total = total + self.got_two[half * 3 + d - 1].astype(F32)
            sums.append(total)
        return sums

    def close(self):
        self.whole(self.got_one, self.one_send, self.one_recv).wait_send()
        self.whole(self.got_two, self.two_send, self.two_recv).wait_send()


def fold(op, value):
    rows, cols = value.shape
    return op(value.reshape(rows // 8, 8, cols), axis=0)


def flatten(ids, flat):
    size, cols = ids.shape[1], flat.shape[1]
    for r in range(ids.shape[0]):
        at = r * size
        flat[at // cols:at // cols + 1, at % cols:at % cols + size] = ids[r:r + 1, :]


def list_rows(tokens, base, rows, group, unit, flat, slot, out):
    lines, lanes = flat.shape
    count = lines * lanes
    flatten(tokens, flat)
    row = flat[:] - base
    mine = (row >= 0) & (row < rows)
    upper = lax.broadcasted_iota(jnp.int32, (lanes, lanes), 0) <= lax.broadcasted_iota(jnp.int32, (lanes, lanes), 1)
    ones = [jnp.where(mask, 1.0, 0.0).astype(BF16) for mask in (mine, upper)]
    seen = dot(*ones)
    total = jnp.zeros((1, 1), F32)
    for r in range(lines):
        line = slice(r, r + 1)
        here = slice(r * lanes, (r + 1) * lanes)
        slot[:1, here] = jnp.where(mine[line], seen[line] + (total - 1.0), -1.0).astype(jnp.int32)
        slot[1:, here] = row[line]
        total = total + seen[line, lanes - 1:]
    number = lax.broadcasted_iota(jnp.int32, (1, count), 1)
    inner = lax.rem(number, group)
    place = inner // unit * (count // group * unit) + number // group * unit + lax.rem(number, unit)
    digits = [part for value in (place, slot[1:, :]) for part in (value // 256, lax.rem(value, 256))]
    which = lax.broadcasted_iota(jnp.int32, (16, count), 0)
    values = sum(jnp.where(which == i, digit, 0) for i, digit in enumerate(digits)).astype(F32).astype(BF16)

    @pl.loop(0, count // group)
    def _(c):
        start = pl.multiple_of(c * group, group)
        pick = jnp.where(slot[:1, :] == start + lax.broadcasted_iota(jnp.int32, (group, count), 0), 1.0, 0.0).astype(BF16)
        found = cols_dot(values, pick)
        for i in BOTH:
            out[i:i + 1, pl.ds(start, group)] = (found[2 * i:2 * i + 1] * 256.0 + found[2 * i + 1:2 * i + 2]).astype(jnp.int32)

    out[2:, :] = jnp.broadcast_to(total, (1, count)).astype(jnp.int32)


def norm_of(x):
    wide = x.astype(F32)
    inv_rms = lax.rsqrt(jnp.mean(wide * wide, axis=-1, keepdims=True) + NORM_EPS)
    return inv_rms, wide * inv_rms


class Spread:
    def __init__(self, plane, source, stages, src, out, line_send, line_recv, die_send, die_recv):
        self.plane, self.source, self.stages, self.src, self.out = plane, source, stages, src, out
        self.line_send, self.line_recv, self.die_send, self.die_recv = line_send, line_recv, die_send, die_recv
        self.stage = lax.axis_index('pp')
        self.core = lax.rem(self.stage, 2)
        self.mate = {'pp': self.stage + 1 - 2 * self.core}
        self.rows = out.shape[1] // 2
        self.lo = pl.multiple_of(self.core * self.rows, self.rows)
        self.others = [p for p in range(stages) if p != source]

    def greet(self):
        source = self.stage == self.source
        twin = self.stage == self.source ^ 1
        pl.when(source)(functools.partial(signal, {'pp': self.source ^ 1}))
        pl.when(jnp.logical_not(source))(functools.partial(signal, {'pp': self.source}))
        pl.when(jnp.logical_not(source | twin))(functools.partial(signal, self.mate))
        return jnp.where(source, len(self.others), 1)

    def line(self, p):
        part = pl.ds((p % 2) * self.rows, self.rows)
        return remote(self.src.at[part], self.out.at[self.plane.tp, part], self.line_send, self.line_recv, {'pp': p})

    def send(self):
        for p in self.others:
            self.line(p).start()
        part = pl.ds(self.lo, self.rows)
        self.out[self.plane.tp, part] = self.src[part]

    def arrive(self):
        mine = self.out.at[self.plane.tp, pl.ds(self.lo, self.rows)]
        remote(mine, mine, self.line_recv, self.line_recv, self.mate).wait_recv()

    def on_block(self, a, half, j, k):
        if a == 0:
            size = self.rows // 2
            ref = self.out.at[self.plane.blk(half, HOPS[j], HOPS[k]), pl.ds(self.lo + half * size, size)]
            remote(ref, ref, self.die_send, self.die_recv, self.mate).start()

    def half(self, lo):
        ref = self.out.at[:, pl.ds(lo, self.rows)]
        return remote(ref, ref, self.die_send, self.die_recv, self.mate)

    def finish(self):
        self.half(pl.multiple_of((1 - self.core) * self.rows, self.rows)).wait_recv()

    def close(self):
        self.half(self.lo).wait_send()

        @pl.when(self.stage == self.source)
        def _():
            sent = self.out.at[pl.ds(0, len(self.others)), pl.ds(self.lo, self.rows)]
            remote(sent, sent, self.line_send, self.line_recv, self.mate).wait_send()


def forward_kernel(last, tokens, emb, w_one, w_two, top, own_x, table, order_out, hid_out, one_out, two_out, x_out, ones, twos, one_t, two_t, hot, parts,
                   got_one, sum_one, got_two, piece, x_buf, y_buf, n_src, a_buf, hid_ref, x_all, ids, flat, slot,
                   send_sem, recv_sem, one_send, one_recv, two_send, two_recv, line_send, line_recv, own_send, own_recv, spread_send, spread_recv, die_send, die_recv,
                   hop_send, hop_recv, lead_sem, loc_sem):
    plane = Plane()
    stage = lax.axis_index('pp')
    tp = plane.tp
    stages = last + 1
    core = lax.rem(stage, 2)
    moves = ((emb, table), (w_one, ones.at[tp]), (w_two, twos.at[tp]), (one_t, one_out), (two_t, two_out), (hid_ref, hid_out), (x_all, x_out))
    load, own_one, own_two, *saves = [local(src, dst, loc_sem.at[i]) for i, (src, dst) in enumerate(moves)]
    save_one, save_two, save_hid, save_x = saves
    load.start()
    own_one.start()
    own_two.start()
    for peer in plane.rings() + [{'pp': lax.rem(stage + d, stages)} for d in range(1, stages)]:
        signal(peer)

    own_one.wait()
    own_two.wait()
    pl.semaphore_wait(pltpu.get_barrier_semaphore(), 6 + last)
    def weight_steps(begun=False):
        return plane_gather(plane, [(ones, 0, ones.shape[1]), (twos, 0, twos.shape[1])], send_sem, recv_sem, begun=begun)

    @pl.when(core == 0)
    def _():
        next(weight_steps())

    rows, width = table.shape
    group = ids.shape[1]
    unit = piece.shape[0]
    count = group // tokens.shape[1]
    flatten(tokens.at[pl.ds(pl.multiple_of(stage * count, count), count)], ids)
    hot[:] = jnp.where(ids[:] - tp * rows == lax.broadcasted_iota(jnp.int32, hot.shape, 0), 1.0, 0.0).astype(BF16)
    load.wait()
    cut = rows // group * group
    for cols in tiles(width):
        picked = rows_dot(hot[:cut], table[:cut, cols]) + rows_dot(hot[cut:], table[cut:, cols])
        parts[:, :, :, cols] = picked.astype(BF16).reshape(*parts.shape[:-1], TILE)
    red = Reduce(plane, parts, got_one, sum_one, got_two, one_send, one_recv, two_send, two_recv)
    for half in BOTH:
        red.begin(half)

    @pl.when(core == 1)
    def _():
        pl.semaphore_wait(lead_sem, 1)
        next(weight_steps())

    gather = weight_steps(True)
    next(gather)

    @pl.when(core == 0)
    def _():
        pl.semaphore_signal(lead_sem, inc=1, device_id={'pp': stage + 1}, device_id_type=MESH)

    next(gather)
    red.middle()
    next(gather)
    next(gather)
    for half, total in enumerate(red.end()):
        piece[:, half * (width // 2):(half + 1) * (width // 2)] = total.astype(BF16)

    def line(p):
        return remote(piece, x_buf.at[pl.ds(pl.multiple_of(p * unit, unit), unit)], line_send, line_recv, {'pp': 0})

    @pl.when(stage != 0)
    def _():
        line(stage).start()

    @pl.when(stage == 0)
    def _():
        x_buf[:unit] = piece[:]

    drain(gather)

    @pl.when(stage == 1)
    def _():
        pl.semaphore_signal(lead_sem, inc=1, device_id={'pp': 0}, device_id_type=MESH)

    blocks, _, cols = ones.shape

    def spare_time():
        @pl.loop(0, blocks)
        def _(k):
            one_t[k] = ones[k].T
            two_t[k] = twos[k].T

        save_one.start()
        save_two.start()
        list_rows(tokens, tp * rows, rows, group, unit, flat, slot, order_out)

    pl.when(stage > 1)(spare_time)
    hop = remote(y_buf, x_buf, hop_send, hop_recv, {'pp': lax.rem(stage + 1, stages)})

    @pl.when(stage == 0)
    def _():
        got = x_buf.at[pl.ds(0, last * unit)]
        remote(got, got, line_send, line_recv, {'pp': last}).wait_recv()

    pl.when(stage > 0)(hop.wait_recv)
    x_act = x_buf[:]
    for k in range(blocks):
        hidden = dot(x_act, ones[k])
        hid_ref[k] = hidden
        a_buf[:, k * cols:(k + 1) * cols] = gelu(hidden).astype(BF16)
    save_hid.start()
    gate = a_buf[:]
    for tile in tiles(width):
        branch = dot(gate, twos[:, :, tile].reshape(blocks * cols, TILE))
        y_buf[:, tile] = (x_buf[:, tile].astype(F32) + branch).astype(BF16)

    pl.when(stage < last)(hop.start)
    x_all[tp] = x_buf[:]

    @pl.when(stage < SIDE)
    def _():
        pl.when(stage <= 1)(spare_time)

        @pl.when(stage == 0)
        def _():
            pl.semaphore_wait(lead_sem, 1)

        steps = plane_gather(plane, [(x_all, 0, x_all.shape[1])], send_sem, recv_sem, base=2)
        drain(steps)

    own_save = local(x_all.at[tp], x_out.at[tp], loc_sem.at[6])
    pl.when(stage < SIDE)(save_x.start)
    pl.when(stage >= SIDE)(own_save.start)

    spread = Spread(plane, last, stages, n_src, top, spread_send, spread_recv, die_send, die_recv)

    def own(p):
        return remote(y_buf.at[pl.ds(p * unit, unit)], own_x, own_send, own_recv, {'pp': p})

    @pl.when(stage == last)
    def _():
        n_src[:] = norm_of(y_buf[:])[1].astype(BF16)
        spread.send()
        for p in spread.others:
            own(p).start()
        own_x[:] = y_buf[last * unit:]

    pl.when(stage < last)(spread.arrive)
    drain(plane_gather(plane, [(top, spread.lo, spread.rows)], send_sem, recv_sem, spread.on_block, base=3))
    spread.finish()
    pl.when(stage < last)(own(last).wait_recv)
    spread.close()

    @pl.when(stage == last)
    def _():
        sent = y_buf.at[pl.ds(0, last * unit)]
        remote(sent, sent, own_send, own_recv, spread.mate).wait_send()

    red.close()

    @pl.when(stage != 0)
    def _():
        line(stage).wait_send()

    pl.when(stage < last)(hop.wait_send)
    for save in saves[:-1]:
        save.wait()
    pl.when(stage < SIDE)(save_x.wait)
    pl.when(stage >= SIDE)(own_save.wait)


def head_kernel(target, stages, chunk, table, top, own_x, labels, loss_out, g_top, g_out, n_out,
                n_buf, lab, g_buf, peak, stat, shared, scale_ref, parts, got_one, sum_one, got_two, piece,
                share_send, share_recv, one_send, one_recv, two_send, two_recv, line_send, line_recv, loc_sem, *e_bufs):
    plane = Plane()
    stage = lax.axis_index('pp')
    tp = plane.tp
    size = shared.shape[1]
    others = [p for p in range(stages) if p != target]
    each, group = peak.shape[1:]
    unit = group // size
    for d in range(1, size):
        signal({'tp': lax.rem(tp + d, size)})

    @pl.when(stage == target)
    def _():
        for p in others:
            signal({'pp': p})

    pl.when(stage != target)(functools.partial(signal, {'pp': target}))
    for p in range(stages):
        n_buf[p * group:(p + 1) * group] = top[:, p * unit:(p + 1) * unit, :].reshape(group, top.shape[2])
    save_n = local(n_buf, n_out, loc_sem.at[1])
    save_n.start()

    rows, width = table.shape
    flatten(labels, lab)
    lab[:] = lab[:] - tp * rows
    pieces = len(e_bufs)
    pair = each * group

    def group_at(b, i):
        return lax.rem(stage // each + b, pieces) * each + i

    def label_of(p):
        return lab[pl.ds(p, 1), :]

    def down(value, start):
        return start + lax.broadcasted_iota(jnp.int32, value.shape, 0)

    def logit_chunk(b, start):
        tokens = n_buf[pl.ds(pl.multiple_of(group_at(b, 0) * group, pair), pair), :]
        logits = cols_dot(table[pl.ds(start, chunk), :], tokens)
        e_bufs[b][pl.ds(start, chunk), :] = logits
        return fold(jnp.max, logits)

    def exp_chunk(b, start, label, top_b, total, hits):
        logits = e_bufs[b][pl.ds(start, chunk), :]
        e = jnp.exp(logits - top_b)
        e_bufs[b][pl.ds(start, chunk), :] = e
        return total + fold(jnp.sum, e), hits + fold(jnp.sum, jnp.where(label == down(logits, start), logits, 0.0))

    def chunks(body, carry):
        return lax.fori_loop(0, rows // chunk, lambda c, carry: body(pl.multiple_of(c * chunk, 8), carry), carry)

    def msg(d, k):
        some = pl.ds(k, 1 + k * (pieces - 2))
        return remote(stat.at[some], shared.at[some, tp], share_send.at[k], share_recv.at[k], {'tp': lax.rem(tp + d, size)})

    def shares(k):
        ref = shared.at[pl.ds(k, 1 + k * (pieces - 2)), pl.ds(0, size - 1)]
        return remote(ref, ref, share_send.at[k], share_recv.at[k], {'tp': plane.at(1, 0)})

    def share(k):
        for d in range(1, size):
            msg(d, k).start()

    losses = []

    def normalise(k):
        shares(k).wait_recv()
        for b in (range(1, pieces) if k else range(1)):
            every = shared[b, :, 0]
            most = jnp.max(every, axis=0)
            log_norm = most + jnp.log(jnp.sum(jnp.exp(every - most[None]), axis=0))
            losses.append(jnp.sum(log_norm - jnp.sum(shared[b, :, 1], axis=0), keepdims=True))
            scale_ref[b] = jnp.exp(peak[b] - log_norm)

    def grad_block(b, i, slot):
        cols = pl.ds(pl.multiple_of(i * group, group), group)
        label = label_of(group_at(b, i))
        factor = scale_ref[b, pl.ds(i, 1), :]

        def part(start, _):
            e = e_bufs[b][pl.ds(start, chunk), cols]
            hit = label == down(e, start)
            g_buf[slot, pl.ds(start, chunk), :] = (e * factor - jnp.where(hit, 1.0, 0.0)).astype(BF16)

        chunks(part, None)

    def save(k):
        slot = 1 + k % 2
        at = pl.multiple_of(group_at(k // each, k % each) * group, group)
        return local(g_buf.at[slot], g_out.at[:, pl.ds(at, group)], loc_sem.at[2 + slot])

    def gradient(k):
        if k >= 2:
            save(k - 2).wait()
        grad_block(k // each, k % each, 1 + k % 2)
        save(k).start()

    cut = rows // group * group
    half = width // 2
    red = Reduce(plane, parts, got_one, sum_one, got_two, one_send, one_recv, two_send, two_recv)

    def own_gradient():
        grad_block(0, lax.rem(stage, each), 0)
        mine_g = g_buf.at[0]
        for cols in tiles(width):
            back = rows_dot(mine_g[:cut, :], table[:cut, cols]) + rows_dot(mine_g[cut:, :], table[cut:, cols])
            parts[:, :, :, cols] = back.reshape(*parts.shape[:-1], TILE)
            if cols.stop % half == 0:
                red.begin(cols.start // half)

    tops = []
    zero = jnp.zeros((8, pair), F32)
    for now, done in ((0, None), (None, 0), (1, None), *((b, b - 1) for b in range(2, pieces)), (None, pieces - 1)):
        label = None if done is None else jnp.concatenate([label_of(group_at(done, i)) for i in range(each)], axis=1)
        top_b = None if done is None else tops[done]

        def both(start, carry, now=now, done=done, top_b=top_b, label=label):
            best, total, hits = carry
            if now is not None:
                best = jnp.maximum(best, logit_chunk(now, start))
            if done is not None:
                total, hits = exp_chunk(done, start, label, top_b, total, hits)
            return best, total, hits

        best, total, hits = chunks(both, (jnp.full((8, pair), -jnp.inf, F32), zero, zero))
        if done is not None:
            found = (top_b + jnp.log(jnp.sum(total, axis=0, keepdims=True)), jnp.sum(hits, axis=0, keepdims=True), top_b)
            for i in range(each):
                cols = slice(i * group, (i + 1) * group)
                for kind in BOTH:
                    stat[done, kind, i:i + 1, :] = found[kind][:, cols]
                peak[done, i:i + 1, :] = found[2][:, cols]
            shared[done, tp] = stat[done]
        if done == 0:
            pl.semaphore_wait(pltpu.get_barrier_semaphore(), size - 1 + jnp.where(stage == target, len(others), 1))
        if now is None:
            share(1 if done else 0)
        else:
            tops.append(jnp.max(best, axis=0, keepdims=True))
        if now == 1:
            normalise(0)
            own_gradient()
        if now == pieces - 1:
            red.middle()

    gradient(0)
    gradient(1)
    sums = red.end()

    inv_rms, normed = norm_of(own_x[:])
    mean = (jnp.sum(normed[:, :half] * sums[0], axis=-1, keepdims=True) + jnp.sum(normed[:, half:] * sums[1], axis=-1, keepdims=True)) / width
    for h in BOTH:
        cols = slice(h * half, (h + 1) * half)
        piece[:, cols] = (inv_rms * (sums[h] - normed[:, cols] * mean)).astype(BF16)

    def line(p):
        return remote(piece, g_top.at[p], line_send, line_recv, {'pp': target})

    @pl.when(stage != target)
    def _():
        line(stage).start()

    normalise(1)
    for k in range(2, stages):
        gradient(k)
    loss_out[:] = sum(losses) / (stages * group)
    @pl.when(stage == target)
    def _():
        g_top[target] = piece[:]
        got = g_top.at[pl.ds(0, len(others))]
        remote(got, got, line_send, line_recv, {'pp': 0}).wait_recv()

    red.close()
    for k in BOTH:
        shares(k).wait_send()
    save_n.wait()
    save(stages - 2).wait()
    save(stages - 1).wait()
    @pl.when(stage != target)
    def _():
        line(stage).wait_send()


def backward_kernel(last, chunk, g_top, hid_in, two_all, one_all, g_all, n_all, x_in, w_one, w_two, de_buf, dx_all, grad_one, grad_two,
                    ones, twos, slope_ref, g_buf, n_buf, x_all, w_one_buf, w_two_buf, dy_all, dy_buf, dx_buf, d_buf,
                    send_sem, recv_sem, spread_send, spread_recv, die_send, die_recv, hop_send, hop_recv, go_sem, ready_sem, g_sem, loc_sem):
    plane = Plane()
    stage = lax.axis_index('pp')
    stages = last + 1
    blocks, cols, width = one_all.shape
    pairs = ((hid_in, slope_ref), (two_all, twos), (one_all, ones), (n_all, n_buf), (w_one, w_one_buf), (w_two, w_two_buf))
    loads = [local(src, dst, loc_sem.at[i]) for i, (src, dst) in enumerate(pairs)]
    lower = stage < SIDE
    upper = stage >= SIDE
    own = plane.tp
    load_x = [local(*pair, loc_sem.at[6]) for pair in ((x_in, x_all), (x_in.at[own], x_all.at[own]))]

    mid = upper & (stage < last - 1)

    def start(some):
        for load in some:
            load.start()

    pl.when(upper)(functools.partial(start, loads[:3]))
    pl.when(lower)(functools.partial(start, loads[3:4]))
    own_load = load_x[1]
    pl.when(mid)(own_load.start)
    spread = Spread(plane, 0, stages, dx_buf, dx_all, spread_send, spread_recv, die_send, die_recv)
    near = plane.near()
    for peer in near:
        signal(peer)
    extra = spread.greet()
    before = {'pp': lax.rem(stage + last, stages)}
    pl.when(stage > 0)(functools.partial(signal, before))
    hop = remote(dx_buf, dy_buf, hop_send, hop_recv, before)
    rows = de_buf.shape[0]
    pieces = -(-rows // chunk)

    def piece_at(c):
        return pl.ds(pl.multiple_of(jnp.minimum(c * chunk, rows - chunk), 8), chunk)

    def fetch(c):
        slot = lax.rem(c, 2)
        return local(g_all.at[piece_at(c)], g_buf.at[slot], g_sem.at[slot])

    def table(lo, hi):
        if lo == 0:
            fetch(0).start()
            loads[3].wait()

        @pl.loop(lo, hi)
        def _(c):
            @pl.when(c < pieces - 1)
            def _():
                fetch(c + 1).start()

            for i, some in enumerate((loads[:2], loads[2:3], loads[4:] + load_x[:1])):
                pl.when(lower & (c == i + 1))(functools.partial(start, some))

            fetch(c).wait()
            de_buf[piece_at(c), :] = dot(g_buf[lax.rem(c, 2)], n_buf[:])

    pl.semaphore_wait(pltpu.get_barrier_semaphore(), len(near) + extra + jnp.where(stage < last, 1, 0))

    @pl.when(stage < last)
    def _():
        pl.semaphore_signal(ready_sem, inc=1, device_id={'pp': lax.rem(stage + 1, stages)}, device_id_type=MESH)

    pl.when(lower)(functools.partial(table, 0, pieces))
    loads[0].wait()
    for k in range(blocks):
        slope_ref[k] = gelu_slope(slope_ref[k])
    loads[1].wait()

    def a_steps(begun=False):
        return plane_gather(plane, [(x_all, 0, x_all.shape[1])], send_sem, recv_sem, base=2, begun=begun)

    mid_steps = a_steps()

    @pl.when(mid)
    def _():
        own_load.wait()
        for _ in range(3):
            next(mid_steps)

    @pl.when(stage == last)
    def _():
        dy_buf[:] = g_top[:]

    pl.when(stage < last)(hop.wait_recv)
    dy_all[plane.tp] = dy_buf[:]
    whole = (dy_all, 0, dy_all.shape[1])
    part = (dx_all, spread.lo, spread.rows)

    def dy_steps(begun):
        return plane_gather(plane, [whole], send_sem, recv_sem, base=1, begun=begun)

    @pl.when(stage <= 1)
    def _():
        next(dy_steps(False))

    grad_y = dy_buf[:]
    for k in range(blocks):
        grad_gate = dot(grad_y, twos[k])
        d_buf[:, k * cols:(k + 1) * cols] = (slope_ref[k] * grad_gate).astype(BF16)
    loads[2].wait()
    grad_hidden = d_buf[:]
    for tile in tiles(width):
        back = dot(grad_hidden, ones[:, :, tile].reshape(blocks * cols, TILE))
        dx_buf[:, tile] = (dy_buf[:, tile].astype(F32) + back).astype(BF16)

    @pl.when(stage > 0)
    def _():
        pl.semaphore_wait(ready_sem, 1)
        hop.start()

    pl.when(stage == 0)(spread.send)
    pl.when(upper)(functools.partial(start, loads[3:]))
    pl.when(upper & jnp.logical_not(mid))(own_load.start)
    for load in loads[4:]:
        load.wait()
    pl.when(lower)(load_x[0].wait)
    pl.when(upper & jnp.logical_not(mid))(own_load.wait)

    grad_one[:] = jnp.zeros_like(grad_one)
    grad_two[:] = jnp.zeros_like(grad_two)

    def weights(ahead):
        step = SIDE

        @pl.loop(0, 2)
        def _(i):
            row = lax.rem(plane.z + (1 + i if ahead else SIDE - i), SIDE)
            part = pl.ds(row * step, step)
            x_act = x_all[part].reshape(step * x_all.shape[1], width)
            grad_y = dy_all[part].reshape(step * x_all.shape[1], width)
            hidden = dot(x_act, w_one_buf[:])
            grad_gate = cols_dot(grad_y, w_two_buf[:])
            grad_hidden = (gelu_slope(hidden) * grad_gate).astype(BF16)
            grad_one[:] += rows_dot(x_act, grad_hidden)
            grad_two[:] += rows_dot(gelu(hidden).astype(BF16), grad_y)

    def dx_steps():
        return plane_gather(plane, [part], send_sem, recv_sem, spread.on_block)

    @pl.when(stage > 1)
    def _():
        hop.wait_send()

        @pl.when(spread.core == 0)
        def _():
            pl.semaphore_signal(go_sem, inc=1, device_id=spread.mate, device_id_type=MESH)

        @pl.when(spread.core == 1)
        def _():
            pl.semaphore_wait(go_sem, 1)

    @pl.when(stage > 1)
    def _():
        next(dy_steps(False))

    @pl.when(upper & jnp.logical_not(mid))
    def _():
        next(a_steps())

    planes = [(stage <= 1, None, 'dxddxdxdxdx', 'xx'), ((stage > 1) & lower, None, 'dddxdxdxdx', 'xxx'),
              (mid, mid_steps, 'dtdadatdaxdaxdx', 'xxx'), (upper & jnp.logical_not(mid), a_steps(True), 'datdadatdaxdaxdax', 'xxx')]
    runs = []
    for here, more, order, rest in planes:
        steps = {'d': dy_steps(True), 'x': dx_steps(), 'a': more}

        def arrived(order=order, steps=steps):
            part = -(-pieces // 2)
            for i, kind in enumerate(order):
                if kind == 't':
                    lo = order[:i].count('t') * part
                    table(lo, min(lo + part, pieces))
                    continue
                if kind == 'x' and 'x' not in order[:i]:
                    pl.when(stage > 0)(spread.arrive)
                next(steps[kind])
            next(steps['d'])
            drain(steps['a'] or ())

        def onward(rest=rest, steps=steps):
            for kind in rest:
                next(steps[kind])
            drain(steps['d'])

        pl.when(here)(arrived)
        runs.append((here, onward, functools.partial(drain, steps['x'])))

    weights(False)
    for here, onward, _ in runs:
        pl.when(here)(onward)
    weights(True)
    for here, _, finish in runs:
        pl.when(here)(finish)

    spread.finish()
    spread.close()

    pl.when(stage == 1)(hop.wait_send)


def add_kernel(pieces, order, dx_ref, de_ref, one_ref, two_ref, de_out, table_out, one_out, two_out, wide, sem):
    saves = [local(one_ref, one_out, sem.at[0]), local(two_ref, two_out, sem.at[1])]
    for save in saves:
        save.start()
    wide[:] = dx_ref[:].astype(F32)

    @pl.loop(0, order[2, 0])
    def _(j):
        row = pl.ds(order[1, j], 1)
        de_out[row, :] = de_out[row, :] + wide[pl.ds(order[0, j], 1), :]

    rows = de_ref.shape[0]
    size = -(-rows // (8 * pieces)) * 8
    for c in range(pieces):
        part = pl.ds(c * size, min(size, rows - c * size))
        saves.append(local(de_out.at[part], table_out.at[part], sem.at[2 + c]))
        saves[-1].start()
    for save in saves:
        save.wait()


def vmem():
    return pl.BlockSpec(memory_space=pltpu.VMEM)


def anywhere():
    return pl.BlockSpec(memory_space=pl.ANY)


def params(cid, mib):
    return pltpu.CompilerParams(collective_id=cid, has_side_effects=True, vmem_limit_bytes=mib << 20)


DMA = pltpu.SemaphoreType.DMA


def solution(mesh):
    pp_size = mesh.shape['pp']
    tp_size = mesh.shape['tp']
    last = pp_size - 1

    def device_fn(tokens, labels, emb_table, w_in, w_out):
        num_tokens = tokens.shape[0] * tokens.shape[1]
        vocab_rows, width = emb_table.shape
        w_one, w_two = w_in[0], w_out[0]
        cols = w_one.shape[1]
        unit = num_tokens // (pp_size * tp_size)
        block = pp_size * unit
        group = tp_size * unit
        half = width // 2
        chunk = vocab_rows // 3
        step = 512
        pair = 2 * group
        shape = jax.ShapeDtypeStruct
        VM = pltpu.VMEM

        def reduce_scratch(dtype):
            return [VM((SIDE, SIDE, unit, width), dtype), VM((6, SIDE, unit, half), dtype), VM((2, SIDE, unit, half), dtype), VM((6, unit, half), dtype), VM((unit, width), BF16)]

        duo = DMA((2,))
        reduce_sems = [DMA, duo, DMA, duo, DMA, DMA]
        many = shape((tp_size, block, width), BF16)
        many_buf = VM((tp_size, block, width), BF16)
        two_sums = 2 * SLOTS
        gather_sems = [DMA((4,)), DMA((4 * two_sums,))]
        spread_sems = [DMA, DMA, DMA, DMA]

        top, own_x, table, order, hidden, one_t, two_t, x_all = pl.pallas_call(
            functools.partial(forward_kernel, last),
            out_shape=(many_buf, VM((unit, width), BF16), VM((vocab_rows, width), BF16), shape((3, num_tokens), jnp.int32), shape((tp_size, block, cols), F32), shape((tp_size, cols, width), BF16), shape((tp_size, width, cols), BF16), many),
            in_specs=[vmem()] + [anywhere()] * 3,
            out_specs=[vmem()] * 4 + [anywhere()] * 4,
            scratch_shapes=[VM((tp_size, width, cols), BF16), VM((tp_size, cols, width), BF16), VM((tp_size, cols, width), BF16), VM((tp_size, width, cols), BF16),
                            VM((vocab_rows, group), BF16), *reduce_scratch(BF16),
                            VM((block, width), BF16), VM((block, width), BF16), VM((block, width), BF16), VM((block, tp_size * cols), BF16), VM((tp_size, block, cols), F32), many_buf, VM((1, group), jnp.int32),
                            VM((num_tokens // 128, 128), jnp.int32), VM((2, num_tokens), jnp.int32),
                            *gather_sems, *reduce_sems, DMA, DMA, *spread_sems, DMA, DMA, pltpu.SemaphoreType.REGULAR, DMA((7,))],
            compiler_params=params(1, 49), name='forward_chain',
        )(tokens, emb_table, w_one, w_two)

        by_pair = (num_tokens // pair, pair // group, group)
        loss, g_top, g_all, n_all = pl.pallas_call(
            functools.partial(head_kernel, last, pp_size, chunk),
            out_shape=(shape((1, 1), F32), pltpu.HBM((pp_size, unit, width), BF16), shape((vocab_rows, num_tokens), BF16), shape((num_tokens, width), BF16)),
            in_specs=[vmem()] * 4,
            out_specs=[vmem()] * 2 + [anywhere()] * 2,
            scratch_shapes=[VM((num_tokens, width), BF16), VM((pp_size, group), jnp.int32), VM((3, vocab_rows, group), BF16),
                            VM(by_pair, F32), VM((by_pair[0], 2, *by_pair[1:]), F32), VM((by_pair[0], tp_size, 2, *by_pair[1:]), F32), VM(by_pair, F32), *reduce_scratch(F32),
                            duo, duo, *reduce_sems, DMA((5,)),
                            *[VM((vocab_rows, pair), F32) for _ in range(num_tokens // pair)]],
            compiler_params=params(2, 49), name='head',
        )(*[pltpu.with_memory_space_constraint(array, pltpu.VMEM) for array in (table, top, own_x)], labels)

        de_head, dx_first, grad_one, grad_two = pl.pallas_call(
            functools.partial(backward_kernel, last, step),
            out_shape=(VM((vocab_rows, width), F32), many_buf, VM((width, cols), F32), VM((cols, width), F32)),
            in_specs=[vmem()] + [anywhere()] * 8, out_specs=[vmem()] * 4,
            scratch_shapes=[VM((tp_size, cols, width), BF16), VM((tp_size, width, cols), BF16), VM((tp_size, block, cols), F32), VM((2, step, num_tokens), BF16), VM((num_tokens, width), BF16),
                            many_buf, VM((width, cols), BF16), VM((cols, width), BF16), many_buf,
                            VM((block, width), BF16), VM((block, width), BF16), VM((block, tp_size * cols), BF16),
                            *gather_sems, *spread_sems, DMA, DMA, pltpu.SemaphoreType.REGULAR, pltpu.SemaphoreType.REGULAR, duo, DMA((7,))],
            compiler_params=params(3, 45), name='backward_chain',
        )(g_top.reshape(block, width), hidden, two_t, one_t, g_all, n_all, x_all, w_one, w_two)

        smem = pl.BlockSpec(memory_space=pltpu.SMEM)
        _, grad_table, grad_one, grad_two = pl.pallas_call(
            functools.partial(add_kernel, 12),
            out_shape=(VM((vocab_rows, width), F32), shape((vocab_rows, width), F32), shape((width, cols), F32), shape((cols, width), F32)),
            in_specs=[smem] + [vmem()] * 4, out_specs=[vmem()] + [anywhere()] * 3,
            scratch_shapes=[VM((num_tokens, width), F32), DMA((14,))], input_output_aliases={2: 0},
            compiler_params=pltpu.CompilerParams(vmem_limit_bytes=24 << 20), name='add_rows',
        )(order, dx_first.reshape(num_tokens, width), de_head, grad_one, grad_two)
        return loss.reshape(1), grad_one[None], grad_two[None], grad_table

    return jax.shard_map(device_fn, mesh=mesh, in_specs=(P('dp', None), P('dp', None), P('tp', None), P('pp', None, 'tp'), P('pp', 'tp', None)), out_specs=(P('dp'), P(('dp', 'pp'), None, 'tp'), P(('dp', 'pp'), 'tp', None), P(('dp', 'tp'), None)), check_vma=False)
```

```python
import functools

import jax
import jax.numpy as jnp
from jax import lax
from jax.experimental import pallas as pl
from jax.experimental.pallas import tpu as pltpu
from jax.sharding import PartitionSpec as P

NORM_EPS = 1e-6
SIDE = 4
MESH = pl.DeviceIdType.MESH
F32 = jnp.float32
BF16 = jnp.bfloat16
CUBE = 0.044715
ROOT = 0.7978845608028654


def dot(lhs, rhs):
    return jnp.dot(lhs, rhs, preferred_element_type=F32)


def rows_dot(lhs, rhs):
    return lax.dot_general(lhs, rhs, (((0,), (0,)), ((), ())), preferred_element_type=F32)


def cols_dot(lhs, rhs):
    return lax.dot_general(lhs, rhs, (((1,), (1,)), ((), ())), preferred_element_type=F32)


def gelu(h):
    return h * (0.5 * (1.0 + jnp.tanh(ROOT * (h + CUBE * (h * h * h)))))


def gelu_slope(h):
    sq = h * h
    t = jnp.tanh(ROOT * (h + CUBE * (sq * h)))
    return 0.5 * (1.0 + t) + (0.5 * h) * (1.0 - t * t) * (ROOT * (1.0 + (3.0 * CUBE) * sq))


def remote(src, dst, send, recv, where):
    return pltpu.make_async_remote_copy(src_ref=src, dst_ref=dst, send_sem=send, recv_sem=recv, device_id=where, device_id_type=MESH)


def signal(peer):
    pl.semaphore_signal(pltpu.get_barrier_semaphore(), inc=1, device_id=peer, device_id_type=MESH)


class Plane:
    def __init__(self):
        self.tp = lax.axis_index('tp')
        self.y = lax.rem(self.tp, SIDE)
        self.z = self.tp // SIDE

    def at(self, dy, dz):
        return lax.rem(self.z + dz + SIDE, SIDE) * SIDE + lax.rem(self.y + dy + SIDE, SIDE)

    def blk(self, half, df, ds):
        return self.at(df, ds) if half == 0 else self.at(ds, df)

    def near(self):
        return [{'tp': self.at(1, 0)}, {'tp': self.at(-1, 0)}, {'tp': self.at(0, 1)}, {'tp': self.at(0, -1)}]

    def rings(self):
        return [{'tp': self.at(d, 0)} for d in (1, 2, 3)] + [{'tp': self.at(0, d)} for d in (1, 2, 3)]


HOPS = (0, -1, 1, 2)
WALK = ((0, -1, None, 1), (0, 1, None, -1), (-1, 2, 0, 1), (1, 2, 1, -1))
BOTH = (0, 1)
TILE = 256
SLOTS = 15


def plane_gather(plane, bufs, send_sem, recv_sem, on_block=lambda *_: None, base=0, begun=False):
    def msg(a, half, slot, block, part, to):
        buf, start, size = bufs[a]
        size = size // 2
        start = start + half * size
        if part is not None:
            size = size // 2
            start = start + part * size
        ref = buf.at[plane.blk(half, *block), pl.ds(start, size)]
        return remote(ref, ref, send_sem.at[base + a], recv_sem.at[((base + a) * 2 + half) * SLOTS + slot], {'tp': plane.blk(half, *to)})

    def f(a, half, k, end):
        step = WALK[k]
        return msg(a, half, min(k, 2), (step[end], 0), None if end and k > 1 else step[2], (step[3], 0))

    def s(a, half, j, k, end):
        step = WALK[k]
        return msg(a, half, 3 * (j + 1) + min(k, 2), (HOPS[j], step[end]), None if end and k > 1 else step[2], (0, step[3]))

    send, recv = BOTH
    pairs = [(a, half) for a in range(len(bufs)) for half in BOTH]

    def across(a, half, j):
        for k in BOTH:
            s(a, half, j, k, send).start()
        on_block(a, half, j, 0)

    def onward(a, half, j):
        for k in BOTH:
            s(a, half, j, k, recv).wait_recv()
            s(a, half, j, k + 2, send).start()
            on_block(a, half, j, k + 1)

    if not begun:
        for pair in pairs:
            for k in BOTH:
                f(*pair, k, send).start()
            across(*pair, 0)
        yield
    for pair in pairs:
        for k in BOTH:
            f(*pair, k, recv).wait_recv()
            f(*pair, k + 2, send).start()
            across(*pair, k + 1)
    yield
    for pair in pairs:
        onward(*pair, 0)
    yield
    for pair in pairs:
        f(*pair, 2, recv).wait_recv()
        across(*pair, SIDE - 1)
    yield
    for j in range(1, SIDE):
        for pair in pairs:
            onward(*pair, j)
        yield
    for j in range(SIDE):
        for pair in pairs:
            s(*pair, j, 2, recv).wait_recv()
            on_block(*pair, j, SIDE - 1)
        if j % 2:
            yield
    for a, (buf, start, size) in enumerate(bufs):
        sent = buf.at[pl.ds(0, SIDE * SIDE - 1), pl.ds(start, size)]
        remote(sent, sent, send_sem.at[base + a], recv_sem.at[0], {'tp': plane.at(1, 0)}).wait_send()


def tiles(width):
    return [slice(n, n + TILE) for n in range(0, width, TILE)]


def drain(steps):
    for _ in steps:
        pass


def local(src, dst, sem):
    return pltpu.make_async_copy(src, dst, sem)


class Reduce:
    def __init__(self, plane, parts, got_one, sum_one, got_two, one_send, one_recv, two_send, two_recv):
        self.plane, self.parts, self.got_one, self.sum_one, self.got_two = plane, parts, got_one, sum_one, got_two
        self.one_send, self.one_recv, self.two_send, self.two_recv = one_send, one_recv, two_send, two_recv

    def row(self, half, index):
        size = self.parts.shape[3] // 2
        cols = pl.ds(half * size, size)
        return self.parts.at[:, index, :, cols] if half == 0 else self.parts.at[index, :, :, cols]

    def here(self, half):
        return (self.plane.y, self.plane.z) if half == 0 else (self.plane.z, self.plane.y)

    def first(self, half, d):
        n = half * 3 + d - 1
        dest = lax.rem(self.here(half)[0] + d, SIDE)
        return remote(self.row(half, dest), self.got_one.at[n], self.one_send, self.one_recv.at[half], {'tp': self.plane.blk(half, d, 0)})

    def second(self, half, d):
        n = half * 3 + d - 1
        dest = lax.rem(self.here(half)[1] + d, SIDE)
        return remote(self.sum_one.at[half, dest], self.got_two.at[n], self.two_send, self.two_recv.at[half], {'tp': self.plane.blk(half, 0, d)})

    def whole(self, got, send, recv, half=None):
        ref = got if half is None else got.at[pl.ds(half * 3, 3)]
        return remote(ref, ref, send, recv.at[half or 0], {'tp': self.plane.at(1, 0)})

    def begin(self, half):
        for d in (2, 1, 3):
            self.first(half, d).start()

    def middle(self):
        for half in BOTH:
            total = self.row(half, self.here(half)[0])[:].astype(F32)
            self.whole(self.got_one, self.one_send, self.one_recv, half).wait_recv()
            for d in (1, 3, 2):
                total = total + self.got_one[half * 3 + d - 1].astype(F32)
            self.sum_one[half] = total.astype(self.sum_one.dtype)
            for d in (2, 1, 3):
                self.second(half, d).start()

    def end(self):
        sums = []
        for half in BOTH:
            total = self.sum_one[half, self.here(half)[1]].astype(F32)
            self.whole(self.got_two, self.two_send, self.two_recv, half).wait_recv()
            for d in (1, 3, 2):
                total = total + self.got_two[half * 3 + d - 1].astype(F32)
            sums.append(total)
        return sums

    def close(self):
        self.whole(self.got_one, self.one_send, self.one_recv).wait_send()
        self.whole(self.got_two, self.two_send, self.two_recv).wait_send()


def fold(op, value):
    rows, cols = value.shape
    return op(value.reshape(rows // 8, 8, cols), axis=0)


def flatten(ids, flat):
    size, cols = ids.shape[1], flat.shape[1]
    for r in range(ids.shape[0]):
        at = r * size
        flat[at // cols:at // cols + 1, at % cols:at % cols + size] = ids[r:r + 1, :]


def list_rows(tokens, base, rows, group, unit, flat, slot, out):
    lines, lanes = flat.shape
    count = lines * lanes
    flatten(tokens, flat)
    row = flat[:] - base
    mine = (row >= 0) & (row < rows)
    upper = lax.broadcasted_iota(jnp.int32, (lanes, lanes), 0) <= lax.broadcasted_iota(jnp.int32, (lanes, lanes), 1)
    ones = [jnp.where(mask, 1.0, 0.0).astype(BF16) for mask in (mine, upper)]
    seen = dot(*ones)
    total = jnp.zeros((1, 1), F32)
    for r in range(lines):
        line = slice(r, r + 1)
        here = slice(r * lanes, (r + 1) * lanes)
        slot[:1, here] = jnp.where(mine[line], seen[line] + (total - 1.0), -1.0).astype(jnp.int32)
        slot[1:, here] = row[line]
        total = total + seen[line, lanes - 1:]
    number = lax.broadcasted_iota(jnp.int32, (1, count), 1)
    inner = lax.rem(number, group)
    place = inner // unit * (count // group * unit) + number // group * unit + lax.rem(number, unit)
    digits = [part for value in (place, slot[1:, :]) for part in (value // 256, lax.rem(value, 256))]
    which = lax.broadcasted_iota(jnp.int32, (16, count), 0)
    values = sum(jnp.where(which == i, digit, 0) for i, digit in enumerate(digits)).astype(F32).astype(BF16)

    @pl.loop(0, count // group)
    def _(c):
        start = pl.multiple_of(c * group, group)
        pick = jnp.where(slot[:1, :] == start + lax.broadcasted_iota(jnp.int32, (group, count), 0), 1.0, 0.0).astype(BF16)
        found = cols_dot(values, pick)
        for i in BOTH:
            out[i:i + 1, pl.ds(start, group)] = (found[2 * i:2 * i + 1] * 256.0 + found[2 * i + 1:2 * i + 2]).astype(jnp.int32)

    out[2:, :] = jnp.broadcast_to(total, (1, count)).astype(jnp.int32)


def norm_of(x):
    wide = x.astype(F32)
    inv_rms = lax.rsqrt(jnp.mean(wide * wide, axis=-1, keepdims=True) + NORM_EPS)
    return inv_rms, wide * inv_rms


class Spread:
    def __init__(self, plane, source, stages, src, out, line_send, line_recv, die_send, die_recv):
        self.plane, self.source, self.stages, self.src, self.out = plane, source, stages, src, out
        self.line_send, self.line_recv, self.die_send, self.die_recv = line_send, line_recv, die_send, die_recv
        self.stage = lax.axis_index('pp')
        self.core = lax.rem(self.stage, 2)
        self.mate = {'pp': self.stage + 1 - 2 * self.core}
        self.rows = out.shape[1] // 2
        self.lo = pl.multiple_of(self.core * self.rows, self.rows)
        self.others = [p for p in range(stages) if p != source]

    def greet(self):
        source = self.stage == self.source
        twin = self.stage == self.source ^ 1
        pl.when(source)(functools.partial(signal, {'pp': self.source ^ 1}))
        pl.when(jnp.logical_not(source))(functools.partial(signal, {'pp': self.source}))
        pl.when(jnp.logical_not(source | twin))(functools.partial(signal, self.mate))
        return jnp.where(source, len(self.others), 1)

    def line(self, p):
        part = pl.ds((p % 2) * self.rows, self.rows)
        return remote(self.src.at[part], self.out.at[self.plane.tp, part], self.line_send, self.line_recv, {'pp': p})

    def send(self):
        for p in self.others:
            self.line(p).start()
        part = pl.ds(self.lo, self.rows)
        self.out[self.plane.tp, part] = self.src[part]

    def arrive(self):
        mine = self.out.at[self.plane.tp, pl.ds(self.lo, self.rows)]
        remote(mine, mine, self.line_recv, self.line_recv, self.mate).wait_recv()

    def on_block(self, a, half, j, k):
        if a == 0:
            size = self.rows // 2
            ref = self.out.at[self.plane.blk(half, HOPS[j], HOPS[k]), pl.ds(self.lo + half * size, size)]
            remote(ref, ref, self.die_send, self.die_recv, self.mate).start()

    def half(self, lo):
        ref = self.out.at[:, pl.ds(lo, self.rows)]
        return remote(ref, ref, self.die_send, self.die_recv, self.mate)

    def finish(self):
        self.half(pl.multiple_of((1 - self.core) * self.rows, self.rows)).wait_recv()

    def close(self):
        self.half(self.lo).wait_send()

        @pl.when(self.stage == self.source)
        def _():
            sent = self.out.at[pl.ds(0, len(self.others)), pl.ds(self.lo, self.rows)]
            remote(sent, sent, self.line_send, self.line_recv, self.mate).wait_send()


def forward_kernel(last, tokens, emb, w_one, w_two, top, own_x, table, order_out, hid_out, one_out, two_out, x_out, ones, twos, one_t, two_t, hot, parts,
                   got_one, sum_one, got_two, piece, x_buf, y_buf, n_src, a_buf, hid_ref, x_all, ids, flat, slot,
                   send_sem, recv_sem, one_send, one_recv, two_send, two_recv, line_send, line_recv, own_send, own_recv, spread_send, spread_recv, die_send, die_recv,
                   hop_send, hop_recv, lead_sem, loc_sem):
    plane = Plane()
    stage = lax.axis_index('pp')
    tp = plane.tp
    stages = last + 1
    core = lax.rem(stage, 2)
    moves = ((emb, table), (w_one, ones.at[tp]), (w_two, twos.at[tp]), (one_t, one_out), (two_t, two_out), (hid_ref, hid_out), (x_all, x_out))
    load, own_one, own_two, *saves = [local(src, dst, loc_sem.at[i]) for i, (src, dst) in enumerate(moves)]
    save_one, save_two, save_hid, save_x = saves
    load.start()
    own_one.start()
    own_two.start()
    for peer in plane.rings() + [{'pp': lax.rem(stage + d, stages)} for d in range(1, stages)]:
        signal(peer)

    own_one.wait()
    own_two.wait()
    pl.semaphore_wait(pltpu.get_barrier_semaphore(), 6 + last)
    def weight_steps(begun=False):
        return plane_gather(plane, [(ones, 0, ones.shape[1]), (twos, 0, twos.shape[1])], send_sem, recv_sem, begun=begun)

    @pl.when(core == 0)
    def _():
        next(weight_steps())

    rows, width = table.shape
    group = ids.shape[1]
    unit = piece.shape[0]
    count = group // tokens.shape[1]
    flatten(tokens.at[pl.ds(pl.multiple_of(stage * count, count), count)], ids)
    hot[:] = jnp.where(ids[:] - tp * rows == lax.broadcasted_iota(jnp.int32, hot.shape, 0), 1.0, 0.0).astype(BF16)
    load.wait()
    cut = rows // group * group
    for cols in tiles(width):
        picked = rows_dot(hot[:cut], table[:cut, cols]) + rows_dot(hot[cut:], table[cut:, cols])
        parts[:, :, :, cols] = picked.astype(BF16).reshape(*parts.shape[:-1], TILE)
    red = Reduce(plane, parts, got_one, sum_one, got_two, one_send, one_recv, two_send, two_recv)
    for half in BOTH:
        red.begin(half)

    @pl.when(core == 1)
    def _():
        pl.semaphore_wait(lead_sem, 1)
        next(weight_steps())

    gather = weight_steps(True)
    next(gather)

    @pl.when(core == 0)
    def _():
        pl.semaphore_signal(lead_sem, inc=1, device_id={'pp': stage + 1}, device_id_type=MESH)

    next(gather)
    red.middle()
    next(gather)
    next(gather)
    for half, total in enumerate(red.end()):
        piece[:, half * (width // 2):(half + 1) * (width // 2)] = total.astype(BF16)

    def line(p):
        return remote(piece, x_buf.at[pl.ds(pl.multiple_of(p * unit, unit), unit)], line_send, line_recv, {'pp': 0})

    @pl.when(stage != 0)
    def _():
        line(stage).start()

    @pl.when(stage == 0)
    def _():
        x_buf[:unit] = piece[:]

    drain(gather)

    @pl.when(stage == 1)
    def _():
        pl.semaphore_signal(lead_sem, inc=1, device_id={'pp': 0}, device_id_type=MESH)

    blocks, _, cols = ones.shape

    def spare_time():
        @pl.loop(0, blocks)
        def _(k):
            one_t[k] = ones[k].T
            two_t[k] = twos[k].T

        save_one.start()
        save_two.start()
        list_rows(tokens, tp * rows, rows, group, unit, flat, slot, order_out)

    pl.when(stage > 1)(spare_time)
    hop = remote(y_buf, x_buf, hop_send, hop_recv, {'pp': lax.rem(stage + 1, stages)})

    @pl.when(stage == 0)
    def _():
        got = x_buf.at[pl.ds(0, last * unit)]
        remote(got, got, line_send, line_recv, {'pp': last}).wait_recv()

    pl.when(stage > 0)(hop.wait_recv)
    x_act = x_buf[:]
    for k in range(blocks):
        hidden = dot(x_act, ones[k])
        hid_ref[k] = hidden
        a_buf[:, k * cols:(k + 1) * cols] = gelu(hidden).astype(BF16)
    save_hid.start()
    gate = a_buf[:]
    for tile in tiles(width):
        branch = dot(gate, twos[:, :, tile].reshape(blocks * cols, TILE))
        y_buf[:, tile] = (x_buf[:, tile].astype(F32) + branch).astype(BF16)

    pl.when(stage < last)(hop.start)
    x_all[tp] = x_buf[:]

    @pl.when(stage < SIDE)
    def _():
        pl.when(stage <= 1)(spare_time)

        @pl.when(stage == 0)
        def _():
            pl.semaphore_wait(lead_sem, 1)

        steps = plane_gather(plane, [(x_all, 0, x_all.shape[1])], send_sem, recv_sem, base=2)
        drain(steps)

    own_save = local(x_all.at[tp], x_out.at[tp], loc_sem.at[6])
    pl.when(stage < SIDE)(save_x.start)
    pl.when(stage >= SIDE)(own_save.start)

    spread = Spread(plane, last, stages, n_src, top, spread_send, spread_recv, die_send, die_recv)

    def own(p):
        return remote(y_buf.at[pl.ds(p * unit, unit)], own_x, own_send, own_recv, {'pp': p})

    @pl.when(stage == last)
    def _():
        n_src[:] = norm_of(y_buf[:])[1].astype(BF16)
        spread.send()
        for p in spread.others:
            own(p).start()
        own_x[:] = y_buf[last * unit:]

    pl.when(stage < last)(spread.arrive)
    drain(plane_gather(plane, [(top, spread.lo, spread.rows)], send_sem, recv_sem, spread.on_block, base=3))
    spread.finish()
    pl.when(stage < last)(own(last).wait_recv)
    spread.close()

    @pl.when(stage == last)
    def _():
        sent = y_buf.at[pl.ds(0, last * unit)]
        remote(sent, sent, own_send, own_recv, spread.mate).wait_send()

    red.close()

    @pl.when(stage != 0)
    def _():
        line(stage).wait_send()

    pl.when(stage < last)(hop.wait_send)
    for save in saves[:-1]:
        save.wait()
    pl.when(stage < SIDE)(save_x.wait)
    pl.when(stage >= SIDE)(own_save.wait)


def head_kernel(target, stages, chunk, table, top, own_x, labels, loss_out, g_top, g_out, n_out,
                n_buf, lab, g_buf, peak, stat, shared, scale_ref, parts, got_one, sum_one, got_two, piece,
                share_send, share_recv, one_send, one_recv, two_send, two_recv, line_send, line_recv, loc_sem, *e_bufs):
    plane = Plane()
    stage = lax.axis_index('pp')
    tp = plane.tp
    size = shared.shape[1]
    others = [p for p in range(stages) if p != target]
    each, group = peak.shape[1:]
    unit = group // size
    for d in range(1, size):
        signal({'tp': lax.rem(tp + d, size)})

    @pl.when(stage == target)
    def _():
        for p in others:
            signal({'pp': p})

    pl.when(stage != target)(functools.partial(signal, {'pp': target}))
    for p in range(stages):
        n_buf[p * group:(p + 1) * group] = top[:, p * unit:(p + 1) * unit, :].reshape(group, top.shape[2])
    save_n = local(n_buf, n_out, loc_sem.at[1])
    save_n.start()

    rows, width = table.shape
    flatten(labels, lab)
    lab[:] = lab[:] - tp * rows
    pieces = len(e_bufs)
    pair = each * group

    def group_at(b, i):
        return lax.rem(stage // each + b, pieces) * each + i

    def label_of(p):
        return lab[pl.ds(p, 1), :]

    def down(value, start):
        return start + lax.broadcasted_iota(jnp.int32, value.shape, 0)

    def logit_chunk(b, start):
        tokens = n_buf[pl.ds(pl.multiple_of(group_at(b, 0) * group, pair), pair), :]
        logits = cols_dot(table[pl.ds(start, chunk), :], tokens)
        e_bufs[b][pl.ds(start, chunk), :] = logits
        return fold(jnp.max, logits)

    def exp_chunk(b, start, label, top_b, total, hits):
        logits = e_bufs[b][pl.ds(start, chunk), :]
        e = jnp.exp(logits - top_b)
        e_bufs[b][pl.ds(start, chunk), :] = e
        return total + fold(jnp.sum, e), hits + fold(jnp.sum, jnp.where(label == down(logits, start), logits, 0.0))

    def chunks(body, carry):
        return lax.fori_loop(0, rows // chunk, lambda c, carry: body(pl.multiple_of(c * chunk, 8), carry), carry)

    def msg(d, k):
        some = pl.ds(k, 1 + k * (pieces - 2))
        return remote(stat.at[some], shared.at[some, tp], share_send.at[k], share_recv.at[k], {'tp': lax.rem(tp + d, size)})

    def shares(k):
        ref = shared.at[pl.ds(k, 1 + k * (pieces - 2)), pl.ds(0, size - 1)]
        return remote(ref, ref, share_send.at[k], share_recv.at[k], {'tp': plane.at(1, 0)})

    def share(k):
        for d in range(1, size):
            msg(d, k).start()

    losses = []

    def normalise(k):
        shares(k).wait_recv()
        for b in (range(1, pieces) if k else range(1)):
            every = shared[b, :, 0]
            most = jnp.max(every, axis=0)
            log_norm = most + jnp.log(jnp.sum(jnp.exp(every - most[None]), axis=0))
            losses.append(jnp.sum(log_norm - jnp.sum(shared[b, :, 1], axis=0), keepdims=True))
            scale_ref[b] = jnp.exp(peak[b] - log_norm)

    def grad_block(b, i, slot):
        cols = pl.ds(pl.multiple_of(i * group, group), group)
        label = label_of(group_at(b, i))
        factor = scale_ref[b, pl.ds(i, 1), :]

        def part(start, _):
            e = e_bufs[b][pl.ds(start, chunk), cols]
            hit = label == down(e, start)
            g_buf[slot, pl.ds(start, chunk), :] = (e * factor - jnp.where(hit, 1.0, 0.0)).astype(BF16)

        chunks(part, None)

    def save(k):
        slot = 1 + k % 2
        at = pl.multiple_of(group_at(k // each, k % each) * group, group)
        return local(g_buf.at[slot], g_out.at[:, pl.ds(at, group)], loc_sem.at[2 + slot])

    def gradient(k):
        if k >= 2:
            save(k - 2).wait()
        grad_block(k // each, k % each, 1 + k % 2)
        save(k).start()

    cut = rows // group * group
    half = width // 2
    red = Reduce(plane, parts, got_one, sum_one, got_two, one_send, one_recv, two_send, two_recv)

    def own_gradient():
        grad_block(0, lax.rem(stage, each), 0)
        mine_g = g_buf.at[0]
        for cols in tiles(width):
            back = rows_dot(mine_g[:cut, :], table[:cut, cols]) + rows_dot(mine_g[cut:, :], table[cut:, cols])
            parts[:, :, :, cols] = back.reshape(*parts.shape[:-1], TILE)
            if cols.stop % half == 0:
                red.begin(cols.start // half)

    tops = []
    zero = jnp.zeros((8, pair), F32)
    for now, done in ((0, None), (None, 0), (1, None), *((b, b - 1) for b in range(2, pieces)), (None, pieces - 1)):
        label = None if done is None else jnp.concatenate([label_of(group_at(done, i)) for i in range(each)], axis=1)
        top_b = None if done is None else tops[done]

        def both(start, carry, now=now, done=done, top_b=top_b, label=label):
            best, total, hits = carry
            if now is not None:
                best = jnp.maximum(best, logit_chunk(now, start))
            if done is not None:
                total, hits = exp_chunk(done, start, label, top_b, total, hits)
            return best, total, hits

        best, total, hits = chunks(both, (jnp.full((8, pair), -jnp.inf, F32), zero, zero))
        if done is not None:
            found = (top_b + jnp.log(jnp.sum(total, axis=0, keepdims=True)), jnp.sum(hits, axis=0, keepdims=True), top_b)
            for i in range(each):
                cols = slice(i * group, (i + 1) * group)
                for kind in BOTH:
                    stat[done, kind, i:i + 1, :] = found[kind][:, cols]
                peak[done, i:i + 1, :] = found[2][:, cols]
            shared[done, tp] = stat[done]
        if done == 0:
            pl.semaphore_wait(pltpu.get_barrier_semaphore(), size - 1 + jnp.where(stage == target, len(others), 1))
        if now is None:
            share(1 if done else 0)
        else:
            tops.append(jnp.max(best, axis=0, keepdims=True))
        if now == 1:
            normalise(0)
            own_gradient()
        if now == pieces - 1:
            red.middle()

    gradient(0)
    gradient(1)
    sums = red.end()

    inv_rms, normed = norm_of(own_x[:])
    mean = (jnp.sum(normed[:, :half] * sums[0], axis=-1, keepdims=True) + jnp.sum(normed[:, half:] * sums[1], axis=-1, keepdims=True)) / width
    for h in BOTH:
        cols = slice(h * half, (h + 1) * half)
        piece[:, cols] = (inv_rms * (sums[h] - normed[:, cols] * mean)).astype(BF16)

    def line(p):
        return remote(piece, g_top.at[p], line_send, line_recv, {'pp': target})

    @pl.when(stage != target)
    def _():
        line(stage).start()

    normalise(1)
    for k in range(2, stages):
        gradient(k)
    loss_out[:] = sum(losses) / (stages * group)
    @pl.when(stage == target)
    def _():
        g_top[target] = piece[:]
        got = g_top.at[pl.ds(0, len(others))]
        remote(got, got, line_send, line_recv, {'pp': 0}).wait_recv()

    red.close()
    for k in BOTH:
        shares(k).wait_send()
    save_n.wait()
    save(stages - 2).wait()
    save(stages - 1).wait()
    @pl.when(stage != target)
    def _():
        line(stage).wait_send()


def backward_kernel(last, chunk, g_top, hid_in, two_all, one_all, g_all, n_all, x_in, w_one, w_two, de_buf, dx_all, grad_one, grad_two,
                    ones, twos, slope_ref, g_buf, n_buf, x_all, w_one_buf, w_two_buf, dy_all, dy_buf, dx_buf, d_buf,
                    send_sem, recv_sem, spread_send, spread_recv, die_send, die_recv, hop_send, hop_recv, go_sem, ready_sem, g_sem, loc_sem):
    plane = Plane()
    stage = lax.axis_index('pp')
    stages = last + 1
    blocks, cols, width = one_all.shape
    pairs = ((hid_in, slope_ref), (two_all, twos), (one_all, ones), (n_all, n_buf), (w_one, w_one_buf), (w_two, w_two_buf))
    loads = [local(src, dst, loc_sem.at[i]) for i, (src, dst) in enumerate(pairs)]
    lower = stage < SIDE
    upper = stage >= SIDE
    own = plane.tp
    load_x = [local(*pair, loc_sem.at[6]) for pair in ((x_in, x_all), (x_in.at[own], x_all.at[own]))]

    mid = upper & (stage < last - 1)

    def start(some):
        for load in some:
            load.start()

    pl.when(upper)(functools.partial(start, loads[:3]))
    pl.when(lower)(functools.partial(start, loads[3:4]))
    own_load = load_x[1]
    pl.when(mid)(own_load.start)
    spread = Spread(plane, 0, stages, dx_buf, dx_all, spread_send, spread_recv, die_send, die_recv)
    near = plane.near()
    for peer in near:
        signal(peer)
    extra = spread.greet()
    before = {'pp': lax.rem(stage + last, stages)}
    pl.when(stage > 0)(functools.partial(signal, before))
    hop = remote(dx_buf, dy_buf, hop_send, hop_recv, before)
    rows = de_buf.shape[0]
    pieces = -(-rows // chunk)

    def piece_at(c):
        return pl.ds(pl.multiple_of(jnp.minimum(c * chunk, rows - chunk), 8), chunk)

    def fetch(c):
        slot = lax.rem(c, 2)
        return local(g_all.at[piece_at(c)], g_buf.at[slot], g_sem.at[slot])

    def table(lo, hi):
        if lo == 0:
            fetch(0).start()
            loads[3].wait()

        @pl.loop(lo, hi)
        def _(c):
            @pl.when(c < pieces - 1)
            def _():
                fetch(c + 1).start()

            for i, some in enumerate((loads[:2], loads[2:3], loads[4:] + load_x[:1])):
                pl.when(lower & (c == i + 1))(functools.partial(start, some))

            fetch(c).wait()
            de_buf[piece_at(c), :] = dot(g_buf[lax.rem(c, 2)], n_buf[:])

    pl.semaphore_wait(pltpu.get_barrier_semaphore(), len(near) + extra + jnp.where(stage < last, 1, 0))

    @pl.when(stage < last)
    def _():
        pl.semaphore_signal(ready_sem, inc=1, device_id={'pp': lax.rem(stage + 1, stages)}, device_id_type=MESH)

    pl.when(lower)(functools.partial(table, 0, pieces))
    loads[0].wait()
    for k in range(blocks):
        slope_ref[k] = gelu_slope(slope_ref[k])
    loads[1].wait()

    def a_steps(begun=False):
        return plane_gather(plane, [(x_all, 0, x_all.shape[1])], send_sem, recv_sem, base=2, begun=begun)

    mid_steps = a_steps()

    @pl.when(mid)
    def _():
        own_load.wait()
        for _ in range(3):
            next(mid_steps)

    @pl.when(stage == last)
    def _():
        dy_buf[:] = g_top[:]

    pl.when(stage < last)(hop.wait_recv)
    dy_all[plane.tp] = dy_buf[:]
    whole = (dy_all, 0, dy_all.shape[1])
    part = (dx_all, spread.lo, spread.rows)

    def dy_steps(begun):
        return plane_gather(plane, [whole], send_sem, recv_sem, base=1, begun=begun)

    @pl.when(stage <= 1)
    def _():
        next(dy_steps(False))

    grad_y = dy_buf[:]
    for k in range(blocks):
        grad_gate = dot(grad_y, twos[k])
        d_buf[:, k * cols:(k + 1) * cols] = (slope_ref[k] * grad_gate).astype(BF16)
    loads[2].wait()
    grad_hidden = d_buf[:]
    for tile in tiles(width):
        back = dot(grad_hidden, ones[:, :, tile].reshape(blocks * cols, TILE))
        dx_buf[:, tile] = (dy_buf[:, tile].astype(F32) + back).astype(BF16)

    @pl.when(stage > 0)
    def _():
        pl.semaphore_wait(ready_sem, 1)
        hop.start()

    pl.when(stage == 0)(spread.send)
    pl.when(upper)(functools.partial(start, loads[3:]))
    pl.when(upper & jnp.logical_not(mid))(own_load.start)
    for load in loads[4:]:
        load.wait()
    pl.when(lower)(load_x[0].wait)
    pl.when(upper & jnp.logical_not(mid))(own_load.wait)

    grad_one[:] = jnp.zeros_like(grad_one)
    grad_two[:] = jnp.zeros_like(grad_two)

    def weights(ahead):
        step = SIDE

        @pl.loop(0, 2)
        def _(i):
            row = lax.rem(plane.z + (1 + i if ahead else SIDE - i), SIDE)
            part = pl.ds(row * step, step)
            x_act = x_all[part].reshape(step * x_all.shape[1], width)
            grad_y = dy_all[part].reshape(step * x_all.shape[1], width)
            hidden = dot(x_act, w_one_buf[:])
            grad_gate = cols_dot(grad_y, w_two_buf[:])
            grad_hidden = (gelu_slope(hidden) * grad_gate).astype(BF16)
            grad_one[:] += rows_dot(x_act, grad_hidden)
            grad_two[:] += rows_dot(gelu(hidden).astype(BF16), grad_y)

    def dx_steps():
        return plane_gather(plane, [part], send_sem, recv_sem, spread.on_block)

    @pl.when(stage > 1)
    def _():
        hop.wait_send()

        @pl.when(spread.core == 0)
        def _():
            pl.semaphore_signal(go_sem, inc=1, device_id=spread.mate, device_id_type=MESH)

        @pl.when(spread.core == 1)
        def _():
            pl.semaphore_wait(go_sem, 1)

    @pl.when(stage > 1)
    def _():
        next(dy_steps(False))

    @pl.when(upper & jnp.logical_not(mid))
    def _():
        next(a_steps())

    planes = [(stage <= 1, None, 'xddxdxdxdxdx', 'x'), ((stage > 1) & lower, None, 'dddxdxdxdx', 'xxx'),
              (mid, mid_steps, 'dtdadatdaxdaxdx', 'xxx'), (upper & jnp.logical_not(mid), a_steps(True), 'datdadatdaxdaxdax', 'xxx')]
    runs = []
    for here, more, order, rest in planes:
        steps = {'d': dy_steps(True), 'x': dx_steps(), 'a': more}

        def arrived(order=order, steps=steps):
            part = -(-pieces // 2)
            for i, kind in enumerate(order):
                if kind == 't':
                    lo = order[:i].count('t') * part
                    table(lo, min(lo + part, pieces))
                    continue
                if kind == 'x' and 'x' not in order[:i]:
                    pl.when(stage > 0)(spread.arrive)
                next(steps[kind])
            next(steps['d'])
            drain(steps['a'] or ())

        def onward(rest=rest, steps=steps):
            for kind in rest:
                next(steps[kind])
            drain(steps['d'])

        pl.when(here)(arrived)
        runs.append((here, onward, functools.partial(drain, steps['x'])))

    weights(False)
    for here, onward, _ in runs:
        pl.when(here)(onward)
    weights(True)
    for here, _, finish in runs:
        pl.when(here)(finish)

    spread.finish()
    spread.close()

    pl.when(stage == 1)(hop.wait_send)


def add_kernel(pieces, order, dx_ref, de_ref, loss_ref, one_ref, two_ref, de_out, loss_out, table_out, one_out, two_out, wide, sem):
    small = ((one_ref, one_out), (two_ref, two_out), (loss_ref, loss_out))
    saves = [local(*pair, sem.at[i]) for i, pair in enumerate(small)]
    for save in saves:
        save.start()
    wide[:] = dx_ref[:].astype(F32)

    @pl.loop(0, order[2, 0])
    def _(j):
        row = pl.ds(order[1, j], 1)
        de_out[row, :] = de_out[row, :] + wide[pl.ds(order[0, j], 1), :]

    rows = de_ref.shape[0]
    size = -(-rows // (8 * pieces)) * 8
    for c in range(pieces):
        part = pl.ds(c * size, min(size, rows - c * size))
        saves.append(local(de_out.at[part], table_out.at[part], sem.at[len(small) + c]))
        saves[-1].start()
    for save in saves:
        save.wait()


def vmem():
    return pl.BlockSpec(memory_space=pltpu.VMEM)


def anywhere():
    return pl.BlockSpec(memory_space=pl.ANY)


def params(cid, mib):
    return pltpu.CompilerParams(collective_id=cid, has_side_effects=True, vmem_limit_bytes=mib << 20)


DMA = pltpu.SemaphoreType.DMA


def solution(mesh):
    pp_size = mesh.shape['pp']
    tp_size = mesh.shape['tp']
    last = pp_size - 1

    def device_fn(tokens, labels, emb_table, w_in, w_out):
        num_tokens = tokens.shape[0] * tokens.shape[1]
        vocab_rows, width = emb_table.shape
        w_one, w_two = w_in[0], w_out[0]
        cols = w_one.shape[1]
        unit = num_tokens // (pp_size * tp_size)
        block = pp_size * unit
        group = tp_size * unit
        half = width // 2
        chunk = vocab_rows // 3
        step = 512
        pair = 2 * group
        shape = jax.ShapeDtypeStruct
        VM = pltpu.VMEM

        def reduce_scratch(dtype):
            return [VM((SIDE, SIDE, unit, width), dtype), VM((6, SIDE, unit, half), dtype), VM((2, SIDE, unit, half), dtype), VM((6, unit, half), dtype), VM((unit, width), BF16)]

        duo = DMA((2,))
        reduce_sems = [DMA, duo, DMA, duo, DMA, DMA]
        many = shape((tp_size, block, width), BF16)
        many_buf = VM((tp_size, block, width), BF16)
        two_sums = 2 * SLOTS
        gather_sems = [DMA((4,)), DMA((4 * two_sums,))]
        spread_sems = [DMA, DMA, DMA, DMA]

        top, own_x, table, order, hidden, one_t, two_t, x_all = pl.pallas_call(
            functools.partial(forward_kernel, last),
            out_shape=(many_buf, VM((unit, width), BF16), VM((vocab_rows, width), BF16), shape((3, num_tokens), jnp.int32), shape((tp_size, block, cols), F32), shape((tp_size, cols, width), BF16), shape((tp_size, width, cols), BF16), many),
            in_specs=[vmem()] + [anywhere()] * 3,
            out_specs=[vmem()] * 4 + [anywhere()] * 4,
            scratch_shapes=[VM((tp_size, width, cols), BF16), VM((tp_size, cols, width), BF16), VM((tp_size, cols, width), BF16), VM((tp_size, width, cols), BF16),
                            VM((vocab_rows, group), BF16), *reduce_scratch(BF16),
                            VM((block, width), BF16), VM((block, width), BF16), VM((block, width), BF16), VM((block, tp_size * cols), BF16), VM((tp_size, block, cols), F32), many_buf, VM((1, group), jnp.int32),
                            VM((num_tokens // 128, 128), jnp.int32), VM((2, num_tokens), jnp.int32),
                            *gather_sems, *reduce_sems, DMA, DMA, *spread_sems, DMA, DMA, pltpu.SemaphoreType.REGULAR, DMA((7,))],
            compiler_params=params(1, 49), name='forward_chain',
        )(tokens, emb_table, w_one, w_two)

        by_pair = (num_tokens // pair, pair // group, group)
        loss, g_top, g_all, n_all = pl.pallas_call(
            functools.partial(head_kernel, last, pp_size, chunk),
            out_shape=(VM((1, 1), F32), pltpu.HBM((pp_size, unit, width), BF16), shape((vocab_rows, num_tokens), BF16), shape((num_tokens, width), BF16)),
            in_specs=[vmem()] * 4,
            out_specs=[vmem()] * 2 + [anywhere()] * 2,
            scratch_shapes=[VM((num_tokens, width), BF16), VM((pp_size, group), jnp.int32), VM((3, vocab_rows, group), BF16),
                            VM(by_pair, F32), VM((by_pair[0], 2, *by_pair[1:]), F32), VM((by_pair[0], tp_size, 2, *by_pair[1:]), F32), VM(by_pair, F32), *reduce_scratch(F32),
                            duo, duo, *reduce_sems, DMA((5,)),
                            *[VM((vocab_rows, pair), F32) for _ in range(num_tokens // pair)]],
            compiler_params=params(2, 49), name='head',
        )(*[pltpu.with_memory_space_constraint(array, pltpu.VMEM) for array in (table, top, own_x)], labels)

        de_head, dx_first, grad_one, grad_two = pl.pallas_call(
            functools.partial(backward_kernel, last, step),
            out_shape=(VM((vocab_rows, width), F32), many_buf, VM((width, cols), F32), VM((cols, width), F32)),
            in_specs=[vmem()] + [anywhere()] * 8, out_specs=[vmem()] * 4,
            scratch_shapes=[VM((tp_size, cols, width), BF16), VM((tp_size, width, cols), BF16), VM((tp_size, block, cols), F32), VM((2, step, num_tokens), BF16), VM((num_tokens, width), BF16),
                            many_buf, VM((width, cols), BF16), VM((cols, width), BF16), many_buf,
                            VM((block, width), BF16), VM((block, width), BF16), VM((block, tp_size * cols), BF16),
                            *gather_sems, *spread_sems, DMA, DMA, pltpu.SemaphoreType.REGULAR, pltpu.SemaphoreType.REGULAR, duo, DMA((7,))],
            compiler_params=params(3, 45), name='backward_chain',
        )(g_top.reshape(block, width), hidden, two_t, one_t, g_all, n_all, x_all, w_one, w_two)

        smem = pl.BlockSpec(memory_space=pltpu.SMEM)
        _, loss, grad_table, grad_one, grad_two = pl.pallas_call(
            functools.partial(add_kernel, 12),
            out_shape=(VM((vocab_rows, width), F32), shape((1, 1), F32), shape((vocab_rows, width), F32), shape((width, cols), F32), shape((cols, width), F32)),
            in_specs=[smem] + [vmem()] * 5, out_specs=[vmem()] + [anywhere()] * 4,
            scratch_shapes=[VM((num_tokens, width), F32), DMA((15,))], input_output_aliases={2: 0},
            compiler_params=pltpu.CompilerParams(vmem_limit_bytes=24 << 20), name='add_rows',
        )(order, dx_first.reshape(num_tokens, width), de_head, loss, grad_one, grad_two)
        return loss.reshape(1), grad_one[None], grad_two[None], grad_table

    return jax.shard_map(device_fn, mesh=mesh, in_specs=(P('dp', None), P('dp', None), P('tp', None), P('pp', None, 'tp'), P('pp', 'tp', None)), out_specs=(P('dp'), P(('dp', 'pp'), None, 'tp'), P(('dp', 'pp'), 'tp', None), P(('dp', 'tp'), None)), check_vma=False)
```

```python
import functools

import jax
import jax.numpy as jnp
from jax import lax
from jax.experimental import pallas as pl
from jax.experimental.pallas import tpu as pltpu
from jax.sharding import PartitionSpec as P

NORM_EPS = 1e-6
SIDE = 4
MESH = pl.DeviceIdType.MESH
F32 = jnp.float32
BF16 = jnp.bfloat16
CUBE = 0.044715
ROOT = 0.7978845608028654


def dot(lhs, rhs):
    return jnp.dot(lhs, rhs, preferred_element_type=F32)


def rows_dot(lhs, rhs):
    return lax.dot_general(lhs, rhs, (((0,), (0,)), ((), ())), preferred_element_type=F32)


def cols_dot(lhs, rhs):
    return lax.dot_general(lhs, rhs, (((1,), (1,)), ((), ())), preferred_element_type=F32)


def gelu(h):
    return h * (0.5 * (1.0 + jnp.tanh(ROOT * (h + CUBE * (h * h * h)))))


def gelu_slope(h):
    sq = h * h
    t = jnp.tanh(ROOT * (h + CUBE * (sq * h)))
    return 0.5 * (1.0 + t) + (0.5 * h) * (1.0 - t * t) * (ROOT * (1.0 + (3.0 * CUBE) * sq))


def remote(src, dst, send, recv, where):
    return pltpu.make_async_remote_copy(src_ref=src, dst_ref=dst, send_sem=send, recv_sem=recv, device_id=where, device_id_type=MESH)


def signal(peer):
    pl.semaphore_signal(pltpu.get_barrier_semaphore(), inc=1, device_id=peer, device_id_type=MESH)


class Plane:
    def __init__(self):
        self.tp = lax.axis_index('tp')
        self.y = lax.rem(self.tp, SIDE)
        self.z = self.tp // SIDE

    def at(self, dy, dz):
        return lax.rem(self.z + dz + SIDE, SIDE) * SIDE + lax.rem(self.y + dy + SIDE, SIDE)

    def blk(self, half, df, ds):
        return self.at(df, ds) if half == 0 else self.at(ds, df)

    def near(self):
        return [{'tp': self.at(1, 0)}, {'tp': self.at(-1, 0)}, {'tp': self.at(0, 1)}, {'tp': self.at(0, -1)}]

    def rings(self):
        return [{'tp': self.at(d, 0)} for d in (1, 2, 3)] + [{'tp': self.at(0, d)} for d in (1, 2, 3)]


HOPS = (0, -1, 1, 2)
WALK = ((0, -1, None, 1), (0, 1, None, -1), (-1, 2, 0, 1), (1, 2, 1, -1))
BOTH = (0, 1)
TILE = 256
SLOTS = 15


def plane_gather(plane, bufs, send_sem, recv_sem, on_block=lambda *_: None, base=0, begun=False):
    def msg(a, half, slot, block, part, to):
        buf, start, size = bufs[a]
        size = size // 2
        start = start + half * size
        if part is not None:
            size = size // 2
            start = start + part * size
        ref = buf.at[plane.blk(half, *block), pl.ds(start, size)]
        return remote(ref, ref, send_sem.at[base + a], recv_sem.at[((base + a) * 2 + half) * SLOTS + slot], {'tp': plane.blk(half, *to)})

    def f(a, half, k, end):
        step = WALK[k]
        return msg(a, half, min(k, 2), (step[end], 0), None if end and k > 1 else step[2], (step[3], 0))

    def s(a, half, j, k, end):
        step = WALK[k]
        return msg(a, half, 3 * (j + 1) + min(k, 2), (HOPS[j], step[end]), None if end and k > 1 else step[2], (0, step[3]))

    send, recv = BOTH
    pairs = [(a, half) for a in range(len(bufs)) for half in BOTH]

    def across(a, half, j):
        for k in BOTH:
            s(a, half, j, k, send).start()
        on_block(a, half, j, 0)

    def onward(a, half, j):
        for k in BOTH:
            s(a, half, j, k, recv).wait_recv()
            s(a, half, j, k + 2, send).start()
            on_block(a, half, j, k + 1)

    if not begun:
        for pair in pairs:
            for k in BOTH:
                f(*pair, k, send).start()
            across(*pair, 0)
        yield
    for pair in pairs:
        for k in BOTH:
            f(*pair, k, recv).wait_recv()
            f(*pair, k + 2, send).start()
            across(*pair, k + 1)
    yield
    for pair in pairs:
        onward(*pair, 0)
    yield
    for pair in pairs:
        f(*pair, 2, recv).wait_recv()
        across(*pair, SIDE - 1)
    yield
    for j in range(1, SIDE):
        for pair in pairs:
            onward(*pair, j)
        yield
    for j in range(SIDE):
        for pair in pairs:
            s(*pair, j, 2, recv).wait_recv()
            on_block(*pair, j, SIDE - 1)
        if j % 2:
            yield
    for a, (buf, start, size) in enumerate(bufs):
        sent = buf.at[pl.ds(0, SIDE * SIDE - 1), pl.ds(start, size)]
        remote(sent, sent, send_sem.at[base + a], recv_sem.at[0], {'tp': plane.at(1, 0)}).wait_send()


def tiles(width):
    return [slice(n, n + TILE) for n in range(0, width, TILE)]


def drain(steps):
    for _ in steps:
        pass


def local(src, dst, sem):
    return pltpu.make_async_copy(src, dst, sem)


class Reduce:
    def __init__(self, plane, parts, got_one, sum_one, got_two, one_send, one_recv, two_send, two_recv):
        self.plane, self.parts, self.got_one, self.sum_one, self.got_two = plane, parts, got_one, sum_one, got_two
        self.one_send, self.one_recv, self.two_send, self.two_recv = one_send, one_recv, two_send, two_recv

    def row(self, half, index):
        size = self.parts.shape[3] // 2
        cols = pl.ds(half * size, size)
        return self.parts.at[:, index, :, cols] if half == 0 else self.parts.at[index, :, :, cols]

    def here(self, half):
        return (self.plane.y, self.plane.z) if half == 0 else (self.plane.z, self.plane.y)

    def first(self, half, d):
        n = half * 3 + d - 1
        dest = lax.rem(self.here(half)[0] + d, SIDE)
        return remote(self.row(half, dest), self.got_one.at[n], self.one_send, self.one_recv.at[half], {'tp': self.plane.blk(half, d, 0)})

    def second(self, half, d):
        n = half * 3 + d - 1
        dest = lax.rem(self.here(half)[1] + d, SIDE)
        return remote(self.sum_one.at[half, dest], self.got_two.at[n], self.two_send, self.two_recv.at[half], {'tp': self.plane.blk(half, 0, d)})

    def whole(self, got, send, recv, half=None):
        ref = got if half is None else got.at[pl.ds(half * 3, 3)]
        return remote(ref, ref, send, recv.at[half or 0], {'tp': self.plane.at(1, 0)})

    def begin(self, half):
        for d in (2, 1, 3):
            self.first(half, d).start()

    def middle(self):
        for half in BOTH:
            total = self.row(half, self.here(half)[0])[:].astype(F32)
            self.whole(self.got_one, self.one_send, self.one_recv, half).wait_recv()
            for d in (1, 3, 2):
                total = total + self.got_one[half * 3 + d - 1].astype(F32)
            self.sum_one[half] = total.astype(self.sum_one.dtype)
            for d in (2, 1, 3):
                self.second(half, d).start()

    def end(self):
        sums = []
        for half in BOTH:
            total = self.sum_one[half, self.here(half)[1]].astype(F32)
            self.whole(self.got_two, self.two_send, self.two_recv, half).wait_recv()
            for d in (1, 3, 2):
                total = total + self.got_two[half * 3 + d - 1].astype(F32)
            sums.append(total)
        return sums

    def close(self):
        self.whole(self.got_one, self.one_send, self.one_recv).wait_send()
        self.whole(self.got_two, self.two_send, self.two_recv).wait_send()


def fold(op, value):
    rows, cols = value.shape
    return op(value.reshape(rows // 8, 8, cols), axis=0)


def flatten(ids, flat):
    size, cols = ids.shape[1], flat.shape[1]
    for r in range(ids.shape[0]):
        at = r * size
        flat[at // cols:at // cols + 1, at % cols:at % cols + size] = ids[r:r + 1, :]


def list_rows(tokens, base, rows, group, unit, flat, slot, out):
    lines, lanes = flat.shape
    count = lines * lanes
    flatten(tokens, flat)
    row = flat[:] - base
    mine = (row >= 0) & (row < rows)
    upper = lax.broadcasted_iota(jnp.int32, (lanes, lanes), 0) <= lax.broadcasted_iota(jnp.int32, (lanes, lanes), 1)
    ones = [jnp.where(mask, 1.0, 0.0).astype(BF16) for mask in (mine, upper)]
    seen = dot(*ones)
    total = jnp.zeros((1, 1), F32)
    for r in range(lines):
        line = slice(r, r + 1)
        here = slice(r * lanes, (r + 1) * lanes)
        slot[:1, here] = jnp.where(mine[line], seen[line] + (total - 1.0), -1.0).astype(jnp.int32)
        slot[1:, here] = row[line]
        total = total + seen[line, lanes - 1:]
    number = lax.broadcasted_iota(jnp.int32, (1, count), 1)
    inner = lax.rem(number, group)
    place = inner // unit * (count // group * unit) + number // group * unit + lax.rem(number, unit)
    digits = [part for value in (place, slot[1:, :]) for part in (value // 256, lax.rem(value, 256))]
    which = lax.broadcasted_iota(jnp.int32, (16, count), 0)
    values = sum(jnp.where(which == i, digit, 0) for i, digit in enumerate(digits)).astype(F32).astype(BF16)

    @pl.loop(0, count // group)
    def _(c):
        start = pl.multiple_of(c * group, group)
        pick = jnp.where(slot[:1, :] == start + lax.broadcasted_iota(jnp.int32, (group, count), 0), 1.0, 0.0).astype(BF16)
        found = cols_dot(values, pick)
        for i in BOTH:
            out[i:i + 1, pl.ds(start, group)] = (found[2 * i:2 * i + 1] * 256.0 + found[2 * i + 1:2 * i + 2]).astype(jnp.int32)

    out[2:, :] = jnp.broadcast_to(total, (1, count)).astype(jnp.int32)


def norm_of(x):
    wide = x.astype(F32)
    inv_rms = lax.rsqrt(jnp.mean(wide * wide, axis=-1, keepdims=True) + NORM_EPS)
    return inv_rms, wide * inv_rms


class Spread:
    def __init__(self, plane, source, stages, src, out, line_send, line_recv, die_send, die_recv):
        self.plane, self.source, self.stages, self.src, self.out = plane, source, stages, src, out
        self.line_send, self.line_recv, self.die_send, self.die_recv = line_send, line_recv, die_send, die_recv
        self.stage = lax.axis_index('pp')
        self.core = lax.rem(self.stage, 2)
        self.mate = {'pp': self.stage + 1 - 2 * self.core}
        self.rows = out.shape[1] // 2
        self.lo = pl.multiple_of(self.core * self.rows, self.rows)
        self.others = [p for p in range(stages) if p != source]

    def greet(self):
        source = self.stage == self.source
        twin = self.stage == self.source ^ 1
        pl.when(source)(functools.partial(signal, {'pp': self.source ^ 1}))
        pl.when(jnp.logical_not(source))(functools.partial(signal, {'pp': self.source}))
        pl.when(jnp.logical_not(source | twin))(functools.partial(signal, self.mate))
        return jnp.where(source, len(self.others), 1)

    def line(self, p):
        part = pl.ds((p % 2) * self.rows, self.rows)
        return remote(self.src.at[part], self.out.at[self.plane.tp, part], self.line_send, self.line_recv, {'pp': p})

    def send(self):
        for p in self.others:
            self.line(p).start()
        part = pl.ds(self.lo, self.rows)
        self.out[self.plane.tp, part] = self.src[part]

    def arrive(self):
        mine = self.out.at[self.plane.tp, pl.ds(self.lo, self.rows)]
        remote(mine, mine, self.line_recv, self.line_recv, self.mate).wait_recv()

    def on_block(self, a, half, j, k):
        if a == 0:
            size = self.rows // 2
            ref = self.out.at[self.plane.blk(half, HOPS[j], HOPS[k]), pl.ds(self.lo + half * size, size)]
            remote(ref, ref, self.die_send, self.die_recv, self.mate).start()

    def half(self, lo):
        ref = self.out.at[:, pl.ds(lo, self.rows)]
        return remote(ref, ref, self.die_send, self.die_recv, self.mate)

    def finish(self):
        self.half(pl.multiple_of((1 - self.core) * self.rows, self.rows)).wait_recv()

    def close(self):
        self.half(self.lo).wait_send()

        @pl.when(self.stage == self.source)
        def _():
            sent = self.out.at[pl.ds(0, len(self.others)), pl.ds(self.lo, self.rows)]
            remote(sent, sent, self.line_send, self.line_recv, self.mate).wait_send()


def forward_kernel(last, tokens, emb, w_one, w_two, top, own_x, table, order_out, hid_out, one_out, two_out, x_out, ones, twos, one_t, two_t, hot, parts,
                   got_one, sum_one, got_two, piece, x_buf, y_buf, n_src, a_buf, hid_ref, x_all, ids, flat, slot,
                   send_sem, recv_sem, one_send, one_recv, two_send, two_recv, line_send, line_recv, own_send, own_recv, spread_send, spread_recv, die_send, die_recv,
                   hop_send, hop_recv, lead_sem, loc_sem):
    plane = Plane()
    stage = lax.axis_index('pp')
    tp = plane.tp
    stages = last + 1
    core = lax.rem(stage, 2)
    moves = ((emb, table), (w_one, ones.at[tp]), (w_two, twos.at[tp]), (one_t, one_out), (two_t, two_out), (hid_ref, hid_out), (x_all, x_out))
    load, own_one, own_two, *saves = [local(src, dst, loc_sem.at[i]) for i, (src, dst) in enumerate(moves)]
    save_one, save_two, save_hid, save_x = saves
    own_one.start()
    own_two.start()
    for peer in plane.rings() + [{'pp': lax.rem(stage + d, stages)} for d in range(1, stages)]:
        signal(peer)

    own_one.wait()
    own_two.wait()
    load.start()
    pl.semaphore_wait(pltpu.get_barrier_semaphore(), 6 + last)
    def weight_steps(begun=False):
        return plane_gather(plane, [(ones, 0, ones.shape[1]), (twos, 0, twos.shape[1])], send_sem, recv_sem, begun=begun)

    @pl.when(core == 0)
    def _():
        next(weight_steps())

    rows, width = table.shape
    group = ids.shape[1]
    unit = piece.shape[0]
    count = group // tokens.shape[1]
    flatten(tokens.at[pl.ds(pl.multiple_of(stage * count, count), count)], ids)
    hot[:] = jnp.where(ids[:] - tp * rows == lax.broadcasted_iota(jnp.int32, hot.shape, 0), 1.0, 0.0).astype(BF16)
    load.wait()
    cut = rows // group * group
    for cols in tiles(width):
        picked = rows_dot(hot[:cut], table[:cut, cols]) + rows_dot(hot[cut:], table[cut:, cols])
        parts[:, :, :, cols] = picked.astype(BF16).reshape(*parts.shape[:-1], TILE)
    red = Reduce(plane, parts, got_one, sum_one, got_two, one_send, one_recv, two_send, two_recv)
    for half in BOTH:
        red.begin(half)

    @pl.when(core == 1)
    def _():
        pl.semaphore_wait(lead_sem, 1)
        next(weight_steps())

    gather = weight_steps(True)
    next(gather)

    @pl.when(core == 0)
    def _():
        pl.semaphore_signal(lead_sem, inc=1, device_id={'pp': stage + 1}, device_id_type=MESH)

    next(gather)
    red.middle()
    next(gather)
    next(gather)
    for half, total in enumerate(red.end()):
        piece[:, half * (width // 2):(half + 1) * (width // 2)] = total.astype(BF16)

    def line(p):
        return remote(piece, x_buf.at[pl.ds(pl.multiple_of(p * unit, unit), unit)], line_send, line_recv, {'pp': 0})

    @pl.when(stage != 0)
    def _():
        line(stage).start()

    @pl.when(stage == 0)
    def _():
        x_buf[:unit] = piece[:]

    drain(gather)

    @pl.when(stage == 1)
    def _():
        pl.semaphore_signal(lead_sem, inc=1, device_id={'pp': 0}, device_id_type=MESH)

    blocks, _, cols = ones.shape

    def spare_time():
        @pl.loop(0, blocks)
        def _(k):
            one_t[k] = ones[k].T
            two_t[k] = twos[k].T

        save_one.start()
        save_two.start()
        list_rows(tokens, tp * rows, rows, group, unit, flat, slot, order_out)

    pl.when(stage > 1)(spare_time)
    hop = remote(y_buf, x_buf, hop_send, hop_recv, {'pp': lax.rem(stage + 1, stages)})

    @pl.when(stage == 0)
    def _():
        got = x_buf.at[pl.ds(0, last * unit)]
        remote(got, got, line_send, line_recv, {'pp': last}).wait_recv()

    pl.when(stage > 0)(hop.wait_recv)
    x_act = x_buf[:]
    for k in range(blocks):
        hidden = dot(x_act, ones[k])
        hid_ref[k] = hidden
        a_buf[:, k * cols:(k + 1) * cols] = gelu(hidden).astype(BF16)
    save_hid.start()
    gate = a_buf[:]
    for tile in tiles(width):
        branch = dot(gate, twos[:, :, tile].reshape(blocks * cols, TILE))
        y_buf[:, tile] = (x_buf[:, tile].astype(F32) + branch).astype(BF16)

    pl.when(stage < last)(hop.start)
    x_all[tp] = x_buf[:]

    @pl.when(stage < SIDE)
    def _():
        pl.when(stage <= 1)(spare_time)

        @pl.when(stage == 0)
        def _():
            pl.semaphore_wait(lead_sem, 1)

        steps = plane_gather(plane, [(x_all, 0, x_all.shape[1])], send_sem, recv_sem, base=2)
        drain(steps)

    own_save = local(x_all.at[tp], x_out.at[tp], loc_sem.at[6])
    pl.when(stage < SIDE)(save_x.start)
    pl.when(stage >= SIDE)(own_save.start)

    spread = Spread(plane, last, stages, n_src, top, spread_send, spread_recv, die_send, die_recv)

    def own(p):
        return remote(y_buf.at[pl.ds(p * unit, unit)], own_x, own_send, own_recv, {'pp': p})

    @pl.when(stage == last)
    def _():
        n_src[:] = norm_of(y_buf[:])[1].astype(BF16)
        spread.send()
        for p in spread.others:
            own(p).start()
        own_x[:] = y_buf[last * unit:]

    pl.when(stage < last)(spread.arrive)
    drain(plane_gather(plane, [(top, spread.lo, spread.rows)], send_sem, recv_sem, spread.on_block, base=3))
    spread.finish()
    pl.when(stage < last)(own(last).wait_recv)
    spread.close()

    @pl.when(stage == last)
    def _():
        sent = y_buf.at[pl.ds(0, last * unit)]
        remote(sent, sent, own_send, own_recv, spread.mate).wait_send()

    red.close()

    @pl.when(stage != 0)
    def _():
        line(stage).wait_send()

    pl.when(stage < last)(hop.wait_send)
    for save in saves[:-1]:
        save.wait()
    pl.when(stage < SIDE)(save_x.wait)
    pl.when(stage >= SIDE)(own_save.wait)


def head_kernel(target, stages, chunk, table, top, own_x, labels, loss_out, g_top, g_out, n_out,
                n_buf, lab, g_buf, peak, stat, shared, scale_ref, parts, got_one, sum_one, got_two, piece,
                share_send, share_recv, one_send, one_recv, two_send, two_recv, line_send, line_recv, loc_sem, *e_bufs):
    plane = Plane()
    stage = lax.axis_index('pp')
    tp = plane.tp
    size = shared.shape[1]
    others = [p for p in range(stages) if p != target]
    each, group = peak.shape[1:]
    unit = group // size
    for d in range(1, size):
        signal({'tp': lax.rem(tp + d, size)})

    @pl.when(stage == target)
    def _():
        for p in others:
            signal({'pp': p})

    pl.when(stage != target)(functools.partial(signal, {'pp': target}))
    for p in range(stages):
        n_buf[p * group:(p + 1) * group] = top[:, p * unit:(p + 1) * unit, :].reshape(group, top.shape[2])
    save_n = local(n_buf, n_out, loc_sem.at[1])
    save_n.start()

    rows, width = table.shape
    flatten(labels, lab)
    lab[:] = lab[:] - tp * rows
    pieces = len(e_bufs)
    pair = each * group

    def group_at(b, i):
        return lax.rem(stage // each + b, pieces) * each + i

    def label_of(p):
        return lab[pl.ds(p, 1), :]

    def down(value, start):
        return start + lax.broadcasted_iota(jnp.int32, value.shape, 0)

    def logit_chunk(b, start):
        tokens = n_buf[pl.ds(pl.multiple_of(group_at(b, 0) * group, pair), pair), :]
        logits = cols_dot(table[pl.ds(start, chunk), :], tokens)
        e_bufs[b][pl.ds(start, chunk), :] = logits
        return fold(jnp.max, logits)

    def exp_chunk(b, start, label, top_b, total, hits):
        logits = e_bufs[b][pl.ds(start, chunk), :]
        e = jnp.exp(logits - top_b)
        e_bufs[b][pl.ds(start, chunk), :] = e
        return total + fold(jnp.sum, e), hits + fold(jnp.sum, jnp.where(label == down(logits, start), logits, 0.0))

    def chunks(body, carry):
        return lax.fori_loop(0, rows // chunk, lambda c, carry: body(pl.multiple_of(c * chunk, 8), carry), carry)

    def msg(d, k):
        some = pl.ds(k, 1 + k * (pieces - 2))
        return remote(stat.at[some], shared.at[some, tp], share_send.at[k], share_recv.at[k], {'tp': lax.rem(tp + d, size)})

    def shares(k):
        ref = shared.at[pl.ds(k, 1 + k * (pieces - 2)), pl.ds(0, size - 1)]
        return remote(ref, ref, share_send.at[k], share_recv.at[k], {'tp': plane.at(1, 0)})

    def share(k):
        for d in range(1, size):
            msg(d, k).start()

    losses = []

    def normalise(k):
        shares(k).wait_recv()
        for b in (range(1, pieces) if k else range(1)):
            every = shared[b, :, 0]
            most = jnp.max(every, axis=0)
            log_norm = most + jnp.log(jnp.sum(jnp.exp(every - most[None]), axis=0))
            losses.append(jnp.sum(log_norm - jnp.sum(shared[b, :, 1], axis=0), keepdims=True))
            scale_ref[b] = jnp.exp(peak[b] - log_norm)

    def grad_block(b, i, slot):
        cols = pl.ds(pl.multiple_of(i * group, group), group)
        label = label_of(group_at(b, i))
        factor = scale_ref[b, pl.ds(i, 1), :]

        def part(start, _):
            e = e_bufs[b][pl.ds(start, chunk), cols]
            hit = label == down(e, start)
            g_buf[slot, pl.ds(start, chunk), :] = (e * factor - jnp.where(hit, 1.0, 0.0)).astype(BF16)

        chunks(part, None)

    def save(k):
        slot = 1 + k % 2
        at = pl.multiple_of(group_at(k // each, k % each) * group, group)
        return local(g_buf.at[slot], g_out.at[:, pl.ds(at, group)], loc_sem.at[2 + slot])

    def gradient(k):
        if k >= 2:
            save(k - 2).wait()
        grad_block(k // each, k % each, 1 + k % 2)
        save(k).start()

    cut = rows // group * group
    half = width // 2
    red = Reduce(plane, parts, got_one, sum_one, got_two, one_send, one_recv, two_send, two_recv)

    def own_gradient():
        grad_block(0, lax.rem(stage, each), 0)
        mine_g = g_buf.at[0]
        for cols in tiles(width):
            back = rows_dot(mine_g[:cut, :], table[:cut, cols]) + rows_dot(mine_g[cut:, :], table[cut:, cols])
            parts[:, :, :, cols] = back.reshape(*parts.shape[:-1], TILE)
            if cols.stop % half == 0:
                red.begin(cols.start // half)

    tops = []
    zero = jnp.zeros((8, pair), F32)
    for now, done in ((0, None), (None, 0), (1, None), *((b, b - 1) for b in range(2, pieces)), (None, pieces - 1)):
        label = None if done is None else jnp.concatenate([label_of(group_at(done, i)) for i in range(each)], axis=1)
        top_b = None if done is None else tops[done]

        def both(start, carry, now=now, done=done, top_b=top_b, label=label):
            best, total, hits = carry
            if now is not None:
                best = jnp.maximum(best, logit_chunk(now, start))
            if done is not None:
                total, hits = exp_chunk(done, start, label, top_b, total, hits)
            return best, total, hits

        best, total, hits = chunks(both, (jnp.full((8, pair), -jnp.inf, F32), zero, zero))
        if done is not None:
            found = (top_b + jnp.log(jnp.sum(total, axis=0, keepdims=True)), jnp.sum(hits, axis=0, keepdims=True), top_b)
            for i in range(each):
                cols = slice(i * group, (i + 1) * group)
                for kind in BOTH:
                    stat[done, kind, i:i + 1, :] = found[kind][:, cols]
                peak[done, i:i + 1, :] = found[2][:, cols]
            shared[done, tp] = stat[done]
        if done == 0:
            pl.semaphore_wait(pltpu.get_barrier_semaphore(), size - 1 + jnp.where(stage == target, len(others), 1))
        if now is None:
            share(1 if done else 0)
        else:
            tops.append(jnp.max(best, axis=0, keepdims=True))
        if now == 1:
            normalise(0)
            own_gradient()
        if now == pieces - 1:
            red.middle()

    gradient(0)
    gradient(1)
    sums = red.end()

    inv_rms, normed = norm_of(own_x[:])
    mean = (jnp.sum(normed[:, :half] * sums[0], axis=-1, keepdims=True) + jnp.sum(normed[:, half:] * sums[1], axis=-1, keepdims=True)) / width
    for h in BOTH:
        cols = slice(h * half, (h + 1) * half)
        piece[:, cols] = (inv_rms * (sums[h] - normed[:, cols] * mean)).astype(BF16)

    def line(p):
        return remote(piece, g_top.at[p], line_send, line_recv, {'pp': target})

    @pl.when(stage != target)
    def _():
        line(stage).start()

    normalise(1)
    for k in range(2, stages):
        gradient(k)
    loss_out[:] = sum(losses) / (stages * group)
    @pl.when(stage == target)
    def _():
        g_top[target] = piece[:]
        got = g_top.at[pl.ds(0, len(others))]
        remote(got, got, line_send, line_recv, {'pp': 0}).wait_recv()

    red.close()
    for k in BOTH:
        shares(k).wait_send()
    save_n.wait()
    save(stages - 2).wait()
    save(stages - 1).wait()
    @pl.when(stage != target)
    def _():
        line(stage).wait_send()


def backward_kernel(last, chunk, g_top, hid_in, two_all, one_all, g_all, n_all, x_in, w_one, w_two, de_buf, dx_all, grad_one, grad_two,
                    ones, twos, slope_ref, g_buf, n_buf, x_all, w_one_buf, w_two_buf, dy_all, dy_buf, dx_buf, d_buf,
                    send_sem, recv_sem, spread_send, spread_recv, die_send, die_recv, hop_send, hop_recv, go_sem, ready_sem, g_sem, loc_sem):
    plane = Plane()
    stage = lax.axis_index('pp')
    stages = last + 1
    blocks, cols, width = one_all.shape
    pairs = ((hid_in, slope_ref), (two_all, twos), (one_all, ones), (n_all, n_buf), (w_one, w_one_buf), (w_two, w_two_buf))
    loads = [local(src, dst, loc_sem.at[i]) for i, (src, dst) in enumerate(pairs)]
    lower = stage < SIDE
    upper = stage >= SIDE
    own = plane.tp
    load_x = [local(*pair, loc_sem.at[6]) for pair in ((x_in, x_all), (x_in.at[own], x_all.at[own]))]

    mid = upper & (stage < last - 1)

    def start(some):
        for load in some:
            load.start()

    pl.when(upper)(functools.partial(start, loads[:3]))
    pl.when(lower)(functools.partial(start, loads[3:4]))
    own_load = load_x[1]
    pl.when(mid)(own_load.start)
    spread = Spread(plane, 0, stages, dx_buf, dx_all, spread_send, spread_recv, die_send, die_recv)
    near = plane.near()
    for peer in near:
        signal(peer)
    extra = spread.greet()
    before = {'pp': lax.rem(stage + last, stages)}
    pl.when(stage > 0)(functools.partial(signal, before))
    hop = remote(dx_buf, dy_buf, hop_send, hop_recv, before)
    rows = de_buf.shape[0]
    pieces = -(-rows // chunk)

    def piece_at(c):
        return pl.ds(pl.multiple_of(jnp.minimum(c * chunk, rows - chunk), 8), chunk)

    def fetch(c):
        slot = lax.rem(c, 2)
        return local(g_all.at[piece_at(c)], g_buf.at[slot], g_sem.at[slot])

    def table(lo, hi):
        if lo == 0:
            fetch(0).start()
            loads[3].wait()

        @pl.loop(lo, hi)
        def _(c):
            @pl.when(c < pieces - 1)
            def _():
                fetch(c + 1).start()

            for i, some in enumerate((loads[:2], loads[2:3], loads[4:] + load_x[:1])):
                pl.when(lower & (c == i + 1))(functools.partial(start, some))

            fetch(c).wait()
            de_buf[piece_at(c), :] = dot(g_buf[lax.rem(c, 2)], n_buf[:])

    pl.semaphore_wait(pltpu.get_barrier_semaphore(), len(near) + extra + jnp.where(stage < last, 1, 0))

    @pl.when(stage < last)
    def _():
        pl.semaphore_signal(ready_sem, inc=1, device_id={'pp': lax.rem(stage + 1, stages)}, device_id_type=MESH)

    pl.when(lower)(functools.partial(table, 0, pieces))
    loads[0].wait()
    for k in range(blocks):
        slope_ref[k] = gelu_slope(slope_ref[k])
    loads[1].wait()

    def a_steps(begun=False):
        return plane_gather(plane, [(x_all, 0, x_all.shape[1])], send_sem, recv_sem, base=2, begun=begun)

    mid_steps = a_steps()

    @pl.when(mid)
    def _():
        own_load.wait()
        for _ in range(3):
            next(mid_steps)

    @pl.when(stage == last)
    def _():
        dy_buf[:] = g_top[:]

    pl.when(stage < last)(hop.wait_recv)
    dy_all[plane.tp] = dy_buf[:]
    whole = (dy_all, 0, dy_all.shape[1])
    part = (dx_all, spread.lo, spread.rows)

    def dy_steps(begun):
        return plane_gather(plane, [whole], send_sem, recv_sem, base=1, begun=begun)

    @pl.when(stage <= 1)
    def _():
        next(dy_steps(False))

    grad_y = dy_buf[:]
    for k in range(blocks):
        grad_gate = dot(grad_y, twos[k])
        d_buf[:, k * cols:(k + 1) * cols] = (slope_ref[k] * grad_gate).astype(BF16)
    loads[2].wait()
    grad_hidden = d_buf[:]
    for tile in tiles(width):
        back = dot(grad_hidden, ones[:, :, tile].reshape(blocks * cols, TILE))
        dx_buf[:, tile] = (dy_buf[:, tile].astype(F32) + back).astype(BF16)

    @pl.when(stage > 0)
    def _():
        pl.semaphore_wait(ready_sem, 1)
        hop.start()

    pl.when(stage == 0)(spread.send)
    pl.when(upper)(functools.partial(start, loads[3:]))
    pl.when(upper & jnp.logical_not(mid))(own_load.start)
    for load in loads[4:]:
        load.wait()
    pl.when(lower)(load_x[0].wait)
    pl.when(upper & jnp.logical_not(mid))(own_load.wait)

    grad_one[:] = jnp.zeros_like(grad_one)
    grad_two[:] = jnp.zeros_like(grad_two)

    def weights(ahead):
        step = SIDE

        @pl.loop(0, 2)
        def _(i):
            row = lax.rem(plane.z + (1 + i if ahead else SIDE - i), SIDE)
            part = pl.ds(row * step, step)
            x_act = x_all[part].reshape(step * x_all.shape[1], width)
            grad_y = dy_all[part].reshape(step * x_all.shape[1], width)
            hidden = dot(x_act, w_one_buf[:])
            grad_gate = cols_dot(grad_y, w_two_buf[:])
            grad_hidden = (gelu_slope(hidden) * grad_gate).astype(BF16)
            grad_one[:] += rows_dot(x_act, grad_hidden)
            grad_two[:] += rows_dot(gelu(hidden).astype(BF16), grad_y)

    def dx_steps():
        return plane_gather(plane, [part], send_sem, recv_sem, spread.on_block)

    @pl.when(stage > 1)
    def _():
        hop.wait_send()

        @pl.when(spread.core == 0)
        def _():
            pl.semaphore_signal(go_sem, inc=1, device_id=spread.mate, device_id_type=MESH)

        @pl.when(spread.core == 1)
        def _():
            pl.semaphore_wait(go_sem, 1)

    @pl.when(stage > 1)
    def _():
        next(dy_steps(False))

    @pl.when(upper & jnp.logical_not(mid))
    def _():
        next(a_steps())

    planes = [(stage <= 1, None, 'xddxdxdxdxdx', 'x'), ((stage > 1) & lower, None, 'dddxdxdxdx', 'xxx'),
              (mid, mid_steps, 'dtdadatdaxdaxdx', 'xxx'), (upper & jnp.logical_not(mid), a_steps(True), 'datdadatdaxdaxdax', 'xxx')]
    runs = []
    for here, more, order, rest in planes:
        steps = {'d': dy_steps(True), 'x': dx_steps(), 'a': more}

        def arrived(order=order, steps=steps):
            part = -(-pieces // 2)
            for i, kind in enumerate(order):
                if kind == 't':
                    lo = order[:i].count('t') * part
                    table(lo, min(lo + part, pieces))
                    continue
                if kind == 'x' and 'x' not in order[:i]:
                    pl.when(stage > 0)(spread.arrive)
                next(steps[kind])
            next(steps['d'])
            drain(steps['a'] or ())

        def onward(rest=rest, steps=steps):
            for kind in rest:
                next(steps[kind])
            drain(steps['d'])

        pl.when(here)(arrived)
        runs.append((here, onward, functools.partial(drain, steps['x'])))

    weights(False)
    for here, onward, _ in runs:
        pl.when(here)(onward)
    weights(True)
    for here, _, finish in runs:
        pl.when(here)(finish)

    spread.finish()
    spread.close()

    pl.when(stage == 1)(hop.wait_send)


def add_kernel(pieces, order, dx_ref, de_ref, loss_ref, one_ref, two_ref, de_out, loss_out, table_out, one_out, two_out, wide, sem):
    small = ((one_ref, one_out), (two_ref, two_out), (loss_ref, loss_out))
    saves = [local(*pair, sem.at[i]) for i, pair in enumerate(small)]
    for save in saves:
        save.start()
    wide[:] = dx_ref[:].astype(F32)

    @pl.loop(0, order[2, 0])
    def _(j):
        row = pl.ds(order[1, j], 1)
        de_out[row, :] = de_out[row, :] + wide[pl.ds(order[0, j], 1), :]

    rows = de_ref.shape[0]
    size = -(-rows // (8 * pieces)) * 8
    for c in range(pieces):
        part = pl.ds(c * size, min(size, rows - c * size))
        saves.append(local(de_out.at[part], table_out.at[part], sem.at[len(small) + c]))
        saves[-1].start()
    for save in saves:
        save.wait()


def vmem():
    return pl.BlockSpec(memory_space=pltpu.VMEM)


def anywhere():
    return pl.BlockSpec(memory_space=pl.ANY)


def params(cid, mib):
    return pltpu.CompilerParams(collective_id=cid, has_side_effects=True, vmem_limit_bytes=mib << 20)


DMA = pltpu.SemaphoreType.DMA


def solution(mesh):
    pp_size = mesh.shape['pp']
    tp_size = mesh.shape['tp']
    last = pp_size - 1

    def device_fn(tokens, labels, emb_table, w_in, w_out):
        num_tokens = tokens.shape[0] * tokens.shape[1]
        vocab_rows, width = emb_table.shape
        w_one, w_two = w_in[0], w_out[0]
        cols = w_one.shape[1]
        unit = num_tokens // (pp_size * tp_size)
        block = pp_size * unit
        group = tp_size * unit
        half = width // 2
        chunk = vocab_rows // 3
        step = 512
        pair = 2 * group
        shape = jax.ShapeDtypeStruct
        VM = pltpu.VMEM

        def reduce_scratch(dtype):
            return [VM((SIDE, SIDE, unit, width), dtype), VM((6, SIDE, unit, half), dtype), VM((2, SIDE, unit, half), dtype), VM((6, unit, half), dtype), VM((unit, width), BF16)]

        duo = DMA((2,))
        reduce_sems = [DMA, duo, DMA, duo, DMA, DMA]
        many = shape((tp_size, block, width), BF16)
        many_buf = VM((tp_size, block, width), BF16)
        two_sums = 2 * SLOTS
        gather_sems = [DMA((4,)), DMA((4 * two_sums,))]
        spread_sems = [DMA, DMA, DMA, DMA]

        top, own_x, table, order, hidden, one_t, two_t, x_all = pl.pallas_call(
            functools.partial(forward_kernel, last),
            out_shape=(many_buf, VM((unit, width), BF16), VM((vocab_rows, width), BF16), shape((3, num_tokens), jnp.int32), shape((tp_size, block, cols), F32), shape((tp_size, cols, width), BF16), shape((tp_size, width, cols), BF16), many),
            in_specs=[vmem()] + [anywhere()] * 3,
            out_specs=[vmem()] * 4 + [anywhere()] * 4,
            scratch_shapes=[VM((tp_size, width, cols), BF16), VM((tp_size, cols, width), BF16), VM((tp_size, cols, width), BF16), VM((tp_size, width, cols), BF16),
                            VM((vocab_rows, group), BF16), *reduce_scratch(BF16),
                            VM((block, width), BF16), VM((block, width), BF16), VM((block, width), BF16), VM((block, tp_size * cols), BF16), VM((tp_size, block, cols), F32), many_buf, VM((1, group), jnp.int32),
                            VM((num_tokens // 128, 128), jnp.int32), VM((2, num_tokens), jnp.int32),
                            *gather_sems, *reduce_sems, DMA, DMA, *spread_sems, DMA, DMA, pltpu.SemaphoreType.REGULAR, DMA((7,))],
            compiler_params=params(1, 49), name='forward_chain',
        )(tokens, emb_table, w_one, w_two)

        by_pair = (num_tokens // pair, pair // group, group)
        loss, g_top, g_all, n_all = pl.pallas_call(
            functools.partial(head_kernel, last, pp_size, chunk),
            out_shape=(VM((1, 1), F32), pltpu.HBM((pp_size, unit, width), BF16), shape((vocab_rows, num_tokens), BF16), shape((num_tokens, width), BF16)),
            in_specs=[vmem()] * 4,
            out_specs=[vmem()] * 2 + [anywhere()] * 2,
            scratch_shapes=[VM((num_tokens, width), BF16), VM((pp_size, group), jnp.int32), VM((3, vocab_rows, group), BF16),
                            VM(by_pair, F32), VM((by_pair[0], 2, *by_pair[1:]), F32), VM((by_pair[0], tp_size, 2, *by_pair[1:]), F32), VM(by_pair, F32), *reduce_scratch(F32),
                            duo, duo, *reduce_sems, DMA((5,)),
                            *[VM((vocab_rows, pair), F32) for _ in range(num_tokens // pair)]],
            compiler_params=params(2, 49), name='head',
        )(*[pltpu.with_memory_space_constraint(array, pltpu.VMEM) for array in (table, top, own_x)], labels)

        de_head, dx_first, grad_one, grad_two = pl.pallas_call(
            functools.partial(backward_kernel, last, step),
            out_shape=(VM((vocab_rows, width), F32), many_buf, VM((width, cols), F32), VM((cols, width), F32)),
            in_specs=[vmem()] + [anywhere()] * 8, out_specs=[vmem()] * 4,
            scratch_shapes=[VM((tp_size, cols, width), BF16), VM((tp_size, width, cols), BF16), VM((tp_size, block, cols), F32), VM((2, step, num_tokens), BF16), VM((num_tokens, width), BF16),
                            many_buf, VM((width, cols), BF16), VM((cols, width), BF16), many_buf,
                            VM((block, width), BF16), VM((block, width), BF16), VM((block, tp_size * cols), BF16),
                            *gather_sems, *spread_sems, DMA, DMA, pltpu.SemaphoreType.REGULAR, pltpu.SemaphoreType.REGULAR, duo, DMA((7,))],
            compiler_params=params(3, 45), name='backward_chain',
        )(g_top.reshape(block, width), hidden, two_t, one_t, g_all, n_all, x_all, w_one, w_two)

        smem = pl.BlockSpec(memory_space=pltpu.SMEM)
        _, loss, grad_table, grad_one, grad_two = pl.pallas_call(
            functools.partial(add_kernel, 12),
            out_shape=(VM((vocab_rows, width), F32), shape((1, 1), F32), shape((vocab_rows, width), F32), shape((width, cols), F32), shape((cols, width), F32)),
            in_specs=[smem] + [vmem()] * 5, out_specs=[vmem()] + [anywhere()] * 4,
            scratch_shapes=[VM((num_tokens, width), F32), DMA((15,))], input_output_aliases={2: 0},
            compiler_params=pltpu.CompilerParams(vmem_limit_bytes=24 << 20), name='add_rows',
        )(order, dx_first.reshape(num_tokens, width), de_head, loss, grad_one, grad_two)
        return loss.reshape(1), grad_one[None], grad_two[None], grad_table

    return jax.shard_map(device_fn, mesh=mesh, in_specs=(P('dp', None), P('dp', None), P('tp', None), P('pp', None, 'tp'), P('pp', 'tp', None)), out_specs=(P('dp'), P(('dp', 'pp'), None, 'tp'), P(('dp', 'pp'), 'tp', None), P(('dp', 'tp'), None)), check_vma=False)
```
